32 devices in a mesh: dp: 8 (over y, x, core), seq: 4 (over z).
Axes of the slice: x: 2, y: 2, z: 4, core: 2. Of those that a mesh axis runs over, the one named last changes fastest.
Arguments:
- tokens: bfloat16 [32, 512, 768], P('dp', 'seq'), may hold values from -6 to 6
- cotangent: bfloat16 [32, 512, 768], P('dp', 'seq'), may hold values from -6 to 6
- tok_weight: int32 [32, 512], P('dp', 'seq'), may hold values from 1 to 4
- mask_count: int32 [32], P('dp'), may hold values from 0 to 512
- owner_list: int32 [384], replicated, may hold values from 0 to 383, as said below
- masters: float32 [384, 36864], P('dp'), may hold values from -0.5412659 to 0.5412659
- moment_one: float32 [384, 36864], P('dp'), may hold values from -13.568 to 13.568
- moment_two: float32 [384, 36864], P('dp'), may hold values from 0.98304 to 1114.112, as said below
- left_basis: float32 [384, 36864], P('dp'), may hold values from -1 to 1, as said below
- right_basis: float32 [384, 36864], P('dp'), may hold values from -1 to 1, as said below
- vectors: float32 [2, 9216], replicated, may hold values from -1.5 to 1.5, as said below
- vec_moment_one: float32 [2, 9216], replicated, may hold values from -23.68 to 23.68
- vec_moment_two: float32 [2, 9216], replicated, may hold values from 209.7152 to 3391.488, as said below
Outputs:
- layer_out: bfloat16 [32, 512, 768], P('dp', 'seq')
- input_grad: float32 [32, 512, 768], P('dp', 'seq')
- new_moment_one: float32 [384, 36864], P('dp')
- new_moment_two: float32 [384, 36864], P('dp')
- new_masters: float32 [384, 36864], P('dp')
- master_copies: bfloat16 [384, 36864], P('dp')
- new_vectors: float32 [2, 9216], replicated
- new_vec_moment_one: float32 [2, 9216], replicated
- new_vec_moment_two: float32 [2, 9216], replicated
The draws below stay inside these ranges and needn't reach their ends.
Inputs may be any that keep to these rules, and one draw needn't show every extreme that they name: `owner_list`: a permutation: each row of the block arrays is named by exactly one block. `moment_two`: all entries positive. `left_basis`: each row, read as a 192 x 192 matrix, is orthogonal. `right_basis`: each row, read as a 192 x 192 matrix, is orthogonal. `vectors`: gains lie in 0.6 to 1.4. `vec_moment_two`: all entries positive.
All inputs are finite; a program needn't handle non-finite values.
Results may differ from the reference program's by a relative error of at most 0.015.
The reference program's roundings to bfloat16 on the way count: a program that leaves them out, or rounds other values in their place, can miss the bound.
Values may be sent and summed in bfloat16 or wider, within the bound.
A program may use at most 512 MiB of HBM per device.

```python
import math
import jax
import jax.numpy as jnp
import numpy as np
from jax import lax

D = 768
HEADS = 12
HDIM = 64
FF = 3072
L = 512
LAYERS = 2
BLK = 192
SEQ_G = 4
SEQS = 32
TOKENS = 16384
VEC = 9216
NBLK = 384
N_DP = 8


decay_ratio = 0.05 / 0.95


def slot_order(key):
    return jax.random.permutation(jax.random.fold_in(key, 7), NBLK).astype(jnp.int32)


def slot_scales(key):
    per_layer = NBLK // LAYERS
    inner_edge = D // BLK
    outer_edge = FF // BLK
    square = inner_edge * inner_edge
    number = jnp.arange(NBLK) % per_layer
    up_end = 4 * square + inner_edge * outer_edge
    weight_scale = jnp.where(number < 3 * square, D ** (-0.5), jnp.where(number < 4 * square, 3.0 * D ** (-0.5), jnp.where(number < up_end, D ** (-0.5), FF ** (-0.5))))
    grad_scale = jnp.where(number < 2 * square, 0.05, jnp.where(number < 3 * square, 0.3, jnp.where(number < 4 * square, 0.15, jnp.where(number < up_end, 0.2, 0.4)))) * TOKENS ** 0.5
    order = slot_order(key)
    weight_slot = jnp.zeros((NBLK,), jnp.float32).at[order].set(weight_scale.astype(jnp.float32))
    grad_slot = jnp.zeros((NBLK,), jnp.float32).at[order].set(grad_scale.astype(jnp.float32))
    return (weight_slot, grad_slot)


def rotation(key):
    keys = jax.random.split(key, 3)
    order = jax.vmap(lambda sub: jax.random.permutation(sub, BLK))(jax.random.split(keys[0], NBLK)).astype(jnp.int32)
    row_sign = (jax.random.randint(keys[1], (NBLK, BLK), 0, 2) * 2 - 1).astype(jnp.float32)
    col_sign = (jax.random.randint(keys[2], (NBLK, BLK), 0, 2) * 2 - 1).astype(jnp.float32)
    column = jnp.arange(BLK, dtype=jnp.int32)
    phase = order[:, :, None] * (2 * column[None, None, :] + 1) % (4 * BLK)
    table = jnp.cos(math.pi * phase.astype(jnp.float32) / (2.0 * BLK)) * math.sqrt(2.0 / BLK)
    table = jnp.where(order[:, :, None] == 0, math.sqrt(1.0 / BLK), table)
    return (table * row_sign[:, :, None] * col_sign[:, None, :]).astype(jnp.float32).reshape(NBLK, BLK * BLK)


def draw_owner_list(key, part):
    return slot_order(key)


def draw_masters(key, part):
    weight_slot, grad_slot = slot_scales(key)
    noise = jnp.clip(jax.random.normal(jax.random.fold_in(key, 11), (NBLK, BLK * BLK), jnp.float32), -5.0, 5.0)
    return noise * weight_slot[:, None]


def draw_moment_one(key, part):
    weight_slot, grad_slot = slot_scales(key)
    noise = jnp.clip(jax.random.normal(jax.random.fold_in(key, 13), (NBLK, BLK * BLK), jnp.float32), -5.0, 5.0)
    return noise * (decay_ratio * grad_slot)[:, None]


def draw_moment_two(key, part):
    weight_slot, grad_slot = slot_scales(key)
    factor = jnp.exp(jax.random.uniform(jax.random.fold_in(key, 17), (NBLK, BLK * BLK), jnp.float32, math.log(0.5), math.log(8.0)))
    return factor * (decay_ratio * grad_slot * grad_slot)[:, None]


def draw_left_basis(key, part):
    return rotation(jax.random.fold_in(key, 19))


def draw_right_basis(key, part):
    return rotation(jax.random.fold_in(key, 23))


def draw_vectors(key, part):
    column = jnp.arange(VEC)
    is_gain = (column >= 4 * D) & (column < 5 * D) | (column >= 6 * D) & (column < 7 * D)
    gains = jax.random.uniform(jax.random.fold_in(key, 29), (LAYERS, VEC), jnp.float32, 0.6, 1.4)
    biases = 0.3 * jnp.clip(jax.random.normal(jax.random.fold_in(key, 31), (LAYERS, VEC), jnp.float32), -5.0, 5.0)
    return jnp.where(is_gain[None, :], gains, biases)


def draw_vec_moment_one(key, part):
    noise = jnp.clip(jax.random.normal(jax.random.fold_in(key, 37), (LAYERS, VEC), jnp.float32), -5.0, 5.0)
    return noise * (decay_ratio * 0.7 * TOKENS ** 0.5)


def draw_vec_moment_two(key, part):
    factor = jnp.exp(jax.random.uniform(jax.random.fold_in(key, 41), (LAYERS, VEC), jnp.float32, math.log(0.5), math.log(8.0)))
    return factor * (decay_ratio * 0.49 * TOKENS)


def plant(values, rng, least, top_value):
    longest = values.shape.index(max(values.shape))
    spots = []
    for shift in (0, 1):
        where = [jax.random.randint(jax.random.fold_in(rng, axis), (), 0, length) for axis, length in enumerate(values.shape)]
        where[longest] = (where[longest] + shift) % values.shape[longest]
        spots.append(tuple(where))
    return values.at[spots[0]].set(least).at[spots[1]].set(top_value)


def block_scale(rng, dims, pieces, smallest, largest):
    level, own = 1.0, jax.random.fold_in(rng, 6)
    for dim, blocks in pieces:
        heights = jnp.exp(jax.random.uniform(jax.random.fold_in(own, dim), (blocks,), jnp.float32, smallest / len(pieces), largest / len(pieces)))
        level = level * jnp.repeat(heights, dims[dim] // blocks).reshape([-1 if axis == dim else 1 for axis in range(len(dims))])
    return level


def rank_bounds(number_of, lean):
    portions = [(1 << 20) // math.isqrt(rank ** lean) + 1 for rank in range(1, number_of + 1)]
    width = 1 + sum(portions) // (1 << 30)
    return np.cumsum(np.array([max(1, weight // width) for weight in portions]))


def skewed_ids(key, extent, number_of, slope):
    grid = rank_bounds(number_of, slope)
    pick = jax.random.randint(jax.random.fold_in(key, 1), extent, 0, int(grid[number_of - 1]))
    standing = jnp.searchsorted(jnp.asarray(grid, jnp.int32), pick, side="right")
    return jax.random.permutation(jax.random.fold_in(key, 2), number_of)[standing].astype(jnp.int32)


def normal_values(rng, dims, width, bound, pieces=(), kind=jnp.bfloat16):
    array = jax.random.normal(rng, dims, jnp.float32) * width
    if len(pieces) > 0:
        array = block_scale(rng, dims, pieces, -0.22, 0.18) * array
    return jnp.clip(array, min=-bound, max=bound).astype(kind)


def setup_inputs(seed: int = 0) -> dict:
    splits = jax.random.split(jax.random.key(seed), 14)
    return {
        "tokens": normal_values(splits[0], (SEQS, L, D), 1.0, 6.0, ((0, 8), (1, 4))),
        "cotangent": normal_values(splits[1], (SEQS, L, D), 1.0, 6.0, ((0, 8), (1, 4))),
        "tok_weight": plant(jax.random.randint(splits[2], (SEQS, L), 1, 5), jax.random.fold_in(splits[2], 1), 1, 4).astype(jnp.int32),
        "mask_count": plant(skewed_ids(splits[3], (SEQS,), L + 1, 2), jax.random.fold_in(splits[3], 3), 0, L).astype(jnp.int32),
        "owner_list": draw_owner_list(jax.random.fold_in(splits[13], 71), 0),
        "masters": draw_masters(jax.random.fold_in(splits[13], 71), 0),
        "moment_one": draw_moment_one(jax.random.fold_in(splits[13], 71), 0),
        "moment_two": draw_moment_two(jax.random.fold_in(splits[13], 71), 0),
        "left_basis": draw_left_basis(jax.random.fold_in(splits[13], 71), 0),
        "right_basis": draw_right_basis(jax.random.fold_in(splits[13], 71), 0),
        "vectors": draw_vectors(jax.random.fold_in(splits[13], 71), 0),
        "vec_moment_one": draw_vec_moment_one(jax.random.fold_in(splits[13], 71), 0),
        "vec_moment_two": draw_vec_moment_two(jax.random.fold_in(splits[13], 71), 0),
    }


@jax.custom_vjp
def low(v):
    return lax.optimization_barrier(v.astype(jnp.bfloat16)).astype(jnp.float32)

@jax.custom_vjp
def low_back(v):
    return v

def low_keep(v):
    return (low(v), None)

def low_pass(kept, grad):
    return (grad,)

def back_keep(v):
    return (v, None)

def back_low(kept, grad):
    return (low(grad),)
low.defvjp(low_keep, low_pass)
low_back.defvjp(back_keep, back_low)
beta_one = 0.95
beta_two = 0.95
adam_eps = 1e-08
matrix_rate = 0.02
vector_rate = 0.2
decay_rate = 0.01
step_count = 6

def matmul_high(left, right):
    return jnp.dot(left, right, precision=lax.Precision.HIGHEST, preferred_element_type=jnp.float32)

def matrix_shapes():
    return [(D, D), (D, D), (D, D), (D, D), (D, FF), (FF, D)]

def to_matrices(blocks):
    result = []
    cursor = 0
    for layer_num in range(LAYERS):
        members = []
        for row_size, col_size in matrix_shapes():
            row_count = row_size // BLK
            col_count = col_size // BLK
            tile_set = blocks[cursor:cursor + row_count * col_count]
            members.append(tile_set.reshape(row_count, col_count, BLK, BLK).transpose(0, 2, 1, 3).reshape(row_size, col_size))
            cursor = cursor + row_count * col_count
        result.append(members)
    return result

def to_blocks(matrices):
    tile_list = []
    for members in matrices:
        for matrix in members:
            row_size, col_size = matrix.shape
            tile_list.append(matrix.reshape(row_size // BLK, BLK, col_size // BLK, BLK).transpose(0, 2, 1, 3).reshape(-1, BLK, BLK))
    return jnp.concatenate(tile_list, axis=0)

def layer_norm(hidden, gain, shift):
    center = hidden - lax.optimization_barrier(jnp.mean(hidden, axis=-1, keepdims=True))
    spread = lax.optimization_barrier(jnp.mean(center * center, axis=-1, keepdims=True))
    return center * lax.rsqrt(spread + 1e-05) * gain + shift

def one_layer(hidden, matrices, vector):
    w_query, w_key, w_value, w_out, w_up, w_down = [low(matrix) for matrix in matrices]
    bias_query = vector[0:D]
    bias_value = vector[D:2 * D]
    bias_out = vector[2 * D:3 * D]
    bias_down = vector[3 * D:4 * D]
    gain_one = vector[4 * D:5 * D]
    shift_one = vector[5 * D:6 * D]
    gain_two = vector[6 * D:7 * D]
    shift_two = vector[7 * D:8 * D]
    bias_up = vector[8 * D:]
    batch = hidden.shape[0]
    hid_low = low(hidden)

    def heads(tensor):
        return low(low_back(tensor)).reshape(batch, L, HEADS, HDIM)
    query = heads(matmul_high(hid_low, w_query) + bias_query)
    keys = heads(matmul_high(hid_low, w_key))
    values = heads(matmul_high(hid_low, w_value) + bias_value)
    scores = jnp.einsum('bqhe,bkhe->bhqk', query, keys, precision=lax.Precision.HIGHEST) * HDIM ** (-0.5)
    scores = low_back(scores)
    probs = low(jax.nn.softmax(scores, axis=-1))
    mixed = jnp.einsum('bhqk,bkhe->bqhe', probs, values, precision=lax.Precision.HIGHEST).reshape(batch, L, D)
    mixed = low(low_back(mixed))
    branch = low_back(matmul_high(mixed, w_out) + bias_out)
    normed = layer_norm(hidden + branch, gain_one, shift_one)
    pre_act = low_back(matmul_high(low(normed), w_up) + bias_up)
    act_low = low(jax.nn.gelu(pre_act, approximate=False))
    down = low_back(matmul_high(act_low, w_down) + bias_down)
    return layer_norm(normed + down, gain_two, shift_two)

def forward(params, hidden):
    matrices, vectors = params
    for layer_num in range(LAYERS):
        hidden = one_layer(hidden, matrices[layer_num], vectors[layer_num])
    return hidden

def reference(tokens, cotangent, tok_weight, mask_count, owner_list, masters, moment_one, moment_two, left_basis, right_basis, vectors, vec_moment_one, vec_moment_two):
    cube = (NBLK, BLK, BLK)
    masters_sq = masters.reshape(cube)
    moment_one_sq = moment_one.reshape(cube)
    moment_two_sq = moment_two.reshape(cube)
    left_sq = left_basis.reshape(cube)
    right_sq = right_basis.reshape(cube)
    matrices = to_matrices(masters_sq[owner_list])
    params = (matrices, vectors)
    positions = jnp.arange(L, dtype=jnp.int32)
    masked = (positions[None, :] < mask_count[:, None]).astype(jnp.float32)
    factor = tok_weight.astype(jnp.float32) * (1.0 + masked) * 0.25
    cot_all = (cotangent.astype(jnp.float32) * factor[:, :, None]).reshape(N_DP, SEQ_G, L, D)
    x_all = tokens.astype(jnp.float32).reshape(N_DP, SEQ_G, L, D)

    def one_batch(totals, batch):
        inputs, cots = batch
        outputs, pull = jax.vjp(forward, params, inputs)
        grad_params, grad_inputs = pull(cots)
        totals = jax.tree.map(jnp.add, totals, grad_params)
        return (totals, (outputs.astype(jnp.bfloat16), grad_inputs))
    zeros = jax.tree.map(jnp.zeros_like, params)
    totals, (layer_out, input_grad) = lax.scan(one_batch, zeros, (x_all, cot_all))
    grad_blocks = to_blocks(totals[0])
    slot_grads = jnp.zeros_like(grad_blocks).at[owner_list].set(grad_blocks)
    vec_grad = totals[1]
    highest = lax.Precision.HIGHEST
    rotated = jnp.einsum('sji,sjk->sik', left_sq, slot_grads, precision=highest)
    rotated = jnp.einsum('sik,skl->sil', rotated, right_sq, precision=highest)
    new_one = beta_one * moment_one_sq + (1.0 - beta_one) * rotated
    new_two = beta_two * moment_two_sq + (1.0 - beta_two) * rotated * rotated
    fix_one = 1.0 - beta_one ** step_count
    fix_two = 1.0 - beta_two ** step_count
    normal_step = new_one / fix_one / (jnp.sqrt(new_two / fix_two) + adam_eps)
    restored = jnp.einsum('sij,sjk->sik', left_sq, normal_step, precision=highest)
    restored = jnp.einsum('sik,slk->sil', restored, right_sq, precision=highest)
    new_masters = masters_sq - matrix_rate * (restored + decay_rate * masters_sq)
    vec_one = beta_one * vec_moment_one + (1.0 - beta_one) * vec_grad
    vec_two = beta_two * vec_moment_two + (1.0 - beta_two) * vec_grad * vec_grad
    new_vectors = vectors - vector_rate * (vec_one / fix_one) / (jnp.sqrt(vec_two / fix_two) + adam_eps)
    flat = (NBLK, BLK * BLK)
    new_masters = new_masters.reshape(flat)
    return (layer_out.reshape(SEQS, L, D), input_grad.reshape(SEQS, L, D), new_one.reshape(flat), new_two.reshape(flat), new_masters, new_masters.astype(jnp.bfloat16), new_vectors, vec_one, vec_two)
```

```python
import functools
import jax
import jax.numpy as jnp
from jax import lax
from jax.experimental import pallas as pl
from jax.experimental.pallas import tpu as pltpu
from jax.sharding import PartitionSpec as P

HEADS = 12
HDIM = 64
BLK = 192
LANE = 128
HALF = BLK // 2
PACK = BLK * BLK // LANE
GROUP = 8

norm_eps = 1e-05
beta_one = 0.95
beta_two = 0.95
adam_eps = 1e-08
matrix_rate = 0.02
vector_rate = 0.2
decay_rate = 0.01
step_count = 6
fix_one = 1.0 - beta_one**step_count
fix_two = 1.0 - beta_two**step_count
bf16 = jnp.bfloat16
f32 = jnp.float32


def params(**kw):
    return pltpu.CompilerParams(vmem_limit_bytes=56 * 2**20, **kw)


def low_lanes(rows):
    return lax.broadcasted_iota(jnp.int32, (rows, LANE), 1) < HDIM


def swap(value):
    return pltpu.roll(value, HDIM, 1)


def row_view(array):
    count = array.shape[0]
    padded = -count % GROUP
    if padded:
        array = jnp.pad(array, ((0, padded), (0, 0)))
    groups = (count + padded) // GROUP
    return (
        array.reshape(groups, GROUP, PACK, LANE)
        .transpose(0, 2, 1, 3)
        .reshape(groups, GROUP * PACK, LANE)
    )


def row_unview(array, count):
    groups = array.shape[0]
    return (
        array.reshape(groups, PACK, GROUP, LANE)
        .transpose(0, 2, 1, 3)
        .reshape(groups * GROUP, PACK * LANE)[:count]
    )


def triple(ref, row):
    return [ref[0, pl.ds(row + GROUP * part, HALF, stride=3 * GROUP), :] for part in range(3)]


def put_triple(ref, row, pieces):
    for part, piece in enumerate(pieces):
        ref[0, pl.ds(row + GROUP * part, HALF, stride=3 * GROUP), :] = piece


def to_square(pieces, main_ref, tail_ref):
    first, second, third = pieces
    low = low_lanes(HALF)
    second_s, third_s = swap(second), swap(third)
    main_ref[pl.ds(0, HALF, stride=2), :] = first
    main_ref[pl.ds(1, HALF, stride=2), :] = jnp.where(low, second_s, third_s)
    tail_ref[pl.ds(0, HALF, stride=2), :] = second
    tail_ref[pl.ds(1, HALF, stride=2), :] = third_s


def from_square(main_ref, tail_ref):
    low = low_lanes(HALF)
    even_main = main_ref[pl.ds(0, HALF, stride=2), :]
    odd_main = swap(main_ref[pl.ds(1, HALF, stride=2), :])
    even_tail = tail_ref[pl.ds(0, HALF, stride=2), :]
    odd_tail = swap(tail_ref[pl.ds(1, HALF, stride=2), :])
    return [even_main, jnp.where(low, even_tail, odd_main), jnp.where(low, odd_main, odd_tail)]


def pack_kernel(src_ref, out_ref, main_ref, tail_ref):
    low = low_lanes(HALF)
    for row in range(GROUP):
        spot = row % 2
        main, tail = main_ref.at[spot], tail_ref.at[spot]
        to_square(triple(src_ref, row), main, tail)
        out_ref[row, 0:BLK, :] = main[...].astype(bf16)
        out_ref[row, BLK:PACK, :] = jnp.where(
            low, tail[0:HALF, :], swap(tail[HALF:BLK, :])
        ).astype(bf16)


def pack_blocks(view):
    groups = view.shape[0]
    return pl.pallas_call(
        pack_kernel,
        grid=(groups,),
        in_specs=[pl.BlockSpec((1, GROUP * PACK, LANE), lambda i: (i, 0, 0))],
        out_specs=pl.BlockSpec((GROUP, PACK, LANE), lambda i: (i, 0, 0)),
        out_shape=jax.ShapeDtypeStruct((groups * GROUP, PACK, LANE), bf16),
        scratch_shapes=[pltpu.VMEM((2, BLK, LANE), f32), pltpu.VMEM((2, BLK, LANE), f32)],
        compiler_params=params(),
        name="pack",
    )(view)


def unfold(block):
    fold = block[BLK:PACK, :]
    return block[0:BLK, :], jnp.concatenate([fold[:, :HDIM], fold[:, HDIM:]], axis=0)


def assemble_kernel(cells, owner_ref, *refs):
    out_ref = refs[-1]
    for number, (row, lanes) in enumerate(cells):
        main_a, tail_a = unfold(refs[2 * number][0])
        main_b, tail_b = unfold(refs[2 * number + 1][0])
        rows = pl.ds(row, BLK)
        out_ref[rows, pl.ds(lanes[0], LANE)] = main_a
        out_ref[rows, pl.ds(lanes[1], LANE)] = jnp.concatenate([tail_a, main_b[:, :HDIM]], axis=1)
        out_ref[rows, pl.ds(lanes[2], LANE)] = jnp.concatenate([main_b[:, HDIM:], tail_b], axis=1)


def assemble(gathered, owner_list, shape, tile, cells, block_of):
    grid = (shape[0] // tile[0], shape[1] // tile[1])
    count = 2 * len(cells)

    def spec(which):
        return pl.BlockSpec(
            (1, PACK, LANE), lambda i, j, owner: (owner[block_of(i, j, which)], 0, 0)
        )

    return pl.pallas_call(
        functools.partial(assemble_kernel, cells),
        grid_spec=pltpu.PrefetchScalarGridSpec(
            num_scalar_prefetch=1,
            grid=grid,
            in_specs=[spec(which) for which in range(count)],
            out_specs=pl.BlockSpec(tile, lambda i, j, owner: (i, j)),
        ),
        out_shape=jax.ShapeDtypeStruct(shape, bf16),
        compiler_params=params(),
        name="assemble",
    )(owner_list, *([gathered] * count))


def layer_weights(gathered, owner_list, base, width, inner):
    cols = width // BLK
    inner_cols = inner // BLK
    square = cols * cols
    cells = []
    for matrix in range(3):
        for pair in range(cols // 2):
            cells.append((0, [3 * LANE * (3 * pair + part) + LANE * matrix for part in range(3)]))
    per_matrix = cols

    def block_qkv(i, j, which):
        return base + (which // per_matrix) * square + i * cols + which % per_matrix

    w_qkv = assemble(gathered, owner_list, (width, 3 * width), (BLK, 3 * width), cells, block_qkv)
    plain = []
    for row in range(2):
        for pair in range(cols // 2):
            plain.append(
                (row * BLK, [2 * BLK * pair + LANE * part for part in range(3)])
            )

    def block_plain(start, row_blocks):
        def block(i, j, which):
            return start + (2 * i + which // cols) * row_blocks + cols * j + which % cols

        return block

    tile = (2 * BLK, width)
    w_out = assemble(
        gathered, owner_list, (width, width), tile, plain, block_plain(base + 3 * square, cols)
    )
    up_base = base + 4 * square
    w_up = assemble(
        gathered, owner_list, (width, inner), tile, plain, block_plain(up_base, inner_cols)
    )
    down_base = up_base + cols * inner_cols
    w_down = assemble(
        gathered, owner_list, (inner, width), tile, plain, block_plain(down_base, cols)
    )
    return w_qkv, w_out, w_up, w_down
def dot(left, right, left_dim=1, right_dim=0):
    return lax.dot_general(
        left, right, (((left_dim,), (right_dim,)), ((), ())), preferred_element_type=f32
    )


def head_masks():
    lane = lax.broadcasted_iota(jnp.int32, (1, LANE), 1)
    first = (lane < HDIM).astype(f32)
    return [first.astype(bf16), (1.0 - first).astype(bf16)]


def attend_kernel(scale, qkv_ref, mix_ref, lse_ref):
    length = qkv_ref.shape[0]
    query, keys, values = (qkv_ref[:, pl.ds(LANE * part, LANE)] for part in range(3))
    mixed, logs = [], []
    for mask in head_masks():
        scores = dot(query * mask, keys, 1, 1) * scale
        highest = jnp.max(scores, axis=1, keepdims=True)
        raised = jnp.exp(scores - highest)
        total = jnp.sum(raised, axis=1, keepdims=True)
        probs = raised * (1.0 / total)
        mixed.append(dot(probs.astype(bf16), values))
        logs.append(highest + jnp.log(total))
    low = low_lanes(length)
    mix_ref[...] = jnp.where(low, mixed[0], mixed[1]).astype(bf16)
    lse_ref[...] = jnp.where(low, logs[0], logs[1])


def attend(qkv, scale):
    length, wide = qkv.shape
    pairs = wide // (3 * LANE)
    return pl.pallas_call(
        functools.partial(attend_kernel, scale),
        grid=(pairs,),
        in_specs=[pl.BlockSpec((length, 3 * LANE), lambda i: (0, i))],
        out_specs=[pl.BlockSpec((length, LANE), lambda i: (0, i))] * 2,
        out_shape=[
            jax.ShapeDtypeStruct((length, wide // 3), bf16),
            jax.ShapeDtypeStruct((length, wide // 3), f32),
        ],
        compiler_params=params(),
        name="attend",
    )(qkv)


def attend_back_kernel(scale, qkv_ref, lse_ref, grad_ref, out_ref):
    length = qkv_ref.shape[0]
    query, keys, values = (qkv_ref[:, pl.ds(LANE * part, LANE)] for part in range(3))
    grad = grad_ref[...]
    parts = []
    for number, mask in enumerate(head_masks()):
        scores = dot(query * mask, keys, 1, 1) * scale
        probs = jnp.exp(scores - lse_ref[:, number * HDIM : number * HDIM + 1])
        grad_probs = dot(grad * mask, values, 1, 1)
        centre = jnp.sum(probs * grad_probs, axis=1, keepdims=True)
        grad_scores = (probs * (grad_probs - centre)).astype(bf16)
        parts.append(
            (
                dot(grad_scores, keys) * scale,
                dot(grad_scores, query, 0, 0) * scale,
                dot(probs.astype(bf16), grad, 0, 0),
            )
        )
    low = low_lanes(length)
    for part in range(3):
        out_ref[:, pl.ds(LANE * part, LANE)] = jnp.where(
            low, parts[0][part], parts[1][part]
        ).astype(bf16)


def attend_back(qkv, lse, grad, scale):
    length, wide = qkv.shape
    pairs = wide // (3 * LANE)
    return pl.pallas_call(
        functools.partial(attend_back_kernel, scale),
        grid=(pairs,),
        in_specs=[
            pl.BlockSpec((length, 3 * LANE), lambda i: (0, i)),
            pl.BlockSpec((length, LANE), lambda i: (0, i)),
            pl.BlockSpec((length, LANE), lambda i: (0, i)),
        ],
        out_specs=pl.BlockSpec((length, 3 * LANE), lambda i: (0, i)),
        out_shape=jax.ShapeDtypeStruct((length, wide), bf16),
        compiler_params=params(),
        name="attend_back",
    )(qkv, lse, grad)


def weight_grad_kernel(lanes_of, block_of, panel, steps, rows_ref, left_ref, right_ref, *refs):
    out_ref, stage_ref, sems = refs[-3:]
    i, j = pl.program_id(0), pl.program_id(1)
    step = i * pl.num_programs(1) + j
    spot = lax.rem(step, 2)
    pairs = panel // (2 * BLK)
    count = 4 * pairs

    def copy(which, slot, row):
        return pltpu.make_async_copy(
            stage_ref.at[slot, which], out_ref.at[row], sems.at[slot, which]
        )

    @pl.when(step >= 2)
    def _():
        for which in range(count):
            copy(which, spot, 0).wait()

    left = left_ref[:, pl.ds(pl.multiple_of(2 * BLK * i, LANE), 2 * BLK)]
    low_top, low_all = low_lanes(HALF), low_lanes(BLK)
    for pair in range(pairs):
        right = jnp.concatenate(
            [
                right_ref[:, pl.ds(pl.multiple_of(lanes_of(j, 3 * pair + part), LANE), LANE)]
                for part in range(3)
            ],
            axis=1,
        )
        product = dot(left, right, 0, 0)
        for half in range(2):
            tile = product[half * BLK : (half + 1) * BLK, :]
            first, second, third = (tile[:, LANE * part : LANE * (part + 1)] for part in range(3))
            which = half * 2 * pairs + 2 * pair
            stage_ref[spot, which, 0:BLK, :] = first.astype(bf16)
            stage_ref[spot, which, BLK:PACK, :] = jnp.where(
                low_top, second[0:HALF, :], swap(second[HALF:BLK, :])
            ).astype(bf16)
            stage_ref[spot, which + 1, 0:BLK, :] = swap(
                jnp.where(low_all, third, second)
            ).astype(bf16)
            stage_ref[spot, which + 1, BLK:PACK, :] = jnp.where(
                low_top, swap(third[0:HALF, :]), third[HALF:BLK, :]
            ).astype(bf16)
    for which in range(count):
        block = block_of(i, j, which // (2 * pairs), which % (2 * pairs))
        copy(which, spot, rows_ref[block]).start()

    @pl.when(step == steps - 1)
    def _():
        for which in range(count):
            copy(which, spot, 0).wait()
            if steps > 1:
                copy(which, 1 - spot, 0).wait()


def weight_grad(slots, slot_shape, rows, left, right, grid, panel, lanes_of, block_of):
    steps = grid[0] * grid[1]
    count = 4 * (panel // (2 * BLK))
    whole = [pl.BlockSpec(left.shape, lambda i, j, s: (0, 0)), pl.BlockSpec(right.shape, lambda i, j, s: (0, 0))]
    extra, aliases = [], {}
    if slots is not None:
        extra = [slots]
        aliases = {3: 0}
    return pl.pallas_call(
        functools.partial(weight_grad_kernel, lanes_of, block_of, panel, steps),
        grid_spec=pltpu.PrefetchScalarGridSpec(
            num_scalar_prefetch=1,
            grid=grid,
            in_specs=whole + [pl.BlockSpec(memory_space=pl.ANY)] * len(extra),
            out_specs=pl.BlockSpec(memory_space=pl.ANY),
            scratch_shapes=[
                pltpu.VMEM((2, count, PACK, LANE), bf16),
                pltpu.SemaphoreType.DMA((2, count)),
            ],
        ),
        out_shape=jax.ShapeDtypeStruct(slot_shape, bf16),
        input_output_aliases=aliases,
        compiler_params=params(),
        name="weight_grad",
    )(rows, left, right, *extra)


def plain_grad(slots, slot_shape, rows, left, right, base, width):
    cols = right.shape[1] // BLK
    per = width // BLK
    return weight_grad(
        slots,
        slot_shape,
        rows,
        left,
        right,
        (left.shape[1] // (2 * BLK), right.shape[1] // width),
        width,
        lambda j, piece: j * width + piece * LANE,
        lambda i, j, half, col: base + (2 * i + half) * cols + j * per + col,
    )


def qkv_grad(slots, slot_shape, rows, left, right, base, width):
    per = width // BLK
    return weight_grad(
        slots,
        slot_shape,
        rows,
        left,
        right,
        (width // (2 * BLK), 3),
        width,
        lambda j, piece: 3 * LANE * piece + LANE * j,
        lambda i, j, half, col: base + j * per * per + (2 * i + half) * per + col,
    )


def soap_kernel(
    masters_ref, one_ref, two_ref, left_ref, right_ref, grad_ref,
    one_out, two_out, masters_out, copies_out, left_sq, right_sq, work, full,
):
    def square(refs):
        return jnp.concatenate([refs[0][...], refs[1][:, :HDIM]], axis=1).astype(bf16)

    def keep(refs, value):
        refs[0][...] = value[:, :LANE]
        refs[1][:, :HDIM] = value[:, LANE:]

    for row in range(GROUP):
        spot = row % 2
        left_refs = [left_sq.at[spot, 0], left_sq.at[spot, 1]]
        right_refs = [right_sq.at[spot, 0], right_sq.at[spot, 1]]
        refs = [work.at[spot, 0], work.at[spot, 1]]
        to_square(triple(left_ref, row), *left_refs)
        to_square(triple(right_ref, row), *right_refs)
        left, right = square(left_refs), square(right_refs)
        main, tail = unfold(grad_ref[row])
        grad = jnp.concatenate([main, tail], axis=1)
        rotated = dot(dot(left, grad, 0, 0).astype(bf16), right)
        keep(refs, rotated)
        pieces = from_square(*refs)
        ones, twos = triple(one_ref, row), triple(two_ref, row)
        ones = [beta_one * old + (1.0 - beta_one) * new for old, new in zip(ones, pieces)]
        twos = [beta_two * old + (1.0 - beta_two) * new * new for old, new in zip(twos, pieces)]
        put_triple(one_out, row, ones)
        put_triple(two_out, row, twos)
        moves = [
            (one / fix_one) / (jnp.sqrt(two / fix_two) + adam_eps) for one, two in zip(ones, twos)
        ]
        to_square(moves, *refs)
        restored = dot(dot(left, square(refs)).astype(bf16), right, 1, 1)
        keep(refs, restored)
        pieces = from_square(*refs)
        old = triple(masters_ref, row)
        new = [
            value - matrix_rate * (step + decay_rate * value) for value, step in zip(old, pieces)
        ]
        put_triple(masters_out, row, new)
        put_triple(full, row, new)
    copies_out[0] = full[0].astype(bf16)


def soap(views, grads):
    groups = views[0].shape[0]
    view_spec = pl.BlockSpec((1, GROUP * PACK, LANE), lambda i: (i, 0, 0))
    shape = (groups, GROUP * PACK, LANE)
    square = pltpu.VMEM((2, 2, BLK, LANE), f32)
    return pl.pallas_call(
        soap_kernel,
        grid=(groups,),
        in_specs=[view_spec] * 5 + [pl.BlockSpec((GROUP, PACK, LANE), lambda i: (i, 0, 0))],
        out_specs=[view_spec] * 4,
        out_shape=[jax.ShapeDtypeStruct(shape, f32)] * 3 + [jax.ShapeDtypeStruct(shape, bf16)],
        scratch_shapes=[square, square, square, pltpu.VMEM((1, GROUP * PACK, LANE), f32)],
        compiler_params=params(),
        name="soap",
    )(*views, grads)


def norm_forward(hidden, gain, shift):
    center = hidden - jnp.mean(hidden, axis=-1, keepdims=True)
    spread = jnp.mean(center * center, axis=-1, keepdims=True)
    inverse = lax.rsqrt(spread + norm_eps)
    unit = center * inverse
    return (unit * gain + shift, unit, inverse)


def norm_backward(incoming, unit, inverse, gain):
    scaled = incoming * gain
    grad_hidden = inverse * (
        scaled
        - jnp.mean(scaled, axis=-1, keepdims=True)
        - unit * jnp.mean(scaled * unit, axis=-1, keepdims=True)
    )
    return (grad_hidden, jnp.sum(incoming * unit, axis=0), jnp.sum(incoming, axis=0))


def gelu_exact(value):
    return jax.nn.gelu(value, approximate=False)


def unpack(vector, width):
    return [vector[number * width : (number + 1) * width] for number in range(8)] + [
        vector[8 * width :]
    ]


def forward_layer(hidden, matrices, pieces, scale):
    w_qkv, w_out, w_up, w_down = matrices
    bias_q, bias_v, bias_out, bias_down, gain_one, shift_one, gain_two, shift_two, bias_up = pieces
    hid_low = hidden.astype(bf16)
    bias_q = bias_q.reshape(-1, LANE)
    bias_qkv = jnp.stack([bias_q, jnp.zeros_like(bias_q), bias_v.reshape(-1, LANE)], axis=1)
    qkv = (dot(hid_low, w_qkv) + bias_qkv.reshape(-1)).astype(bf16)
    mixed, lse = attend(qkv, scale)
    branch = dot(mixed, w_out) + bias_out
    normed, unit_one, inv_one = norm_forward(hidden + branch, gain_one, shift_one)
    norm_low = normed.astype(bf16)
    pre_act = dot(norm_low, w_up) + bias_up
    act_low = gelu_exact(pre_act).astype(bf16)
    down = dot(act_low, w_down) + bias_down
    result, unit_two, inv_two = norm_forward(normed + down, gain_two, shift_two)
    kept = (
        hid_low, qkv, lse, mixed, unit_one, inv_one, norm_low, pre_act, act_low, unit_two, inv_two
    )
    return (result, kept)


def backward_layer(incoming, matrices, pieces, kept, scale, slots, slot_shape, rows, base):
    w_qkv, w_out, w_up, w_down = matrices
    gain_one, gain_two = pieces[4], pieces[6]
    hid_low, qkv, lse, mixed, unit_one, inv_one, norm_low, pre_act, act_low, unit_two, inv_two = kept
    width = mixed.shape[1]
    square = (width // BLK) ** 2
    up_count = act_low.shape[1] // BLK * (width // BLK)
    grad_two, gain_two_g, shift_two_g = norm_backward(incoming, unit_two, inv_two, gain_two)
    down_low = grad_two.astype(bf16)
    slots = plain_grad(
        slots, slot_shape, rows, act_low, down_low, base + 4 * square + up_count, width
    )
    grad_act = dot(down_low, w_down, 1, 1)
    (grad_pre,) = jax.vjp(gelu_exact, pre_act)[1](grad_act)
    up_low = grad_pre.astype(bf16)
    slots = plain_grad(slots, slot_shape, rows, norm_low, up_low, base + 4 * square, width)
    grad_norm = grad_two + dot(up_low, w_up, 1, 1)
    grad_one, gain_one_g, shift_one_g = norm_backward(grad_norm, unit_one, inv_one, gain_one)
    out_low = grad_one.astype(bf16)
    slots = plain_grad(slots, slot_shape, rows, mixed, out_low, base + 3 * square, width)
    grad_mix = dot(out_low, w_out, 1, 1).astype(bf16)
    grad_qkv = attend_back(qkv, lse, grad_mix, scale)
    slots = qkv_grad(slots, slot_shape, rows, hid_low, grad_qkv, base, width)
    grad_hidden = grad_one + dot(grad_qkv, w_qkv, 1, 1)

    def total(array):
        return jnp.sum(array, axis=0, dtype=f32)

    bias_qkv = total(grad_qkv).reshape(-1, 3, LANE)
    vec_grad = jnp.concatenate(
        [
            bias_qkv[:, 0].reshape(-1),
            bias_qkv[:, 2].reshape(-1),
            total(out_low),
            total(down_low),
            gain_one_g,
            shift_one_g,
            gain_two_g,
            shift_two_g,
            total(up_low),
        ]
    )
    return grad_hidden, slots, vec_grad


def swap_in(array):
    return lax.all_to_all(array, "seq", split_axis=0, concat_axis=1, tiled=True)


def swap_out(array):
    return lax.all_to_all(array, "seq", split_axis=1, concat_axis=0, tiled=True)


def local(
    tokens,
    cotangent,
    tok_weight,
    mask_count,
    owner_list,
    masters,
    moment_one,
    moment_two,
    left_basis,
    right_basis,
    vectors,
    vec_moment_one,
    vec_moment_two,
):
    data_parts = lax.axis_size("dp")
    seq_count, local_len, width = tokens.shape
    layer_count = vectors.shape[0]
    inner = vectors.shape[-1] - 8 * width
    owned_count = masters.shape[0]
    block_total = owner_list.shape[0]
    scale = HDIM ** (-0.5)

    master_view = row_view(masters)
    packed = pack_blocks(master_view)[:owned_count]
    gathered = lax.all_gather(packed, "dp", axis=0, tiled=True)

    positions = lax.axis_index("seq") * local_len + jnp.arange(local_len, dtype=jnp.int32)
    masked = (positions[None, :] < mask_count[:, None]).astype(f32)
    factor = tok_weight.astype(f32) * (1.0 + masked) * 0.25
    hidden = swap_in(tokens)
    per_seq = hidden.shape[0]
    full_len = hidden.shape[1]
    hidden = hidden.reshape(full_len, width).astype(f32)
    incoming = swap_in(cotangent).reshape(full_len, width).astype(f32)
    incoming = incoming * swap_in(factor).reshape(full_len, 1)

    per_layer = block_total // layer_count
    weights = [
        layer_weights(gathered, owner_list, per_layer * number, width, inner)
        for number in range(layer_count)
    ]
    saved = []
    for number in range(layer_count):
        hidden, kept = forward_layer(
            hidden, weights[number], unpack(vectors[number], width), scale
        )
        saved.append(kept)
    layer_out = swap_out(hidden.astype(bf16).reshape(per_seq, full_len, width))

    chunk = owned_count + 1
    rows = owner_list + owner_list // owned_count
    slot_shape = (data_parts * chunk, PACK, LANE)
    slots = None
    vec_grads = [None] * layer_count
    for number in reversed(range(layer_count)):
        incoming, slots, vec_grads[number] = backward_layer(
            incoming,
            weights[number],
            unpack(vectors[number], width),
            saved[number],
            scale,
            slots,
            slot_shape,
            rows,
            per_layer * number,
        )
    vec_grad = jnp.stack(vec_grads)
    vec_high = vec_grad.astype(bf16)
    vec_low = (vec_grad - vec_high.astype(f32)).astype(bf16)
    vec_slot = jnp.concatenate([vec_high.reshape(-1, LANE), vec_low.reshape(-1, LANE)], axis=0)
    for part in range(data_parts):
        slots = lax.dynamic_update_slice(
            slots, vec_slot[None], (part * chunk + owned_count, 0, 0)
        )
    owned = lax.psum_scatter(slots, "dp", scatter_dimension=0, tiled=True)
    owned = lax.psum(owned, "seq")
    input_grad = swap_out(incoming.reshape(per_seq, full_len, width))

    vec_rows = owned[owned_count].astype(f32)
    half = PACK // 2
    vec_total = (vec_rows[:half] + vec_rows[half:]).reshape(vectors.shape)
    views = [master_view] + [
        row_view(array) for array in (moment_one, moment_two, left_basis, right_basis)
    ]
    extra = views[0].shape[0] * GROUP - chunk
    if extra > 0:
        owned = jnp.pad(owned, ((0, extra), (0, 0), (0, 0)))
    new_one, new_two, new_masters, copies = [
        row_unview(array, owned_count) for array in soap(views, owned)
    ]
    vec_one = beta_one * vec_moment_one + (1.0 - beta_one) * vec_total
    vec_two = beta_two * vec_moment_two + (1.0 - beta_two) * vec_total * vec_total
    new_vectors = vectors - vector_rate * (vec_one / fix_one) / (
        jnp.sqrt(vec_two / fix_two) + adam_eps
    )
    return (
        layer_out, input_grad, new_one, new_two, new_masters, copies, new_vectors, vec_one, vec_two
    )


def solution(mesh):
    rows = P("dp", None)
    tokens = P("dp", "seq", None)
    return jax.shard_map(
        local,
        mesh=mesh,
        in_specs=(tokens, tokens, P("dp", "seq"), P("dp"), P()) + (rows,) * 5 + (P(),) * 3,
        out_specs=(tokens, tokens) + (rows,) * 4 + (P(),) * 3,
        check_vma=False,
    )
```

```python
import functools
import math
import jax
import jax.numpy as jnp
from jax import lax
from jax.experimental import pallas as pl
from jax.experimental.pallas import tpu as pltpu
from jax.sharding import PartitionSpec as P

HEADS = 12
HDIM = 64
BLK = 192
LANE = 128
HALF = BLK // 2
PACK = BLK * BLK // LANE
GROUP = 8
GATHER_ROWS = 144
GATHER_LAG = 2
REDUCE_ROWS = 144
REDUCE_LAG = 2
WAIT_BYTES = 3 * 10**8

norm_eps = 1e-05
beta_one = 0.95
beta_two = 0.95
adam_eps = 1e-08
matrix_rate = 0.02
vector_rate = 0.2
decay_rate = 0.01
step_count = 6
fix_one = 1.0 - beta_one**step_count
fix_two = 1.0 - beta_two**step_count
bf16 = jnp.bfloat16
f32 = jnp.float32


def params(**kw):
    return pltpu.CompilerParams(vmem_limit_bytes=56 * 2**20, **kw)


def low_lanes(rows):
    return lax.broadcasted_iota(jnp.int32, (rows, LANE), 1) < HDIM


def swap(value):
    return pltpu.roll(value, HDIM, 1)


def row_view(array):
    count = array.shape[0]
    padded = -count % GROUP
    if padded:
        array = jnp.pad(array, ((0, padded), (0, 0)))
    groups = (count + padded) // GROUP
    return (
        array.reshape(groups, GROUP, PACK, LANE)
        .transpose(0, 2, 1, 3)
        .reshape(groups, GROUP * PACK, LANE)
    )


def row_unview(array, count):
    groups = array.shape[0]
    return (
        array.reshape(groups, PACK, GROUP, LANE)
        .transpose(0, 2, 1, 3)
        .reshape(groups * GROUP, PACK * LANE)[:count]
    )


def triple(ref, row):
    return [ref[0, pl.ds(row + GROUP * part, HALF, stride=3 * GROUP), :] for part in range(3)]


def put_triple(ref, row, pieces):
    for part, piece in enumerate(pieces):
        ref[0, pl.ds(row + GROUP * part, HALF, stride=3 * GROUP), :] = piece


def to_square(pieces, main_ref, tail_ref):
    first, second, third = pieces
    low = low_lanes(HALF)
    second_s, third_s = swap(second), swap(third)
    main_ref[pl.ds(0, HALF, stride=2), :] = first
    main_ref[pl.ds(1, HALF, stride=2), :] = jnp.where(low, second_s, third_s)
    tail_ref[pl.ds(0, HALF, stride=2), :] = second
    tail_ref[pl.ds(1, HALF, stride=2), :] = third_s


def from_square(main_ref, tail_ref):
    low = low_lanes(HALF)
    even_main = main_ref[pl.ds(0, HALF, stride=2), :]
    odd_main = swap(main_ref[pl.ds(1, HALF, stride=2), :])
    even_tail = tail_ref[pl.ds(0, HALF, stride=2), :]
    odd_tail = swap(tail_ref[pl.ds(1, HALF, stride=2), :])
    return [even_main, jnp.where(low, even_tail, odd_main), jnp.where(low, odd_main, odd_tail)]


def pack_kernel(src_ref, out_ref, main_ref, tail_ref):
    low = low_lanes(HALF)
    for row in range(GROUP):
        spot = row % 2
        main, tail = main_ref.at[spot], tail_ref.at[spot]
        to_square(triple(src_ref, row), main, tail)
        out_ref[row, 0:BLK, :] = main[...].astype(bf16)
        out_ref[row, BLK:PACK, :] = jnp.where(
            low, tail[0:HALF, :], swap(tail[HALF:BLK, :])
        ).astype(bf16)


def pack_blocks(view):
    groups = view.shape[0]
    return pl.pallas_call(
        pack_kernel,
        grid=(groups,),
        in_specs=[pl.BlockSpec((1, GROUP * PACK, LANE), lambda i: (i, 0, 0))],
        out_specs=pl.BlockSpec((GROUP, PACK, LANE), lambda i: (i, 0, 0)),
        out_shape=jax.ShapeDtypeStruct((groups * GROUP, PACK, LANE), bf16),
        scratch_shapes=[pltpu.VMEM((2, BLK, LANE), f32), pltpu.VMEM((2, BLK, LANE), f32)],
        compiler_params=params(),
        name="pack",
    )(view)


def unfold(block):
    fold = block[BLK:PACK, :]
    return block[0:BLK, :], jnp.concatenate([fold[:, :HDIM], fold[:, HDIM:]], axis=0)


def assemble_kernel(cells, owner_ref, *refs):
    out_ref = refs[-1]
    for number, (row, lanes) in enumerate(cells):
        main_a, tail_a = unfold(refs[2 * number][0])
        main_b, tail_b = unfold(refs[2 * number + 1][0])
        rows = pl.ds(row, BLK)
        out_ref[rows, pl.ds(lanes[0], LANE)] = main_a
        out_ref[rows, pl.ds(lanes[1], LANE)] = jnp.concatenate([tail_a, main_b[:, :HDIM]], axis=1)
        out_ref[rows, pl.ds(lanes[2], LANE)] = jnp.concatenate([main_b[:, HDIM:], tail_b], axis=1)


def assemble(gathered, owner_list, shape, tile, cells, block_of):
    grid = (shape[0] // tile[0], shape[1] // tile[1])
    count = 2 * len(cells)

    def spec(which):
        return pl.BlockSpec(
            (1, PACK, LANE), lambda i, j, owner: (owner[block_of(i, j, which)], 0, 0)
        )

    return pl.pallas_call(
        functools.partial(assemble_kernel, cells),
        grid_spec=pltpu.PrefetchScalarGridSpec(
            num_scalar_prefetch=1,
            grid=grid,
            in_specs=[spec(which) for which in range(count)],
            out_specs=pl.BlockSpec(tile, lambda i, j, owner: (i, j)),
        ),
        out_shape=jax.ShapeDtypeStruct(shape, bf16),
        compiler_params=params(),
        name="assemble",
    )(owner_list, *([gathered] * count))


def layer_weights(gathered, owner_list, base, width, inner):
    cols = width // BLK
    inner_cols = inner // BLK
    square = cols * cols
    cells = []
    for matrix in range(3):
        for pair in range(cols // 2):
            cells.append((0, [3 * LANE * (3 * pair + part) + LANE * matrix for part in range(3)]))
    per_matrix = cols

    def block_qkv(i, j, which):
        return base + (which // per_matrix) * square + i * cols + which % per_matrix

    w_qkv = assemble(gathered, owner_list, (width, 3 * width), (BLK, 3 * width), cells, block_qkv)
    plain = []
    for row in range(2):
        for pair in range(cols // 2):
            plain.append(
                (row * BLK, [2 * BLK * pair + LANE * part for part in range(3)])
            )

    def block_plain(start, row_blocks):
        def block(i, j, which):
            return start + (2 * i + which // cols) * row_blocks + cols * j + which % cols

        return block

    tile = (2 * BLK, width)
    w_out = assemble(
        gathered, owner_list, (width, width), tile, plain, block_plain(base + 3 * square, cols)
    )
    up_base = base + 4 * square
    w_up = assemble(
        gathered, owner_list, (width, inner), tile, plain, block_plain(up_base, inner_cols)
    )
    down_base = up_base + cols * inner_cols
    w_down = assemble(
        gathered, owner_list, (inner, width), tile, plain, block_plain(down_base, cols)
    )
    return w_qkv, w_out, w_up, w_down
def dot(left, right, left_dim=1, right_dim=0):
    return lax.dot_general(
        left, right, (((left_dim,), (right_dim,)), ((), ())), preferred_element_type=f32
    )


def head_masks():
    lane = lax.broadcasted_iota(jnp.int32, (1, LANE), 1)
    first = (lane < HDIM).astype(f32)
    return [first.astype(bf16), (1.0 - first).astype(bf16)]


def attend_kernel(scale, qkv_ref, mix_ref, lse_ref):
    length = qkv_ref.shape[0]
    query, keys, values = (qkv_ref[:, pl.ds(LANE * part, LANE)] for part in range(3))
    mixed, logs = [], []
    for mask in head_masks():
        scores = dot(query * mask, keys, 1, 1) * scale
        highest = jnp.max(scores, axis=1, keepdims=True)
        raised = jnp.exp(scores - highest)
        total = jnp.sum(raised, axis=1, keepdims=True)
        probs = raised * (1.0 / total)
        mixed.append(dot(probs.astype(bf16), values))
        logs.append(highest + jnp.log(total))
    low = low_lanes(length)
    mix_ref[...] = jnp.where(low, mixed[0], mixed[1]).astype(bf16)
    lse_ref[...] = jnp.where(low, logs[0], logs[1])


def attend(qkv, scale):
    length, wide = qkv.shape
    pairs = wide // (3 * LANE)
    return pl.pallas_call(
        functools.partial(attend_kernel, scale),
        grid=(pairs,),
        in_specs=[pl.BlockSpec((length, 3 * LANE), lambda i: (0, i))],
        out_specs=[pl.BlockSpec((length, LANE), lambda i: (0, i))] * 2,
        out_shape=[
            jax.ShapeDtypeStruct((length, wide // 3), bf16),
            jax.ShapeDtypeStruct((length, wide // 3), f32),
        ],
        compiler_params=params(),
        name="attend",
    )(qkv)


def attend_back_kernel(scale, qkv_ref, lse_ref, grad_ref, out_ref):
    length = qkv_ref.shape[0]
    query, keys, values = (qkv_ref[:, pl.ds(LANE * part, LANE)] for part in range(3))
    grad = grad_ref[...]
    parts = []
    for number, mask in enumerate(head_masks()):
        scores = dot(query * mask, keys, 1, 1) * scale
        probs = jnp.exp(scores - lse_ref[:, number * HDIM : number * HDIM + 1])
        grad_probs = dot(grad * mask, values, 1, 1)
        centre = jnp.sum(probs * grad_probs, axis=1, keepdims=True)
        grad_scores = (probs * (grad_probs - centre)).astype(bf16)
        parts.append(
            (
                dot(grad_scores, keys) * scale,
                dot(grad_scores, query, 0, 0) * scale,
                dot(probs.astype(bf16), grad, 0, 0),
            )
        )
    low = low_lanes(length)
    for part in range(3):
        out_ref[:, pl.ds(LANE * part, LANE)] = jnp.where(
            low, parts[0][part], parts[1][part]
        ).astype(bf16)


def attend_back(qkv, lse, grad, scale):
    length, wide = qkv.shape
    pairs = wide // (3 * LANE)
    return pl.pallas_call(
        functools.partial(attend_back_kernel, scale),
        grid=(pairs,),
        in_specs=[
            pl.BlockSpec((length, 3 * LANE), lambda i: (0, i)),
            pl.BlockSpec((length, LANE), lambda i: (0, i)),
            pl.BlockSpec((length, LANE), lambda i: (0, i)),
        ],
        out_specs=pl.BlockSpec((length, 3 * LANE), lambda i: (0, i)),
        out_shape=jax.ShapeDtypeStruct((length, wide), bf16),
        compiler_params=params(),
        name="attend_back",
    )(qkv, lse, grad)


def weight_grad_kernel(lanes_of, block_of, panel, steps, rows_ref, left_ref, right_ref, *refs):
    out_ref, stage_ref, sems = refs[-3:]
    i, j = pl.program_id(0), pl.program_id(1)
    step = i * pl.num_programs(1) + j
    spot = lax.rem(step, 2)
    pairs = panel // (2 * BLK)
    count = 4 * pairs

    def copy(which, slot, row):
        return pltpu.make_async_copy(
            stage_ref.at[slot, which], out_ref.at[row], sems.at[slot, which]
        )

    @pl.when(step >= 2)
    def _():
        for which in range(count):
            copy(which, spot, 0).wait()

    left = left_ref[:, pl.ds(pl.multiple_of(2 * BLK * i, LANE), 2 * BLK)]
    low_top, low_all = low_lanes(HALF), low_lanes(BLK)
    for pair in range(pairs):
        right = jnp.concatenate(
            [
                right_ref[:, pl.ds(pl.multiple_of(lanes_of(j, 3 * pair + part), LANE), LANE)]
                for part in range(3)
            ],
            axis=1,
        )
        product = dot(left, right, 0, 0)
        for half in range(2):
            tile = product[half * BLK : (half + 1) * BLK, :]
            first, second, third = (tile[:, LANE * part : LANE * (part + 1)] for part in range(3))
            which = half * 2 * pairs + 2 * pair
            stage_ref[spot, which, 0:BLK, :] = first.astype(bf16)
            stage_ref[spot, which, BLK:PACK, :] = jnp.where(
                low_top, second[0:HALF, :], swap(second[HALF:BLK, :])
            ).astype(bf16)
            stage_ref[spot, which + 1, 0:BLK, :] = swap(
                jnp.where(low_all, third, second)
            ).astype(bf16)
            stage_ref[spot, which + 1, BLK:PACK, :] = jnp.where(
                low_top, swap(third[0:HALF, :]), third[HALF:BLK, :]
            ).astype(bf16)
    for which in range(count):
        block = block_of(i, j, which // (2 * pairs), which % (2 * pairs))
        copy(which, spot, rows_ref[block]).start()

    @pl.when(step == steps - 1)
    def _():
        for which in range(count):
            copy(which, spot, 0).wait()
            if steps > 1:
                copy(which, 1 - spot, 0).wait()


def weight_grad(slots, slot_shape, rows, left, right, grid, panel, lanes_of, block_of):
    steps = grid[0] * grid[1]
    count = 4 * (panel // (2 * BLK))
    whole = [pl.BlockSpec(left.shape, lambda i, j, s: (0, 0)), pl.BlockSpec(right.shape, lambda i, j, s: (0, 0))]
    extra, aliases = [], {}
    if slots is not None:
        extra = [slots]
        aliases = {3: 0}
    return pl.pallas_call(
        functools.partial(weight_grad_kernel, lanes_of, block_of, panel, steps),
        grid_spec=pltpu.PrefetchScalarGridSpec(
            num_scalar_prefetch=1,
            grid=grid,
            in_specs=whole + [pl.BlockSpec(memory_space=pl.ANY)] * len(extra),
            out_specs=pl.BlockSpec(memory_space=pl.ANY),
            scratch_shapes=[
                pltpu.VMEM((2, count, PACK, LANE), bf16),
                pltpu.SemaphoreType.DMA((2, count)),
            ],
        ),
        out_shape=jax.ShapeDtypeStruct(slot_shape, bf16),
        input_output_aliases=aliases,
        compiler_params=params(),
        name="weight_grad",
    )(rows, left, right, *extra)


def plain_grad(slots, slot_shape, rows, left, right, base, width):
    cols = right.shape[1] // BLK
    per = width // BLK
    return weight_grad(
        slots,
        slot_shape,
        rows,
        left,
        right,
        (left.shape[1] // (2 * BLK), right.shape[1] // width),
        width,
        lambda j, piece: j * width + piece * LANE,
        lambda i, j, half, col: base + (2 * i + half) * cols + j * per + col,
    )


def qkv_grad(slots, slot_shape, rows, left, right, base, width):
    per = width // BLK
    return weight_grad(
        slots,
        slot_shape,
        rows,
        left,
        right,
        (width // (2 * BLK), 3),
        width,
        lambda j, piece: 3 * LANE * piece + LANE * j,
        lambda i, j, half, col: base + j * per * per + (2 * i + half) * per + col,
    )


def soap_kernel(
    masters_ref, one_ref, two_ref, left_ref, right_ref, grad_ref,
    one_out, two_out, masters_out, copies_out, left_sq, right_sq, work, full,
):
    def square(refs):
        return jnp.concatenate([refs[0][...], refs[1][:, :HDIM]], axis=1).astype(bf16)

    def keep(refs, value):
        refs[0][...] = value[:, :LANE]
        refs[1][:, :HDIM] = value[:, LANE:]

    for row in range(GROUP):
        spot = row % 2
        left_refs = [left_sq.at[spot, 0], left_sq.at[spot, 1]]
        right_refs = [right_sq.at[spot, 0], right_sq.at[spot, 1]]
        refs = [work.at[spot, 0], work.at[spot, 1]]
        to_square(triple(left_ref, row), *left_refs)
        to_square(triple(right_ref, row), *right_refs)
        left, right = square(left_refs), square(right_refs)
        main, tail = unfold(grad_ref[row])
        grad = jnp.concatenate([main, tail], axis=1)
        rotated = dot(dot(left, grad, 0, 0).astype(bf16), right)
        keep(refs, rotated)
        pieces = from_square(*refs)
        ones, twos = triple(one_ref, row), triple(two_ref, row)
        ones = [beta_one * old + (1.0 - beta_one) * new for old, new in zip(ones, pieces)]
        twos = [beta_two * old + (1.0 - beta_two) * new * new for old, new in zip(twos, pieces)]
        put_triple(one_out, row, ones)
        put_triple(two_out, row, twos)
        moves = [
            (one / fix_one) / (jnp.sqrt(two / fix_two) + adam_eps) for one, two in zip(ones, twos)
        ]
        to_square(moves, *refs)
        restored = dot(dot(left, square(refs)).astype(bf16), right, 1, 1)
        keep(refs, restored)
        pieces = from_square(*refs)
        old = triple(masters_ref, row)
        new = [
            value - matrix_rate * (step + decay_rate * value) for value, step in zip(old, pieces)
        ]
        put_triple(masters_out, row, new)
        put_triple(full, row, new)
    copies_out[0] = full[0].astype(bf16)


def soap(views, grads):
    groups = views[0].shape[0]
    view_spec = pl.BlockSpec((1, GROUP * PACK, LANE), lambda i: (i, 0, 0))
    shape = (groups, GROUP * PACK, LANE)
    square = pltpu.VMEM((2, 2, BLK, LANE), f32)
    return pl.pallas_call(
        soap_kernel,
        grid=(groups,),
        in_specs=[view_spec] * 5 + [pl.BlockSpec((GROUP, PACK, LANE), lambda i: (i, 0, 0))],
        out_specs=[view_spec] * 4,
        out_shape=[jax.ShapeDtypeStruct(shape, f32)] * 3 + [jax.ShapeDtypeStruct(shape, bf16)],
        scratch_shapes=[square, square, square, pltpu.VMEM((1, GROUP * PACK, LANE), f32)],
        compiler_params=params(),
        name="soap",
    )(*views, grads)


MESH = pl.DeviceIdType.MESH


def place(size):
    index = lax.axis_index("dp")
    core = lax.rem(index, 2)
    col = lax.rem(lax.div(index, 2), size[1])
    row = lax.div(index, 2 * size[1])
    return row, col, core


def device(row, col, core, size, depth):
    return {"dp": (row * size[1] + col) * 2 + core, "seq": depth}


def greet(partners, layers, level, above, below):
    barrier = pltpu.get_barrier_semaphore()
    for partner in partners:
        pl.semaphore_signal(barrier, inc=1, device_id=partner, device_id_type=MESH)

    @pl.when(level > 0)
    def _():
        pl.semaphore_signal(barrier, inc=1, device_id=below, device_id_type=MESH)

    @pl.when(level < layers - 1)
    def _():
        pl.semaphore_signal(barrier, inc=1, device_id=above, device_id_type=MESH)

    inner = (level > 0).astype(jnp.int32) + (level < layers - 1).astype(jnp.int32)
    pl.semaphore_wait(barrier, len(partners) + inner)


def reduce_kernel(
    steps, rows, layers, lag, slots_ref, out_ref, own, inbox, first, second, up, down, down_sum,
    own_sem, core_send, core_recv, one_send, one_recv, two_send, two_recv,
    up_send, up_recv, down_send, down_recv,
):
    size = (2, 2)
    y, x, core = place(size)
    level = lax.axis_index("seq")
    other_core = device(y, x, 1 - core, size, level)
    across_x = device(y, 1 - x, core, size, level)
    across_y = device(1 - y, x, core, size, level)
    above = device(y, x, core, size, lax.rem(level + 1, layers))
    below = device(y, x, core, size, lax.rem(level + layers - 1, layers))
    firsts, seconds = [across_x, across_y], [across_y, across_x]

    def span(half, step):
        return pl.ds(pl.multiple_of((half * steps + step) * rows, rows), rows)

    def remote(source, target, send, recv, half, step, where):
        return pltpu.make_async_remote_copy(
            src_ref=source,
            dst_ref=target,
            send_sem=send.at[half, step],
            recv_sem=recv.at[half, step],
            device_id=where,
            device_id_type=MESH,
        )

    def own_copy(half, step):
        part = span(half, step)
        return pltpu.make_async_copy(
            slots_ref.at[:, :, core, part], own.at[:, :, part], own_sem.at[half, step]
        )

    def core_copy(half, step):
        part = span(half, step)
        return remote(
            slots_ref.at[:, :, 1 - core, part], inbox.at[:, :, part],
            core_send, core_recv, half, step, other_core,
        )

    def one_copy(half, step):
        part = span(half, step)
        source = own.at[:, 1 - x, part] if half == 0 else own.at[1 - y, :, part]
        return remote(source, first.at[:, part], one_send, one_recv, half, step, firsts[half])

    def two_copy(half, step):
        part = span(half, step)
        source = own.at[1 - y, x, part] if half == 0 else own.at[y, 1 - x, part]
        return remote(source, second.at[part], two_send, two_recv, half, step, seconds[half])

    def up_copy(half, step):
        part = span(half, step)
        return remote(up.at[part], up.at[part], up_send, up_recv, half, step, above)

    def down_copy(half, step):
        part = span(half, step)
        return remote(down_sum.at[part], down.at[part], down_send, down_recv, half, step, below)

    def inside(step):
        return jnp.logical_and(step >= 0, step < steps)

    greet([other_core, across_x, across_y], layers, level, above, below)

    @pl.loop(0, steps)
    def _(step):
        for half in range(2):
            own_copy(half, step).start()
            core_copy(half, step).start()

    @pl.loop(0, steps + lag * (layers + 1))
    def _(tick):
        one_step = tick - lag
        two_step = tick - 2 * lag
        up_step = two_step - lag * level
        down_step = two_step - lag * (layers - 1 - level)
        last_step = two_step - lag * (layers - 1)

        @pl.when(inside(tick))
        def _():
            for half in range(2):
                part = span(half, tick)
                own_copy(half, tick).wait()
                core_copy(half, tick).wait_recv()
                own[:, :, part] = own[:, :, part] + inbox[:, :, part]

        @pl.when(inside(one_step))
        def _():
            for half in range(2):
                part = span(half, one_step)
                one_copy(half, one_step).wait_recv()
                if half == 0:
                    own[:, x, part] = own[:, x, part] + first[:, part]
                else:
                    own[y, :, part] = own[y, :, part] + first[:, part]

        @pl.when(inside(two_step))
        def _():
            for half in range(2):
                part = span(half, two_step)
                two_copy(half, two_step).wait_recv()
                own[y, x, part] = own[y, x, part] + second[part]

        @pl.when(inside(up_step))
        def _():
            for half in range(2):
                part = span(half, up_step)

                @pl.when(level > 0)
                def _():
                    up_copy(half, up_step).wait_recv()
                    up[part] = up[part] + own[y, x, part]

                @pl.when(level == 0)
                def _():
                    up[part] = own[y, x, part]

        @pl.when(inside(down_step))
        def _():
            for half in range(2):
                part = span(half, down_step)

                @pl.when(level < layers - 1)
                def _():
                    down_copy(half, down_step).wait_recv()
                    down_sum[part] = down[part] + own[y, x, part]

                @pl.when(level == layers - 1)
                def _():
                    down_sum[part] = own[y, x, part]

        @pl.when(inside(last_step))
        def _():
            for half in range(2):
                part = span(half, last_step)

                @pl.when(level < layers - 1)
                def _():
                    out_ref[part] = up[part] + down[part]

                @pl.when(level == layers - 1)
                def _():
                    out_ref[part] = up[part]

        @pl.when(inside(tick))
        def _():
            for half in range(2):
                one_copy(half, tick).start()

        @pl.when(inside(one_step))
        def _():
            for half in range(2):
                two_copy(half, one_step).start()

        @pl.when(jnp.logical_and(inside(up_step), level < layers - 1))
        def _():
            for half in range(2):
                up_copy(half, up_step).start()

        @pl.when(jnp.logical_and(inside(down_step), level > 0))
        def _():
            for half in range(2):
                down_copy(half, down_step).start()

    @pl.loop(0, steps)
    def _(step):
        for half in range(2):
            core_copy(half, step).wait_send()
            one_copy(half, step).wait_send()
            two_copy(half, step).wait_send()

            @pl.when(level < layers - 1)
            def _():
                up_copy(half, step).wait_send()

            @pl.when(level > 0)
            def _():
                down_copy(half, step).wait_send()


def reduce_slots(slots, layers, rows, lag):
    total = slots.shape[0] // 8 * PACK
    steps = total // (2 * rows)
    chunk = (total, LANE)
    sems = pltpu.SemaphoreType.DMA((2, steps))
    out = pl.pallas_call(
        functools.partial(reduce_kernel, steps, rows, layers, lag),
        in_specs=[pl.BlockSpec(memory_space=pl.ANY)],
        out_specs=pl.BlockSpec(memory_space=pltpu.VMEM),
        out_shape=jax.ShapeDtypeStruct(chunk, bf16),
        scratch_shapes=[
            pltpu.VMEM((2, 2) + chunk, bf16),
            pltpu.VMEM((2, 2) + chunk, bf16),
            pltpu.VMEM((2,) + chunk, bf16),
        ]
        + [pltpu.VMEM(chunk, bf16)] * 4
        + [sems] * 11,
        compiler_params=pltpu.CompilerParams(
            vmem_limit_bytes=62 * 2**20, collective_id=0, has_side_effects=True
        ),
        cost_estimate=pl.CostEstimate(flops=0, bytes_accessed=WAIT_BYTES, transcendentals=0),
        name="reduce_slots",
    )(slots.reshape((2, 2, 2) + chunk))
    return out.reshape(total // PACK, PACK, LANE)


def gather_kernel(
    steps, rows, lag, mine_ref, out_ref, own_sem, one_send, one_recv, two_send, two_recv,
    near_send, near_recv, far_send, far_recv, core_send, core_recv,
):
    size = (2, 2)
    y, x, core = place(size)
    level = lax.axis_index("seq")
    side = lax.rem(level, 2)
    other_core = device(y, x, 1 - core, size, level)
    across_x = device(y, 1 - x, core, size, level)
    across_y = device(1 - y, x, core, size, level)
    beside = device(y, x, core, size, level + 1 - 2 * side)
    firsts, seconds = [across_x, across_y], [across_y, across_x]

    def span(kind, half, step):
        return pl.ds(pl.multiple_of(((kind * 2 + half) * steps + step) * rows, rows), rows)

    def kind_of(turn):
        late = lax.div(turn, steps)
        return side + (2 - side) * late, lax.rem(turn, steps)

    def remote(source, target, send, recv, where):
        return pltpu.make_async_remote_copy(
            src_ref=source,
            dst_ref=target,
            send_sem=send,
            recv_sem=recv,
            device_id=where,
            device_id_type=MESH,
        )

    def own_copy():
        return pltpu.make_async_copy(mine_ref, out_ref.at[y, x, core], own_sem)

    def one_copy(half, turn):
        kind, step = kind_of(turn)
        part = span(kind, half, step)
        return remote(
            mine_ref.at[part], out_ref.at[y, x, core, part],
            one_send.at[half, turn], one_recv.at[half, turn], firsts[half],
        )

    def two_copy(half, turn):
        kind, step = kind_of(turn)
        part = span(kind, half, step)
        ref = out_ref.at[y, :, core, part] if half == 0 else out_ref.at[:, x, core, part]
        return remote(
            ref, ref, two_send.at[half, turn], two_recv.at[half, turn], seconds[half]
        )

    def near_copy(half, step):
        part = span(side, half, step)
        ref = out_ref.at[y, 1 - x, core, part] if half == 0 else out_ref.at[1 - y, x, core, part]
        return remote(ref, ref, near_send.at[half, step], near_recv.at[half, step], beside)

    def far_copy(half, step):
        part = span(side, half, step)
        ref = out_ref.at[1 - y, :, core, part] if half == 0 else out_ref.at[:, 1 - x, core, part]
        return remote(ref, ref, far_send.at[half, step], far_recv.at[half, step], beside)

    def core_copy(kind, half, step, slot):
        ref = out_ref.at[:, :, core, span(kind, half, step)]
        return remote(ref, ref, core_send.at[half, slot], core_recv.at[half, slot], other_core)

    partners = [other_core, across_x, across_y, beside]
    barrier = pltpu.get_barrier_semaphore()
    for partner in partners:
        pl.semaphore_signal(barrier, inc=1, device_id=partner, device_id_type=MESH)
    pl.semaphore_wait(barrier, len(partners))

    own_copy().start()
    turns = 2 * steps

    @pl.loop(0, turns + 4 * lag + 2)
    def _(tick):
        @pl.when(tick < turns)
        def _():
            for half in range(2):
                one_copy(half, tick).start()

        @pl.when(tick == lag)
        def _():
            own_copy().wait()

        turn = tick - lag

        @pl.when(jnp.logical_and(turn >= 0, turn < turns))
        def _():
            for half in range(2):
                one_copy(half, turn).wait_recv()
                two_copy(half, turn).start()

        @pl.when(jnp.logical_and(turn >= 0, turn < steps))
        def _():
            for half in range(2):
                near_copy(half, turn).start()

        after = tick - 2 * lag

        @pl.when(jnp.logical_and(after >= 0, after < turns))
        def _():
            kind, step = kind_of(after)
            for half in range(2):
                two_copy(half, after).wait_recv()
                core_copy(kind, half, step, after).start()

        @pl.when(jnp.logical_and(after >= 0, after < steps))
        def _():
            for half in range(2):
                far_copy(half, after).start()

        late = tick - 4 * lag
        given = lax.div(late, 2)

        @pl.when(jnp.logical_and(late >= 0, jnp.logical_and(given < steps, late == 2 * given)))
        def _():
            for half in range(2):
                near_copy(half, given).wait_recv()
                far_copy(half, given).wait_recv()
                core_copy(1 - side, half, given, turns + given).start()

    @pl.loop(0, turns)
    def _(turn):
        kind, step = kind_of(turn)
        for half in range(2):
            one_copy(half, turn).wait_send()
            two_copy(half, turn).wait_send()
            core_copy(kind, half, step, turn).wait()

    @pl.loop(0, steps)
    def _(step):
        for half in range(2):
            near_copy(half, step).wait_send()
            far_copy(half, step).wait_send()
            core_copy(1 - side, half, step, turns + step).wait()


def gather_slots(packed, rows, lag):
    total = packed.shape[0] * PACK
    steps = total // (6 * rows)

    def sems(count):
        return [pltpu.SemaphoreType.DMA((2, count))] * 2

    out = pl.pallas_call(
        functools.partial(gather_kernel, steps, rows, lag),
        in_specs=[pl.BlockSpec(memory_space=pltpu.VMEM)],
        out_specs=pl.BlockSpec(memory_space=pl.ANY),
        out_shape=jax.ShapeDtypeStruct((2, 2, 2, total, LANE), bf16),
        scratch_shapes=[pltpu.SemaphoreType.DMA]
        + sems(2 * steps) + sems(2 * steps) + sems(steps) + sems(steps) + sems(3 * steps),
        compiler_params=pltpu.CompilerParams(
            vmem_limit_bytes=62 * 2**20, collective_id=1, has_side_effects=True
        ),
        cost_estimate=pl.CostEstimate(flops=0, bytes_accessed=WAIT_BYTES, transcendentals=0),
        name="gather_slots",
    )(packed.reshape(total, LANE))
    return out.reshape(8 * packed.shape[0], PACK, LANE)


def norm_forward(hidden, gain, shift):
    center = hidden - jnp.mean(hidden, axis=-1, keepdims=True)
    spread = jnp.mean(center * center, axis=-1, keepdims=True)
    inverse = lax.rsqrt(spread + norm_eps)
    unit = center * inverse
    return (unit * gain + shift, unit, inverse)


def norm_backward(incoming, unit, inverse, gain):
    scaled = incoming * gain
    grad_hidden = inverse * (
        scaled
        - jnp.mean(scaled, axis=-1, keepdims=True)
        - unit * jnp.mean(scaled * unit, axis=-1, keepdims=True)
    )
    return (grad_hidden, jnp.sum(incoming * unit, axis=0), jnp.sum(incoming, axis=0))


def gelu(value):
    return 0.5 * value * (1.0 + lax.erf(value * 0.5**0.5))


def gelu_slope(value):
    bell = jnp.exp(-0.5 * value * value) * (0.5 / math.pi) ** 0.5
    return 0.5 * (1.0 + lax.erf(value * 0.5**0.5)) + value * bell


def unpack(vector, width):
    return [vector[number * width : (number + 1) * width] for number in range(8)] + [
        vector[8 * width :]
    ]


def forward_layer(hidden, matrices, pieces, scale):
    w_qkv, w_out, w_up, w_down = matrices
    bias_q, bias_v, bias_out, bias_down, gain_one, shift_one, gain_two, shift_two, bias_up = pieces
    hid_low = hidden.astype(bf16)
    bias_q = bias_q.reshape(-1, LANE)
    bias_qkv = jnp.stack([bias_q, jnp.zeros_like(bias_q), bias_v.reshape(-1, LANE)], axis=1)
    qkv = (dot(hid_low, w_qkv) + bias_qkv.reshape(-1)).astype(bf16)
    mixed, lse = attend(qkv, scale)
    branch = dot(mixed, w_out) + bias_out
    normed, unit_one, inv_one = norm_forward(hidden + branch, gain_one, shift_one)
    norm_low = normed.astype(bf16)
    pre_act = dot(norm_low, w_up) + bias_up
    act_low = gelu(pre_act).astype(bf16)
    down = dot(act_low, w_down) + bias_down
    result, unit_two, inv_two = norm_forward(normed + down, gain_two, shift_two)
    kept = (
        hid_low, qkv, lse, mixed, unit_one, inv_one, norm_low, pre_act, act_low, unit_two, inv_two
    )
    return (result, kept)


def backward_layer(incoming, matrices, pieces, kept, scale, slots, slot_shape, rows, base):
    w_qkv, w_out, w_up, w_down = matrices
    gain_one, gain_two = pieces[4], pieces[6]
    hid_low, qkv, lse, mixed, unit_one, inv_one, norm_low, pre_act, act_low, unit_two, inv_two = kept
    width = mixed.shape[1]
    square = (width // BLK) ** 2
    up_count = act_low.shape[1] // BLK * (width // BLK)
    grad_two, gain_two_g, shift_two_g = norm_backward(incoming, unit_two, inv_two, gain_two)
    down_low = grad_two.astype(bf16)
    slots = plain_grad(
        slots, slot_shape, rows, act_low, down_low, base + 4 * square + up_count, width
    )
    grad_act = dot(down_low, w_down, 1, 1)
    up_low = (gelu_slope(pre_act) * grad_act).astype(bf16)
    slots = plain_grad(slots, slot_shape, rows, norm_low, up_low, base + 4 * square, width)
    grad_norm = grad_two + dot(up_low, w_up, 1, 1)
    grad_one, gain_one_g, shift_one_g = norm_backward(grad_norm, unit_one, inv_one, gain_one)
    out_low = grad_one.astype(bf16)
    slots = plain_grad(slots, slot_shape, rows, mixed, out_low, base + 3 * square, width)
    grad_mix = dot(out_low, w_out, 1, 1).astype(bf16)
    grad_qkv = attend_back(qkv, lse, grad_mix, scale)
    slots = qkv_grad(slots, slot_shape, rows, hid_low, grad_qkv, base, width)
    grad_hidden = grad_one + dot(grad_qkv, w_qkv, 1, 1)

    def total(array):
        return jnp.sum(array, axis=0, dtype=f32)

    bias_qkv = total(grad_qkv).reshape(-1, 3, LANE)
    vec_grad = jnp.concatenate(
        [
            bias_qkv[:, 0].reshape(-1),
            bias_qkv[:, 2].reshape(-1),
            total(out_low),
            total(down_low),
            gain_one_g,
            shift_one_g,
            gain_two_g,
            shift_two_g,
            total(up_low),
        ]
    )
    return grad_hidden, slots, vec_grad


def swap_in(array):
    return lax.all_to_all(array, "seq", split_axis=0, concat_axis=1, tiled=True)


def swap_out(array):
    return lax.all_to_all(array, "seq", split_axis=1, concat_axis=0, tiled=True)


def near_group():
    return lax.axis_size("dp") == 8 and lax.axis_size("seq") % 2 == 0


def gather_blocks(packed):
    total = packed.shape[0] * PACK
    if near_group() and total % (6 * GATHER_ROWS) == 0:
        return gather_slots(packed, GATHER_ROWS, GATHER_LAG)
    return lax.all_gather(packed, "dp", axis=0, tiled=True)


def reduce_blocks(slots):
    total = slots.shape[0] // lax.axis_size("dp") * PACK
    if near_group() and total % (2 * REDUCE_ROWS) == 0:
        return reduce_slots(slots, lax.axis_size("seq"), REDUCE_ROWS, REDUCE_LAG)
    return lax.psum(lax.psum_scatter(slots, "dp", scatter_dimension=0, tiled=True), "seq")


def local(
    tokens,
    cotangent,
    tok_weight,
    mask_count,
    owner_list,
    masters,
    moment_one,
    moment_two,
    left_basis,
    right_basis,
    vectors,
    vec_moment_one,
    vec_moment_two,
):
    data_parts = lax.axis_size("dp")
    seq_count, local_len, width = tokens.shape
    layer_count = vectors.shape[0]
    inner = vectors.shape[-1] - 8 * width
    owned_count = masters.shape[0]
    block_total = owner_list.shape[0]
    scale = HDIM ** (-0.5)

    master_view = row_view(masters)
    packed = pack_blocks(master_view)[:owned_count]
    gathered = gather_blocks(packed)

    hidden = swap_in(tokens)
    per_seq = hidden.shape[0]
    full_len = hidden.shape[1]
    hidden = hidden.reshape(full_len, width).astype(f32)
    incoming = swap_in(cotangent).reshape(full_len, width).astype(f32)
    first = lax.axis_index("seq") * per_seq
    weight = lax.all_gather(tok_weight, "seq", axis=1, tiled=True)
    weight = lax.dynamic_slice_in_dim(weight, first, per_seq, 0).reshape(full_len, 1)
    count = lax.dynamic_slice_in_dim(mask_count, first, per_seq, 0)
    positions = jnp.arange(full_len, dtype=jnp.int32)
    masked = (positions < count[0]).astype(f32)[:, None]
    incoming = incoming * (weight.astype(f32) * (1.0 + masked) * 0.25)

    per_layer = block_total // layer_count
    weights = [
        layer_weights(gathered, owner_list, per_layer * number, width, inner)
        for number in range(layer_count)
    ]
    saved = []
    for number in range(layer_count):
        hidden, kept = forward_layer(
            hidden, weights[number], unpack(vectors[number], width), scale
        )
        saved.append(kept)
    layer_out = swap_out(hidden.astype(bf16).reshape(per_seq, full_len, width))

    chunk = owned_count + 1
    rows = owner_list + owner_list // owned_count
    slot_shape = (data_parts * chunk, PACK, LANE)
    slots = None
    vec_grads = [None] * layer_count
    for number in reversed(range(layer_count)):
        incoming, slots, vec_grads[number] = backward_layer(
            incoming,
            weights[number],
            unpack(vectors[number], width),
            saved[number],
            scale,
            slots,
            slot_shape,
            rows,
            per_layer * number,
        )
    vec_grad = jnp.stack(vec_grads)
    vec_high = vec_grad.astype(bf16)
    vec_low = (vec_grad - vec_high.astype(f32)).astype(bf16)
    vec_slot = jnp.concatenate([vec_high.reshape(-1, LANE), vec_low.reshape(-1, LANE)], axis=0)
    slots = slots.reshape((data_parts, chunk) + vec_slot.shape)
    vec_slots = jnp.broadcast_to(vec_slot, (data_parts, 1) + vec_slot.shape)
    slots = lax.dynamic_update_slice(slots, vec_slots, (0, owned_count, 0, 0))
    owned = reduce_blocks(slots.reshape(slot_shape))
    input_grad = swap_out(incoming.reshape(per_seq, full_len, width))

    vec_rows = owned[owned_count].astype(f32)
    half = PACK // 2
    vec_total = (vec_rows[:half] + vec_rows[half:]).reshape(vectors.shape)
    views = [master_view] + [
        row_view(array) for array in (moment_one, moment_two, left_basis, right_basis)
    ]
    extra = views[0].shape[0] * GROUP - chunk
    if extra > 0:
        owned = jnp.pad(owned, ((0, extra), (0, 0), (0, 0)))
    new_one, new_two, new_masters, copies = [
        row_unview(array, owned_count) for array in soap(views, owned)
    ]
    vec_one = beta_one * vec_moment_one + (1.0 - beta_one) * vec_total
    vec_two = beta_two * vec_moment_two + (1.0 - beta_two) * vec_total * vec_total
    new_vectors = vectors - vector_rate * (vec_one / fix_one) / (
        jnp.sqrt(vec_two / fix_two) + adam_eps
    )
    return (
        layer_out, input_grad, new_one, new_two, new_masters, copies, new_vectors, vec_one, vec_two
    )


def solution(mesh):
    rows = P("dp", None)
    tokens = P("dp", "seq", None)
    return jax.shard_map(
        local,
        mesh=mesh,
        in_specs=(tokens, tokens, P("dp", "seq"), P("dp"), P()) + (rows,) * 5 + (P(),) * 3,
        out_specs=(tokens, tokens) + (rows,) * 4 + (P(),) * 3,
        check_vma=False,
    )
```

```python
import functools
import math
import jax
import jax.numpy as jnp
from jax import lax
from jax.experimental import pallas as pl
from jax.experimental.pallas import tpu as pltpu
from jax.sharding import PartitionSpec as P

HEADS = 12
HDIM = 64
BLK = 192
LANE = 128
HALF = BLK // 2
PACK = BLK * BLK // LANE
GROUP = 8
GATHER_ROWS = 144
GATHER_LAG = 2
ALONE_SHARE = 0.28
SPREAD = 3
REDUCE_ROWS = 144
REDUCE_LAG = 2
WAIT_BYTES = 3 * 10**8

norm_eps = 1e-05
beta_one = 0.95
beta_two = 0.95
adam_eps = 1e-08
matrix_rate = 0.02
vector_rate = 0.2
decay_rate = 0.01
step_count = 6
fix_one = 1.0 - beta_one**step_count
fix_two = 1.0 - beta_two**step_count
bf16 = jnp.bfloat16
f32 = jnp.float32


def params(**kw):
    return pltpu.CompilerParams(vmem_limit_bytes=56 * 2**20, **kw)


def low_lanes(rows):
    return lax.broadcasted_iota(jnp.int32, (rows, LANE), 1) < HDIM


def swap(value):
    return pltpu.roll(value, HDIM, 1)


def row_view(array):
    count = array.shape[0]
    padded = -count % GROUP
    if padded:
        array = jnp.pad(array, ((0, padded), (0, 0)))
    groups = (count + padded) // GROUP
    return (
        array.reshape(groups, GROUP, PACK, LANE)
        .transpose(0, 2, 1, 3)
        .reshape(groups, GROUP * PACK, LANE)
    )


def row_unview(array, count):
    groups = array.shape[0]
    return (
        array.reshape(groups, PACK, GROUP, LANE)
        .transpose(0, 2, 1, 3)
        .reshape(groups * GROUP, PACK * LANE)[:count]
    )


def triple(ref, row):
    return [ref[0, pl.ds(row + GROUP * part, HALF, stride=3 * GROUP), :] for part in range(3)]


def put_triple(ref, row, pieces):
    for part, piece in enumerate(pieces):
        ref[0, pl.ds(row + GROUP * part, HALF, stride=3 * GROUP), :] = piece


def to_square(pieces, main_ref, tail_ref):
    first, second, third = pieces
    low = low_lanes(HALF)
    second_s, third_s = swap(second), swap(third)
    main_ref[pl.ds(0, HALF, stride=2), :] = first
    main_ref[pl.ds(1, HALF, stride=2), :] = jnp.where(low, second_s, third_s)
    tail_ref[pl.ds(0, HALF, stride=2), :] = second
    tail_ref[pl.ds(1, HALF, stride=2), :] = third_s


def from_square(main_ref, tail_ref):
    low = low_lanes(HALF)
    even_main = main_ref[pl.ds(0, HALF, stride=2), :]
    odd_main = swap(main_ref[pl.ds(1, HALF, stride=2), :])
    even_tail = tail_ref[pl.ds(0, HALF, stride=2), :]
    odd_tail = swap(tail_ref[pl.ds(1, HALF, stride=2), :])
    return [even_main, jnp.where(low, even_tail, odd_main), jnp.where(low, odd_main, odd_tail)]


def pack_kernel(src_ref, out_ref, main_ref, tail_ref):
    low = low_lanes(HALF)
    for row in range(GROUP):
        spot = row % 2
        main, tail = main_ref.at[spot], tail_ref.at[spot]
        to_square(triple(src_ref, row), main, tail)
        out_ref[row, 0:BLK, :] = main[...].astype(bf16)
        out_ref[row, BLK:PACK, :] = jnp.where(
            low, tail[0:HALF, :], swap(tail[HALF:BLK, :])
        ).astype(bf16)


def pack_blocks(view):
    groups = view.shape[0]
    return pl.pallas_call(
        pack_kernel,
        grid=(groups,),
        in_specs=[pl.BlockSpec((1, GROUP * PACK, LANE), lambda i: (i, 0, 0))],
        out_specs=pl.BlockSpec((GROUP, PACK, LANE), lambda i: (i, 0, 0)),
        out_shape=jax.ShapeDtypeStruct((groups * GROUP, PACK, LANE), bf16),
        scratch_shapes=[pltpu.VMEM((2, BLK, LANE), f32), pltpu.VMEM((2, BLK, LANE), f32)],
        compiler_params=params(),
        name="pack",
    )(view)


def unfold(block):
    fold = block[BLK:PACK, :]
    return block[0:BLK, :], jnp.concatenate([fold[:, :HDIM], fold[:, HDIM:]], axis=0)


def assemble_kernel(cells, owner_ref, *refs):
    out_ref = refs[-1]
    low = low_lanes(HALF)
    for number, (row, lanes) in enumerate(cells):
        left, right = refs[2 * number], refs[2 * number + 1]
        fold_a = left[0, BLK:PACK, :].astype(f32)
        fold_b = right[0, BLK:PACK, :].astype(f32)
        tails = [(fold_a, swap(fold_b)), (swap(fold_a), fold_b)]
        out_ref[pl.ds(row, BLK), pl.ds(lanes[0], LANE)] = left[0, 0:BLK, :]
        for half, (tail_a, tail_b) in enumerate(tails):
            main_b = swap(right[0, half * HALF : (half + 1) * HALF, :].astype(f32))
            rows = pl.ds(row + half * HALF, HALF)
            out_ref[rows, pl.ds(lanes[1], LANE)] = jnp.where(low, tail_a, main_b).astype(bf16)
            out_ref[rows, pl.ds(lanes[2], LANE)] = jnp.where(low, main_b, tail_b).astype(bf16)


def assemble(gathered, owner_list, shape, tile, cells, block_of):
    grid = (shape[0] // tile[0], shape[1] // tile[1])
    count = 2 * len(cells)

    def spec(which):
        return pl.BlockSpec(
            (1, PACK, LANE), lambda i, j, owner: (owner[block_of(i, j, which)], 0, 0)
        )

    return pl.pallas_call(
        functools.partial(assemble_kernel, cells),
        grid_spec=pltpu.PrefetchScalarGridSpec(
            num_scalar_prefetch=1,
            grid=grid,
            in_specs=[spec(which) for which in range(count)],
            out_specs=pl.BlockSpec(tile, lambda i, j, owner: (i, j)),
        ),
        out_shape=jax.ShapeDtypeStruct(shape, bf16),
        compiler_params=params(),
        name="assemble",
    )(owner_list, *([gathered] * count))


def layer_weights(gathered, owner_list, base, width, inner):
    cols = width // BLK
    inner_cols = inner // BLK
    square = cols * cols
    cells = []
    for matrix in range(3):
        for pair in range(cols // 2):
            cells.append((0, [3 * LANE * (3 * pair + part) + LANE * matrix for part in range(3)]))
    per_matrix = cols

    def block_qkv(i, j, which):
        return base + (which // per_matrix) * square + i * cols + which % per_matrix

    w_qkv = assemble(gathered, owner_list, (width, 3 * width), (BLK, 3 * width), cells, block_qkv)
    plain = []
    for row in range(2):
        for pair in range(cols // 2):
            plain.append(
                (row * BLK, [2 * BLK * pair + LANE * part for part in range(3)])
            )

    def block_plain(start, row_blocks):
        def block(i, j, which):
            return start + (2 * i + which // cols) * row_blocks + cols * j + which % cols

        return block

    tile = (2 * BLK, width)
    w_out = assemble(
        gathered, owner_list, (width, width), tile, plain, block_plain(base + 3 * square, cols)
    )
    up_base = base + 4 * square
    w_up = assemble(
        gathered, owner_list, (width, inner), tile, plain, block_plain(up_base, inner_cols)
    )
    down_base = up_base + cols * inner_cols
    w_down = assemble(
        gathered, owner_list, (inner, width), tile, plain, block_plain(down_base, cols)
    )
    return w_qkv, w_out, w_up, w_down
def dot(left, right, left_dim=1, right_dim=0):
    return lax.dot_general(
        left, right, (((left_dim,), (right_dim,)), ((), ())), preferred_element_type=f32
    )


def head_masks():
    lane = lax.broadcasted_iota(jnp.int32, (1, LANE), 1)
    first = (lane < HDIM).astype(f32)
    return [first.astype(bf16), (1.0 - first).astype(bf16)]


def attend_kernel(scale, qkv_ref, mix_ref, lse_ref):
    length = qkv_ref.shape[0]
    query, keys, values = (qkv_ref[:, pl.ds(LANE * part, LANE)] for part in range(3))
    mixed, logs = [], []
    for mask in head_masks():
        scores = dot(query * mask, keys, 1, 1) * scale
        highest = jnp.max(scores, axis=1, keepdims=True)
        raised = jnp.exp(scores - highest)
        total = jnp.sum(raised, axis=1, keepdims=True)
        probs = raised * (1.0 / total)
        mixed.append(dot(probs.astype(bf16), values))
        logs.append(highest + jnp.log(total))
    low = low_lanes(length)
    mix_ref[...] = jnp.where(low, mixed[0], mixed[1]).astype(bf16)
    lse_ref[...] = jnp.where(low, logs[0], logs[1])


def attend(qkv, scale):
    length, wide = qkv.shape
    pairs = wide // (3 * LANE)
    return pl.pallas_call(
        functools.partial(attend_kernel, scale),
        grid=(pairs,),
        in_specs=[pl.BlockSpec((length, 3 * LANE), lambda i: (0, i))],
        out_specs=[pl.BlockSpec((length, LANE), lambda i: (0, i))] * 2,
        out_shape=[
            jax.ShapeDtypeStruct((length, wide // 3), bf16),
            jax.ShapeDtypeStruct((length, wide // 3), f32),
        ],
        compiler_params=params(),
        name="attend",
    )(qkv)


def attend_back_kernel(scale, qkv_ref, lse_ref, grad_ref, out_ref):
    length = qkv_ref.shape[0]
    query, keys, values = (qkv_ref[:, pl.ds(LANE * part, LANE)] for part in range(3))
    grad = grad_ref[...]
    parts = []
    for number, mask in enumerate(head_masks()):
        scores = dot(query * mask, keys, 1, 1) * scale
        probs = jnp.exp(scores - lse_ref[:, number * HDIM : number * HDIM + 1])
        grad_probs = dot(grad * mask, values, 1, 1)
        centre = jnp.sum(probs * grad_probs, axis=1, keepdims=True)
        grad_scores = (probs * (grad_probs - centre)).astype(bf16)
        parts.append(
            (
                dot(grad_scores, keys) * scale,
                dot(grad_scores, query, 0, 0) * scale,
                dot(probs.astype(bf16), grad, 0, 0),
            )
        )
    low = low_lanes(length)
    for part in range(3):
        out_ref[:, pl.ds(LANE * part, LANE)] = jnp.where(
            low, parts[0][part], parts[1][part]
        ).astype(bf16)


def attend_back(qkv, lse, grad, scale):
    length, wide = qkv.shape
    pairs = wide // (3 * LANE)
    return pl.pallas_call(
        functools.partial(attend_back_kernel, scale),
        grid=(pairs,),
        in_specs=[
            pl.BlockSpec((length, 3 * LANE), lambda i: (0, i)),
            pl.BlockSpec((length, LANE), lambda i: (0, i)),
            pl.BlockSpec((length, LANE), lambda i: (0, i)),
        ],
        out_specs=pl.BlockSpec((length, 3 * LANE), lambda i: (0, i)),
        out_shape=jax.ShapeDtypeStruct((length, wide), bf16),
        compiler_params=params(),
        name="attend_back",
    )(qkv, lse, grad)


def weight_grad_kernel(lanes_of, block_of, panel, steps, rows_ref, left_ref, right_ref, *refs):
    out_ref, stage_ref, turned_ref, sems = refs[-4:]
    i, j = pl.program_id(0), pl.program_id(1)
    step = i * pl.num_programs(1) + j
    spot = lax.rem(step, 2)
    pairs = panel // (2 * BLK)
    count = 4 * pairs

    def copy(which, slot, row):
        return pltpu.make_async_copy(
            stage_ref.at[slot, which], out_ref.at[row], sems.at[slot, which]
        )

    @pl.when(step >= 2)
    def _():
        for which in range(count):
            copy(which, spot, 0).wait()

    @pl.when(j == 0)
    def _():
        turned_ref[...] = left_ref[...].T

    left = turned_ref[...]
    low_top, low_all = low_lanes(HALF), low_lanes(BLK)
    for pair in range(pairs):
        right = jnp.concatenate(
            [
                right_ref[:, pl.ds(pl.multiple_of(lanes_of(j, 3 * pair + part), LANE), LANE)]
                for part in range(3)
            ],
            axis=1,
        )
        product = dot(left, right)
        for half in range(2):
            tile = product[half * BLK : (half + 1) * BLK, :]
            first, second, third = (tile[:, LANE * part : LANE * (part + 1)] for part in range(3))
            which = half * 2 * pairs + 2 * pair
            stage_ref[spot, which, 0:BLK, :] = first.astype(bf16)
            stage_ref[spot, which, BLK:PACK, :] = jnp.where(
                low_top, second[0:HALF, :], swap(second[HALF:BLK, :])
            ).astype(bf16)
            stage_ref[spot, which + 1, 0:BLK, :] = swap(
                jnp.where(low_all, third, second)
            ).astype(bf16)
            stage_ref[spot, which + 1, BLK:PACK, :] = jnp.where(
                low_top, swap(third[0:HALF, :]), third[HALF:BLK, :]
            ).astype(bf16)
    for which in range(count):
        block = block_of(i, j, which // (2 * pairs), which % (2 * pairs))
        copy(which, spot, rows_ref[block]).start()

    @pl.when(step == steps - 1)
    def _():
        for which in range(count):
            copy(which, spot, 0).wait()
            if steps > 1:
                copy(which, 1 - spot, 0).wait()


def weight_grad(slots, slot_shape, rows, left, right, grid, panel, right_spec, lanes_of, block_of):
    steps = grid[0] * grid[1]
    count = 4 * (panel // (2 * BLK))
    whole = [pl.BlockSpec((left.shape[0], 2 * BLK), lambda i, j, s: (0, i)), right_spec]
    extra, aliases = [], {}
    if slots is not None:
        extra = [slots]
        aliases = {3: 0}
    return pl.pallas_call(
        functools.partial(weight_grad_kernel, lanes_of, block_of, panel, steps),
        grid_spec=pltpu.PrefetchScalarGridSpec(
            num_scalar_prefetch=1,
            grid=grid,
            in_specs=whole + [pl.BlockSpec(memory_space=pl.ANY)] * len(extra),
            out_specs=pl.BlockSpec(memory_space=pl.ANY),
            scratch_shapes=[
                pltpu.VMEM((2, count, PACK, LANE), bf16),
                pltpu.VMEM((2 * BLK, left.shape[0]), bf16),
                pltpu.SemaphoreType.DMA((2, count)),
            ],
        ),
        out_shape=jax.ShapeDtypeStruct(slot_shape, bf16),
        input_output_aliases=aliases,
        compiler_params=params(),
        name="weight_grad",
    )(rows, left, right, *extra)


def plain_grad(slots, slot_shape, rows, left, right, base, width):
    cols = right.shape[1] // BLK
    per = width // BLK
    return weight_grad(
        slots,
        slot_shape,
        rows,
        left,
        right,
        (left.shape[1] // (2 * BLK), right.shape[1] // width),
        width,
        pl.BlockSpec((right.shape[0], width), lambda i, j, s: (0, j)),
        lambda j, piece: piece * LANE,
        lambda i, j, half, col: base + (2 * i + half) * cols + j * per + col,
    )


def qkv_grad(slots, slot_shape, rows, left, right, base, width):
    per = width // BLK
    return weight_grad(
        slots,
        slot_shape,
        rows,
        left,
        right,
        (width // (2 * BLK), 3),
        width,
        pl.BlockSpec(right.shape, lambda i, j, s: (0, 0)),
        lambda j, piece: 3 * LANE * piece + LANE * j,
        lambda i, j, half, col: base + j * per * per + (2 * i + half) * per + col,
    )


def soap_kernel(
    masters_ref, one_ref, two_ref, left_ref, right_ref, grad_ref,
    one_out, two_out, masters_out, copies_out, left_sq, right_sq, work, full,
):
    def square(refs):
        return jnp.concatenate([refs[0][...], refs[1][:, :HDIM]], axis=1).astype(bf16)

    def keep(refs, value):
        refs[0][...] = value[:, :LANE]
        refs[1][:, :HDIM] = value[:, LANE:]

    for row in range(GROUP):
        spot = row
        left_refs = [left_sq.at[spot, 0], left_sq.at[spot, 1]]
        right_refs = [right_sq.at[spot, 0], right_sq.at[spot, 1]]
        refs = [work.at[spot, 0], work.at[spot, 1]]
        to_square(triple(left_ref, row), *left_refs)
        to_square(triple(right_ref, row), *right_refs)
        left, right = square(left_refs), square(right_refs)
        main, tail = unfold(grad_ref[row])
        grad = jnp.concatenate([main, tail], axis=1)
        rotated = dot(dot(left, grad, 0, 0).astype(bf16), right)
        keep(refs, rotated)
        pieces = from_square(*refs)
        ones, twos = triple(one_ref, row), triple(two_ref, row)
        ones = [beta_one * old + (1.0 - beta_one) * new for old, new in zip(ones, pieces)]
        twos = [beta_two * old + (1.0 - beta_two) * new * new for old, new in zip(twos, pieces)]
        put_triple(one_out, row, ones)
        put_triple(two_out, row, twos)
        moves = [
            (one / fix_one) / (jnp.sqrt(two / fix_two) + adam_eps) for one, two in zip(ones, twos)
        ]
        to_square(moves, *refs)
        restored = dot(dot(left, square(refs)).astype(bf16), right, 1, 1)
        keep(refs, restored)
        pieces = from_square(*refs)
        old = triple(masters_ref, row)
        new = [
            value - matrix_rate * (step + decay_rate * value) for value, step in zip(old, pieces)
        ]
        put_triple(masters_out, row, new)
        put_triple(full, row, new)
    copies_out[0] = full[0].astype(bf16)


def soap(views, grads):
    groups = views[0].shape[0]
    view_spec = pl.BlockSpec((1, GROUP * PACK, LANE), lambda i: (i, 0, 0))
    shape = (groups, GROUP * PACK, LANE)
    square = pltpu.VMEM((GROUP, 2, BLK, LANE), f32)
    return pl.pallas_call(
        soap_kernel,
        grid=(groups,),
        in_specs=[view_spec] * 5 + [pl.BlockSpec((GROUP, PACK, LANE), lambda i: (i, 0, 0))],
        out_specs=[view_spec] * 4,
        out_shape=[jax.ShapeDtypeStruct(shape, f32)] * 3 + [jax.ShapeDtypeStruct(shape, bf16)],
        scratch_shapes=[square, square, square, pltpu.VMEM((1, GROUP * PACK, LANE), f32)],
        compiler_params=params(),
        name="soap",
    )(*views, grads)


MESH = pl.DeviceIdType.MESH


def place(size):
    index = lax.axis_index("dp")
    core = lax.rem(index, 2)
    col = lax.rem(lax.div(index, 2), size[1])
    row = lax.div(index, 2 * size[1])
    return row, col, core


def device(row, col, core, size, depth):
    return {"dp": (row * size[1] + col) * 2 + core, "seq": depth}


def greet(partners):
    barrier = pltpu.get_barrier_semaphore()
    for partner in partners:
        pl.semaphore_signal(barrier, inc=1, device_id=partner, device_id_type=MESH)
    pl.semaphore_wait(barrier, len(partners))


def send_to(source, target, send, recv, where):
    return pltpu.make_async_remote_copy(
        src_ref=source,
        dst_ref=target,
        send_sem=send,
        recv_sem=recv,
        device_id=where,
        device_id_type=MESH,
    )


def exchange(level, layers, pairs, keep_sem, send, recv):
    copies = []
    for which, (source, target) in enumerate(pairs):
        copies.append(
            pltpu.make_async_copy(source.at[level], target.at[level], keep_sem.at[which])
        )
        for hop in range(layers - 1):
            to = lax.rem(level + hop + 1, layers)
            copies.append(
                send_to(
                    source.at[to], target.at[level],
                    send.at[which, hop], recv.at[which, hop], {"seq": to},
                )
            )
    return copies


def exchange_sems(count, layers):
    return [
        pltpu.SemaphoreType.DMA((count,)),
        pltpu.SemaphoreType.DMA((count, layers - 1)),
        pltpu.SemaphoreType.DMA((count, layers - 1)),
    ]


def reduce_kernel(
    steps, rows, layers, lag, slots_ref, last_ref, grad_ref, out_ref, last_out, grad_out,
    own, inbox, first, second, up, down, down_sum, keep_sem, swap_send, swap_recv, own_sem, core_send, core_recv, one_send, one_recv, two_send, two_recv,
    up_send, up_recv, down_send, down_recv,
):
    size = (2, 2)
    y, x, core = place(size)
    level = lax.axis_index("seq")
    other_core = device(y, x, 1 - core, size, level)
    across_x = device(y, 1 - x, core, size, level)
    across_y = device(1 - y, x, core, size, level)
    above = device(y, x, core, size, lax.rem(level + 1, layers))
    below = device(y, x, core, size, lax.rem(level + layers - 1, layers))
    firsts, seconds = [across_x, across_y], [across_y, across_x]

    def span(half, step):
        return pl.ds(pl.multiple_of((half * steps + step) * rows, rows), rows)

    def remote(source, target, send, recv, half, step, where):
        return send_to(source, target, send.at[half, step], recv.at[half, step], where)

    def own_copy(half, step):
        part = span(half, step)
        return pltpu.make_async_copy(
            slots_ref.at[:, :, core, part], own.at[:, :, part], own_sem.at[half, step]
        )

    def core_copy(half, step):
        part = span(half, step)
        return remote(
            slots_ref.at[:, :, 1 - core, part], inbox.at[:, :, part],
            core_send, core_recv, half, step, other_core,
        )

    def one_copy(half, step):
        part = span(half, step)
        source = own.at[:, 1 - x, part] if half == 0 else own.at[1 - y, :, part]
        return remote(source, first.at[:, part], one_send, one_recv, half, step, firsts[half])

    def two_copy(half, step):
        part = span(half, step)
        source = own.at[1 - y, x, part] if half == 0 else own.at[y, 1 - x, part]
        return remote(source, second.at[part], two_send, two_recv, half, step, seconds[half])

    def up_copy(half, step):
        part = span(half, step)
        return remote(up.at[part], up.at[part], up_send, up_recv, half, step, above)

    def down_copy(half, step):
        part = span(half, step)
        return remote(down_sum.at[part], down.at[part], down_send, down_recv, half, step, below)

    def inside(step):
        return jnp.logical_and(step >= 0, step < steps)

    peers = [
        device(y, x, core, size, lax.rem(level + hop + 1, layers)) for hop in range(layers - 1)
    ]
    greet([other_core, across_x, across_y] + peers)
    moves = exchange(
        level, layers, [(last_ref, last_out), (grad_ref, grad_out)], keep_sem, swap_send, swap_recv
    )
    for move in moves:
        move.start()

    @pl.loop(0, steps)
    def _(step):
        for half in range(2):
            own_copy(half, step).start()
            core_copy(half, step).start()

    @pl.loop(0, steps + lag * (layers + 1))
    def _(tick):
        one_step = tick - lag
        two_step = tick - 2 * lag
        up_step = two_step - lag * level
        down_step = two_step - lag * (layers - 1 - level)
        last_step = two_step - lag * (layers - 1)

        @pl.when(inside(tick))
        def _():
            for half in range(2):
                part = span(half, tick)
                own_copy(half, tick).wait()
                core_copy(half, tick).wait_recv()
                own[:, :, part] = own[:, :, part] + inbox[:, :, part]

        @pl.when(inside(one_step))
        def _():
            for half in range(2):
                part = span(half, one_step)
                one_copy(half, one_step).wait_recv()
                if half == 0:
                    own[:, x, part] = own[:, x, part] + first[:, part]
                else:
                    own[y, :, part] = own[y, :, part] + first[:, part]

        @pl.when(inside(two_step))
        def _():
            for half in range(2):
                part = span(half, two_step)
                two_copy(half, two_step).wait_recv()
                own[y, x, part] = own[y, x, part] + second[part]

        @pl.when(inside(up_step))
        def _():
            for half in range(2):
                part = span(half, up_step)

                @pl.when(level > 0)
                def _():
                    up_copy(half, up_step).wait_recv()
                    up[part] = up[part] + own[y, x, part]

                @pl.when(level == 0)
                def _():
                    up[part] = own[y, x, part]

        @pl.when(inside(down_step))
        def _():
            for half in range(2):
                part = span(half, down_step)

                @pl.when(level < layers - 1)
                def _():
                    down_copy(half, down_step).wait_recv()
                    down_sum[part] = down[part] + own[y, x, part]

                @pl.when(level == layers - 1)
                def _():
                    down_sum[part] = own[y, x, part]

        @pl.when(inside(last_step))
        def _():
            for half in range(2):
                part = span(half, last_step)

                @pl.when(level < layers - 1)
                def _():
                    out_ref[part] = up[part] + down[part]

                @pl.when(level == layers - 1)
                def _():
                    out_ref[part] = up[part]

        @pl.when(inside(tick))
        def _():
            for half in range(2):
                one_copy(half, tick).start()

        @pl.when(inside(one_step))
        def _():
            for half in range(2):
                two_copy(half, one_step).start()

        @pl.when(jnp.logical_and(inside(up_step), level < layers - 1))
        def _():
            for half in range(2):
                up_copy(half, up_step).start()

        @pl.when(jnp.logical_and(inside(down_step), level > 0))
        def _():
            for half in range(2):
                down_copy(half, down_step).start()

    for move in moves:
        move.wait()

    @pl.loop(0, steps)
    def _(step):
        for half in range(2):
            core_copy(half, step).wait_send()
            one_copy(half, step).wait_send()
            two_copy(half, step).wait_send()

            @pl.when(level < layers - 1)
            def _():
                up_copy(half, step).wait_send()

            @pl.when(level > 0)
            def _():
                down_copy(half, step).wait_send()


def reduce_slots(slots, last, grad, layers, rows, lag):
    total = slots.shape[0] // 8 * PACK
    steps = total // (2 * rows)
    chunk = (total, LANE)
    sems = pltpu.SemaphoreType.DMA((2, steps))
    anywhere = pl.BlockSpec(memory_space=pl.ANY)
    out, last, grad = pl.pallas_call(
        functools.partial(reduce_kernel, steps, rows, layers, lag),
        in_specs=[anywhere] * 3,
        out_specs=[pl.BlockSpec(memory_space=pltpu.VMEM), anywhere, anywhere],
        out_shape=[
            jax.ShapeDtypeStruct(chunk, bf16),
            jax.ShapeDtypeStruct(last.shape, last.dtype),
            jax.ShapeDtypeStruct(grad.shape, grad.dtype),
        ],
        scratch_shapes=[
            pltpu.VMEM((2, 2) + chunk, bf16),
            pltpu.VMEM((2, 2) + chunk, bf16),
            pltpu.VMEM((2,) + chunk, bf16),
        ]
        + [pltpu.VMEM(chunk, bf16)] * 4
        + exchange_sems(2, layers)
        + [sems] * 11,
        compiler_params=pltpu.CompilerParams(
            vmem_limit_bytes=62 * 2**20, collective_id=0, has_side_effects=True
        ),
        cost_estimate=pl.CostEstimate(flops=0, bytes_accessed=WAIT_BYTES, transcendentals=0),
        name="reduce_slots",
    )(slots.reshape((2, 2, 2) + chunk), last, grad)
    return out.reshape(total // PACK, PACK, LANE), last, grad


def gather_kernel(
    alone, steps, rows, lag, layers, mine_ref, token_ref, cot_ref, weight_ref,
    out_ref, token_out, cot_out, weight_out, own_sem, keep_sem, swap_send, swap_recv,
    one_send, one_recv, two_send, two_recv,
    near_send, near_recv, far_send, far_recv, core_send, core_recv,
):
    size = (2, 2)
    y, x, core = place(size)
    level = lax.axis_index("seq")
    side = lax.rem(level, 2)
    other_core = device(y, x, 1 - core, size, level)
    across_x = device(y, 1 - x, core, size, level)
    across_y = device(1 - y, x, core, size, level)
    beside = device(y, x, core, size, level + 1 - 2 * side)
    firsts, seconds = [across_x, across_y], [across_y, across_x]

    half_rows = (2 * alone + steps) * rows
    turns = alone + steps

    def span(half, step):
        return pl.ds(pl.multiple_of(half * half_rows + step * rows, rows), rows)

    def place_of(turn):
        late = jnp.where(turn >= alone, 1, 0)
        return turn + side * alone * (1 - late) + alone * late

    def given_place(step):
        return (1 - side) * alone + step

    def own_copy():
        return pltpu.make_async_copy(mine_ref, out_ref.at[y, x, core], own_sem)

    def one_copy(half, turn):
        part = span(half, place_of(turn))
        return send_to(
            mine_ref.at[part], out_ref.at[y, x, core, part],
            one_send.at[half, turn], one_recv.at[half, turn], firsts[half],
        )

    def two_copy(half, turn):
        part = span(half, place_of(turn))
        ref = out_ref.at[y, :, core, part] if half == 0 else out_ref.at[:, x, core, part]
        return send_to(
            ref, ref, two_send.at[half, turn], two_recv.at[half, turn], seconds[half]
        )

    def near_copy(half, step):
        part = span(half, side * alone + step)
        ref = out_ref.at[y, 1 - x, core, part] if half == 0 else out_ref.at[1 - y, x, core, part]
        return send_to(ref, ref, near_send.at[half, step], near_recv.at[half, step], beside)

    def far_copy(half, step):
        part = span(half, side * alone + step)
        ref = out_ref.at[1 - y, :, core, part] if half == 0 else out_ref.at[:, 1 - x, core, part]
        return send_to(ref, ref, far_send.at[half, step], far_recv.at[half, step], beside)

    def core_copy(half, step, slot):
        ref = out_ref.at[:, :, core, span(half, step)]
        return send_to(ref, ref, core_send.at[half, slot], core_recv.at[half, slot], other_core)

    peers = [
        device(y, x, core, size, lax.rem(level + hop + 1, layers)) for hop in range(layers - 1)
    ]
    greet([other_core, across_x, across_y] + peers)
    pairs = [(weight_ref, weight_out), (token_ref, token_out), (cot_ref, cot_out)]
    moves = exchange(level, layers, pairs, keep_sem, swap_send, swap_recv)
    own_copy().start()
    for move in moves:
        move.start()

    @pl.loop(0, max(turns + 2 * lag, SPREAD * alone + 4 * lag))
    def _(tick):
        @pl.when(tick < turns)
        def _():
            for half in range(2):
                one_copy(half, tick).start()

        @pl.when(tick == lag)
        def _():
            own_copy().wait()

        turn = tick - lag

        @pl.when(jnp.logical_and(turn >= 0, turn < turns))
        def _():
            for half in range(2):
                one_copy(half, turn).wait_recv()
                two_copy(half, turn).start()

        @pl.when(jnp.logical_and(turn >= 0, turn < alone))
        def _():
            for half in range(2):
                near_copy(half, turn).start()

        after = tick - 2 * lag

        @pl.when(jnp.logical_and(after >= 0, after < turns))
        def _():
            for half in range(2):
                two_copy(half, after).wait_recv()
                core_copy(half, place_of(after), after).start()

        @pl.when(jnp.logical_and(after >= 0, after < alone))
        def _():
            for half in range(2):
                far_copy(half, after).start()

        late = tick - 4 * lag
        given = lax.div(jnp.maximum(late, 0), SPREAD)

        @pl.when(jnp.logical_and(given < alone, late == SPREAD * given))
        def _():
            for half in range(2):
                near_copy(half, given).wait_recv()
                far_copy(half, given).wait_recv()
                core_copy(half, given_place(given), turns + given).start()

    for move in moves:
        move.wait()

    @pl.loop(0, turns)
    def _(turn):
        for half in range(2):
            one_copy(half, turn).wait_send()
            two_copy(half, turn).wait_send()
            core_copy(half, place_of(turn), turn).wait()

    @pl.loop(0, alone)
    def _(step):
        for half in range(2):
            near_copy(half, step).wait_send()
            far_copy(half, step).wait_send()
            core_copy(half, given_place(step), turns + step).wait()


def gather_slots(packed, tokens, cotangent, weight, layers, rows, lag):
    total = packed.shape[0] * PACK
    alone = int(total // (2 * rows) * ALONE_SHARE)
    steps = total // (2 * rows) - 2 * alone

    def sems(count):
        return [pltpu.SemaphoreType.DMA((2, count))] * 2

    anywhere = pl.BlockSpec(memory_space=pl.ANY)
    out, tokens, cotangent, weight = pl.pallas_call(
        functools.partial(gather_kernel, alone, steps, rows, lag, layers),
        in_specs=[pl.BlockSpec(memory_space=pltpu.VMEM)] + [anywhere] * 3,
        out_specs=[anywhere] * 4,
        out_shape=[jax.ShapeDtypeStruct((2, 2, 2, total, LANE), bf16)]
        + [jax.ShapeDtypeStruct(array.shape, array.dtype) for array in (tokens, cotangent, weight)],
        scratch_shapes=[pltpu.SemaphoreType.DMA]
        + exchange_sems(3, layers)
        + sems(alone + steps) * 2 + sems(alone) * 2 + sems(2 * alone + steps),
        compiler_params=pltpu.CompilerParams(
            vmem_limit_bytes=62 * 2**20, collective_id=1, has_side_effects=True
        ),
        cost_estimate=pl.CostEstimate(flops=0, bytes_accessed=WAIT_BYTES, transcendentals=0),
        name="gather_slots",
    )(packed.reshape(total, LANE), tokens, cotangent, weight)
    return out.reshape(8 * packed.shape[0], PACK, LANE), tokens, cotangent, weight


def norm_forward(hidden, gain, shift):
    center = hidden - jnp.mean(hidden, axis=-1, keepdims=True)
    spread = jnp.mean(center * center, axis=-1, keepdims=True)
    inverse = lax.rsqrt(spread + norm_eps)
    unit = center * inverse
    return (unit * gain + shift, unit, inverse)


def norm_backward(incoming, unit, inverse, gain):
    scaled = incoming * gain
    grad_hidden = inverse * (
        scaled
        - jnp.mean(scaled, axis=-1, keepdims=True)
        - unit * jnp.mean(scaled * unit, axis=-1, keepdims=True)
    )
    return (grad_hidden, jnp.sum(incoming * unit, axis=0), jnp.sum(incoming, axis=0))


def gelu(value):
    return 0.5 * value * (1.0 + lax.erf(value * 0.5**0.5))


def gelu_slope(value):
    bell = jnp.exp(-0.5 * value * value) * (0.5 / math.pi) ** 0.5
    return 0.5 * (1.0 + lax.erf(value * 0.5**0.5)) + value * bell


def unpack(vector, width):
    return [vector[number * width : (number + 1) * width] for number in range(8)] + [
        vector[8 * width :]
    ]


def forward_layer(hidden, matrices, pieces, scale):
    w_qkv, w_out, w_up, w_down = matrices
    bias_q, bias_v, bias_out, bias_down, gain_one, shift_one, gain_two, shift_two, bias_up = pieces
    hid_low = hidden.astype(bf16)
    bias_q = bias_q.reshape(-1, LANE)
    bias_qkv = jnp.stack([bias_q, jnp.zeros_like(bias_q), bias_v.reshape(-1, LANE)], axis=1)
    qkv = (dot(hid_low, w_qkv) + bias_qkv.reshape(-1)).astype(bf16)
    mixed, lse = attend(qkv, scale)
    branch = dot(mixed, w_out) + bias_out
    normed, unit_one, inv_one = norm_forward(hidden + branch, gain_one, shift_one)
    norm_low = normed.astype(bf16)
    pre_act = dot(norm_low, w_up) + bias_up
    act_low = gelu(pre_act).astype(bf16)
    down = dot(act_low, w_down) + bias_down
    result, unit_two, inv_two = norm_forward(normed + down, gain_two, shift_two)
    kept = (
        hid_low, qkv, lse, mixed, unit_one, inv_one, norm_low, pre_act, act_low, unit_two, inv_two
    )
    return (result, kept)


def backward_layer(incoming, matrices, pieces, kept, scale, slots, slot_shape, rows, base):
    w_qkv, w_out, w_up, w_down = matrices
    gain_one, gain_two = pieces[4], pieces[6]
    hid_low, qkv, lse, mixed, unit_one, inv_one, norm_low, pre_act, act_low, unit_two, inv_two = kept
    width = mixed.shape[1]
    square = (width // BLK) ** 2
    up_count = act_low.shape[1] // BLK * (width // BLK)
    grad_two, gain_two_g, shift_two_g = norm_backward(incoming, unit_two, inv_two, gain_two)
    down_low = grad_two.astype(bf16)
    slots = plain_grad(
        slots, slot_shape, rows, act_low, down_low, base + 4 * square + up_count, width
    )
    grad_act = dot(down_low, w_down, 1, 1)
    up_low = (gelu_slope(pre_act) * grad_act).astype(bf16)
    slots = plain_grad(slots, slot_shape, rows, norm_low, up_low, base + 4 * square, width)
    grad_norm = grad_two + dot(up_low, w_up, 1, 1)
    grad_one, gain_one_g, shift_one_g = norm_backward(grad_norm, unit_one, inv_one, gain_one)
    out_low = grad_one.astype(bf16)
    slots = plain_grad(slots, slot_shape, rows, mixed, out_low, base + 3 * square, width)
    grad_mix = dot(out_low, w_out, 1, 1).astype(bf16)
    grad_qkv = attend_back(qkv, lse, grad_mix, scale)
    slots = qkv_grad(slots, slot_shape, rows, hid_low, grad_qkv, base, width)
    grad_hidden = grad_one + dot(grad_qkv, w_qkv, 1, 1)

    def total(array):
        return jnp.sum(array, axis=0, dtype=f32)

    bias_qkv = total(grad_qkv).reshape(-1, 3, LANE)
    vec_grad = jnp.concatenate(
        [
            bias_qkv[:, 0].reshape(-1),
            bias_qkv[:, 2].reshape(-1),
            total(out_low),
            total(down_low),
            gain_one_g,
            shift_one_g,
            gain_two_g,
            shift_two_g,
            total(up_low),
        ]
    )
    return grad_hidden, slots, vec_grad


def swap_in(array):
    return lax.all_to_all(array, "seq", split_axis=0, concat_axis=1, tiled=True)


def swap_out(array):
    return lax.all_to_all(array, "seq", split_axis=1, concat_axis=0, tiled=True)


def near_group(seq_count):
    layers = lax.axis_size("seq")
    return lax.axis_size("dp") == 8 and layers % 2 == 0 and seq_count == layers


def gather_blocks(packed, tokens, cotangent, tok_weight):
    layers = lax.axis_size("seq")
    total = packed.shape[0] * PACK
    if near_group(tokens.shape[0]) and total % (2 * GATHER_ROWS) == 0:
        gathered, hidden, incoming, weight = gather_slots(
            packed, tokens, cotangent, tok_weight[:, None, :], layers, GATHER_ROWS, GATHER_LAG
        )
        width = tokens.shape[-1]
        return (
            gathered, hidden.reshape(1, -1, width), incoming.reshape(1, -1, width), weight.reshape(1, -1)
        )
    gathered = lax.all_gather(packed, "dp", axis=0, tiled=True)
    return gathered, swap_in(tokens), swap_in(cotangent), swap_in(tok_weight)


def reduce_blocks(slots, last, grad):
    layers = lax.axis_size("seq")
    total = slots.shape[0] // lax.axis_size("dp") * PACK
    if near_group(last.shape[0] * layers) and total % (2 * REDUCE_ROWS) == 0:
        shape = (layers, last.shape[1] // layers, last.shape[2])
        return reduce_slots(
            slots, last.reshape(shape), grad.reshape(shape), layers, REDUCE_ROWS, REDUCE_LAG
        )
    owned = lax.psum(lax.psum_scatter(slots, "dp", scatter_dimension=0, tiled=True), "seq")
    return owned, swap_out(last), swap_out(grad)


def local(
    tokens,
    cotangent,
    tok_weight,
    mask_count,
    owner_list,
    masters,
    moment_one,
    moment_two,
    left_basis,
    right_basis,
    vectors,
    vec_moment_one,
    vec_moment_two,
):
    data_parts = lax.axis_size("dp")
    seq_count, local_len, width = tokens.shape
    layer_count = vectors.shape[0]
    inner = vectors.shape[-1] - 8 * width
    owned_count = masters.shape[0]
    block_total = owner_list.shape[0]
    scale = HDIM ** (-0.5)

    master_view = row_view(masters)
    packed = pack_blocks(master_view)[:owned_count]
    gathered, hidden, incoming, weight = gather_blocks(packed, tokens, cotangent, tok_weight)

    per_seq = hidden.shape[0]
    full_len = hidden.shape[1]
    hidden = hidden.reshape(full_len, width).astype(f32)
    incoming = incoming.reshape(full_len, width).astype(f32)
    first = lax.axis_index("seq") * per_seq
    count = lax.dynamic_slice_in_dim(mask_count, first, per_seq, 0)
    positions = jnp.arange(full_len, dtype=jnp.int32)
    masked = (positions < count[0]).astype(f32)[:, None]
    incoming = incoming * (weight.reshape(full_len, 1).astype(f32) * (1.0 + masked) * 0.25)

    per_layer = block_total // layer_count
    weights = [
        layer_weights(gathered, owner_list, per_layer * number, width, inner)
        for number in range(layer_count)
    ]
    saved = []
    for number in range(layer_count):
        hidden, kept = forward_layer(
            hidden, weights[number], unpack(vectors[number], width), scale
        )
        saved.append(kept)
    last = hidden.astype(bf16).reshape(per_seq, full_len, width)

    chunk = owned_count + 1
    rows = owner_list + owner_list // owned_count
    slot_shape = (data_parts * chunk, PACK, LANE)
    slots = None
    vec_grads = [None] * layer_count
    for number in reversed(range(layer_count)):
        incoming, slots, vec_grads[number] = backward_layer(
            incoming,
            weights[number],
            unpack(vectors[number], width),
            saved[number],
            scale,
            slots,
            slot_shape,
            rows,
            per_layer * number,
        )
    vec_grad = jnp.stack(vec_grads)
    vec_high = vec_grad.astype(bf16)
    vec_low = (vec_grad - vec_high.astype(f32)).astype(bf16)
    vec_slot = jnp.concatenate([vec_high.reshape(-1, LANE), vec_low.reshape(-1, LANE)], axis=0)
    slots = slots.reshape((data_parts, chunk) + vec_slot.shape)
    vec_slots = jnp.broadcast_to(vec_slot, (data_parts, 1) + vec_slot.shape)
    slots = lax.dynamic_update_slice(slots, vec_slots, (0, owned_count, 0, 0))
    owned, layer_out, input_grad = reduce_blocks(
        slots.reshape(slot_shape), last, incoming.astype(bf16).reshape(per_seq, full_len, width)
    )
    input_grad = input_grad.astype(f32)

    vec_rows = owned[owned_count].astype(f32)
    half = PACK // 2
    vec_total = (vec_rows[:half] + vec_rows[half:]).reshape(vectors.shape)
    views = [master_view] + [
        row_view(array) for array in (moment_one, moment_two, left_basis, right_basis)
    ]
    extra = views[0].shape[0] * GROUP - chunk
    if extra > 0:
        owned = jnp.pad(owned, ((0, extra), (0, 0), (0, 0)))
    new_one, new_two, new_masters, copies = [
        row_unview(array, owned_count) for array in soap(views, owned)
    ]
    vec_one = beta_one * vec_moment_one + (1.0 - beta_one) * vec_total
    vec_two = beta_two * vec_moment_two + (1.0 - beta_two) * vec_total * vec_total
    new_vectors = vectors - vector_rate * (vec_one / fix_one) / (
        jnp.sqrt(vec_two / fix_two) + adam_eps
    )
    return (
        layer_out, input_grad, new_one, new_two, new_masters, copies, new_vectors, vec_one, vec_two
    )


def solution(mesh):
    rows = P("dp", None)
    tokens = P("dp", "seq", None)
    return jax.shard_map(
        local,
        mesh=mesh,
        in_specs=(tokens, tokens, P("dp", "seq"), P("dp"), P()) + (rows,) * 5 + (P(),) * 3,
        out_specs=(tokens, tokens) + (rows,) * 4 + (P(),) * 3,
        check_vma=False,
    )
```

```python
import functools
import math
import jax
import jax.numpy as jnp
from jax import lax
from jax.experimental import pallas as pl
from jax.experimental.pallas import tpu as pltpu
from jax.sharding import PartitionSpec as P

HEADS = 12
HDIM = 64
BLK = 192
LANE = 128
HALF = BLK // 2
PACK = BLK * BLK // LANE
GROUP = 8
GATHER_ROWS = 144
GATHER_LAG = 2
ALONE_SHARE = 0.23
SPREAD = 2
LOADS = 8
STORES = 4
REDUCE_ROWS = 144
REDUCE_LAG = 3
WAIT_BYTES = 3 * 10**8

norm_eps = 1e-05
beta_one = 0.95
beta_two = 0.95
adam_eps = 1e-08
matrix_rate = 0.02
vector_rate = 0.2
decay_rate = 0.01
step_count = 6
fix_one = 1.0 - beta_one**step_count
fix_two = 1.0 - beta_two**step_count
bf16 = jnp.bfloat16
f32 = jnp.float32


def params(**kw):
    return pltpu.CompilerParams(vmem_limit_bytes=56 * 2**20, **kw)


def low_lanes(rows):
    return lax.broadcasted_iota(jnp.int32, (rows, LANE), 1) < HDIM


def swap(value):
    return pltpu.roll(value, HDIM, 1)


def row_view(array):
    count = array.shape[0]
    padded = -count % GROUP
    if padded:
        array = jnp.pad(array, ((0, padded), (0, 0)))
    groups = (count + padded) // GROUP
    return (
        array.reshape(groups, GROUP, PACK, LANE)
        .transpose(0, 2, 1, 3)
        .reshape(groups, GROUP * PACK, LANE)
    )


def row_unview(array, count):
    groups = array.shape[0]
    return (
        array.reshape(groups, PACK, GROUP, LANE)
        .transpose(0, 2, 1, 3)
        .reshape(groups * GROUP, PACK * LANE)[:count]
    )


def triple(ref, row):
    return [ref[0, pl.ds(row + GROUP * part, HALF, stride=3 * GROUP), :] for part in range(3)]


def put_triple(ref, row, pieces):
    for part, piece in enumerate(pieces):
        ref[0, pl.ds(row + GROUP * part, HALF, stride=3 * GROUP), :] = piece


def to_square(pieces, main_ref, tail_ref):
    first, second, third = pieces
    low = low_lanes(HALF)
    second_s, third_s = swap(second), swap(third)
    main_ref[pl.ds(0, HALF, stride=2), :] = first
    main_ref[pl.ds(1, HALF, stride=2), :] = jnp.where(low, second_s, third_s)
    tail_ref[pl.ds(0, HALF, stride=2), :] = second
    tail_ref[pl.ds(1, HALF, stride=2), :] = third_s


def from_square(main_ref, tail_ref):
    low = low_lanes(HALF)
    even_main = main_ref[pl.ds(0, HALF, stride=2), :]
    odd_main = swap(main_ref[pl.ds(1, HALF, stride=2), :])
    even_tail = tail_ref[pl.ds(0, HALF, stride=2), :]
    odd_tail = swap(tail_ref[pl.ds(1, HALF, stride=2), :])
    return [even_main, jnp.where(low, even_tail, odd_main), jnp.where(low, odd_main, odd_tail)]


def pack_kernel(src_ref, out_ref, main_ref, tail_ref):
    low = low_lanes(HALF)
    for row in range(GROUP):
        spot = row % 2
        main, tail = main_ref.at[spot], tail_ref.at[spot]
        to_square(triple(src_ref, row), main, tail)
        out_ref[row, 0:BLK, :] = main[...].astype(bf16)
        out_ref[row, BLK:PACK, :] = jnp.where(
            low, tail[0:HALF, :], swap(tail[HALF:BLK, :])
        ).astype(bf16)


def pack_blocks(view):
    groups = view.shape[0]
    return pl.pallas_call(
        pack_kernel,
        grid=(groups,),
        in_specs=[pl.BlockSpec((1, GROUP * PACK, LANE), lambda i: (i, 0, 0))],
        out_specs=pl.BlockSpec((GROUP, PACK, LANE), lambda i: (i, 0, 0)),
        out_shape=jax.ShapeDtypeStruct((groups * GROUP, PACK, LANE), bf16),
        scratch_shapes=[pltpu.VMEM((2, BLK, LANE), f32), pltpu.VMEM((2, BLK, LANE), f32)],
        compiler_params=params(),
        name="pack",
    )(view)


def unfold(block):
    fold = block[BLK:PACK, :]
    return block[0:BLK, :], jnp.concatenate([fold[:, :HDIM], fold[:, HDIM:]], axis=0)


def assemble_kernel(plan, panels, owner_ref, gathered_ref, *refs):
    outs, (blocks, stage, in_sems, out_sems) = refs[:-4], refs[-4:]
    groups = 2 * BLK // LANE * 2

    def load(panel, which):
        spot = lax.rem(panel, LOADS)
        return pltpu.make_async_copy(
            gathered_ref.at[owner_ref[4 * panel + which]],
            blocks.at[spot, which],
            in_sems.at[spot, which],
        )

    def store(panel, out_ref, row, lanes_of, group):
        spot = lax.rem(panel, STORES)
        return pltpu.make_async_copy(
            stage.at[spot, group],
            out_ref.at[pl.ds(row, BLK), pl.ds(lanes_of(group), LANE)],
            out_sems.at[spot, group],
        )

    def freed(panel):
        for group in range(groups):
            store(panel, outs[0], 0, lambda group: group * LANE, group).wait()

    @pl.loop(0, LOADS - 1)
    def _(panel):
        for which in range(4):
            load(panel, which).start()

    low = low_lanes(HALF)

    def work(panel, out_ref, row, lanes_of):
        @pl.when(panel + LOADS - 1 < panels)
        def _():
            for which in range(4):
                load(panel + LOADS - 1, which).start()

        for which in range(4):
            load(panel, which).wait()

        @pl.when(panel >= STORES)
        def _():
            freed(panel)

        spot, target = lax.rem(panel, LOADS), lax.rem(panel, STORES)
        for pair in range(2):
            fold_a = blocks[spot, 2 * pair, BLK:PACK, :].astype(f32)
            fold_b = blocks[spot, 2 * pair + 1, BLK:PACK, :].astype(f32)
            tails = [(fold_a, swap(fold_b)), (swap(fold_a), fold_b)]
            stage[target, 3 * pair] = blocks[spot, 2 * pair, 0:BLK, :]
            for half, (tail_a, tail_b) in enumerate(tails):
                rows = pl.ds(half * HALF, HALF)
                main_b = swap(blocks[spot, 2 * pair + 1, rows, :].astype(f32))
                stage[target, 3 * pair + 1, rows] = jnp.where(low, tail_a, main_b).astype(bf16)
                stage[target, 3 * pair + 2, rows] = jnp.where(low, main_b, tail_b).astype(bf16)
        for group in range(groups):
            store(panel, out_ref, row, lanes_of, group).start()

    for start, count, number, kind in plan:
        out_ref = outs[number]

        @pl.loop(0, count)
        def _(step):
            if kind is None:
                across = out_ref.shape[1] // (4 * BLK)
                row, col = lax.div(step, across), lax.rem(step, across)
                first, stride = col * 4 * BLK, LANE
            else:
                row, first, stride = step, kind * LANE, 3 * LANE
            work(
                start + step,
                out_ref,
                pl.multiple_of(row * BLK, BLK),
                lambda group: pl.multiple_of(first + group * stride, LANE),
            )

    for panel in range(max(panels - STORES, 0), panels):
        freed(panel)


def all_weights(gathered, owner_list, layers, width, inner):
    side = width // BLK
    plan, shapes, start = [], [], 0
    for layer in range(layers):
        number = len(shapes)
        shapes += [(width, 3 * width), (width, width), (width, inner), (inner, width)]
        parts = [(number, kind, side) for kind in range(3)] + [
            (number + 1, None, side),
            (number + 2, None, side * (inner // width)),
            (number + 3, None, inner // BLK),
        ]
        for out, kind, count in parts:
            plan.append((start, count, out, kind))
            start += count
    anywhere = pl.BlockSpec(memory_space=pl.ANY)
    groups = 4 * BLK // LANE
    outs = pl.pallas_call(
        functools.partial(assemble_kernel, plan, start),
        grid_spec=pltpu.PrefetchScalarGridSpec(
            num_scalar_prefetch=1,
            grid=(1,),
            in_specs=[anywhere],
            out_specs=[anywhere] * len(shapes),
            scratch_shapes=[
                pltpu.VMEM((LOADS, 4, PACK, LANE), bf16),
                pltpu.VMEM((STORES, groups, BLK, LANE), bf16),
                pltpu.SemaphoreType.DMA((LOADS, 4)),
                pltpu.SemaphoreType.DMA((STORES, groups)),
            ],
        ),
        out_shape=[jax.ShapeDtypeStruct(shape, bf16) for shape in shapes],
        compiler_params=params(),
        name="assemble",
    )(owner_list, gathered)
    return [outs[4 * layer : 4 * layer + 4] for layer in range(layers)]
def dot(left, right, left_dim=1, right_dim=0):
    return lax.dot_general(
        left, right, (((left_dim,), (right_dim,)), ((), ())), preferred_element_type=f32
    )


def head_masks():
    lane = lax.broadcasted_iota(jnp.int32, (1, LANE), 1)
    first = (lane < HDIM).astype(f32)
    return [first.astype(bf16), (1.0 - first).astype(bf16)]


def attend_kernel(scale, qkv_ref, mix_ref, lse_ref):
    length = qkv_ref.shape[0]
    query, keys, values = (qkv_ref[:, pl.ds(LANE * part, LANE)] for part in range(3))
    mixed, logs = [], []
    for mask in head_masks():
        scores = dot(query * mask, keys, 1, 1) * scale
        highest = jnp.max(scores, axis=1, keepdims=True)
        raised = jnp.exp(scores - highest)
        total = jnp.sum(raised, axis=1, keepdims=True)
        probs = raised * (1.0 / total)
        mixed.append(dot(probs.astype(bf16), values))
        logs.append(highest + jnp.log(total))
    low = low_lanes(length)
    mix_ref[...] = jnp.where(low, mixed[0], mixed[1]).astype(bf16)
    lse_ref[...] = jnp.where(low, logs[0], logs[1])


def attend(qkv, scale):
    length, wide = qkv.shape
    pairs = wide // (3 * LANE)
    return pl.pallas_call(
        functools.partial(attend_kernel, scale),
        grid=(pairs,),
        in_specs=[pl.BlockSpec((length, 3 * LANE), lambda i: (0, i))],
        out_specs=[pl.BlockSpec((length, LANE), lambda i: (0, i))] * 2,
        out_shape=[
            jax.ShapeDtypeStruct((length, wide // 3), bf16),
            jax.ShapeDtypeStruct((length, wide // 3), f32),
        ],
        compiler_params=params(),
        name="attend",
    )(qkv)


def attend_back_kernel(scale, qkv_ref, lse_ref, grad_ref, out_ref):
    length = qkv_ref.shape[0]
    query, keys, values = (qkv_ref[:, pl.ds(LANE * part, LANE)] for part in range(3))
    grad = grad_ref[...]
    parts = []
    for number, mask in enumerate(head_masks()):
        scores = dot(query * mask, keys, 1, 1) * scale
        probs = jnp.exp(scores - lse_ref[:, number * HDIM : number * HDIM + 1])
        grad_probs = dot(grad * mask, values, 1, 1)
        centre = jnp.sum(probs * grad_probs, axis=1, keepdims=True)
        grad_scores = (probs * (grad_probs - centre)).astype(bf16)
        parts.append(
            (
                dot(grad_scores, keys) * scale,
                dot(grad_scores, query, 0, 0) * scale,
                dot(probs.astype(bf16), grad, 0, 0),
            )
        )
    low = low_lanes(length)
    for part in range(3):
        out_ref[:, pl.ds(LANE * part, LANE)] = jnp.where(
            low, parts[0][part], parts[1][part]
        ).astype(bf16)


def attend_back(qkv, lse, grad, scale):
    length, wide = qkv.shape
    pairs = wide // (3 * LANE)
    return pl.pallas_call(
        functools.partial(attend_back_kernel, scale),
        grid=(pairs,),
        in_specs=[
            pl.BlockSpec((length, 3 * LANE), lambda i: (0, i)),
            pl.BlockSpec((length, LANE), lambda i: (0, i)),
            pl.BlockSpec((length, LANE), lambda i: (0, i)),
        ],
        out_specs=pl.BlockSpec((length, 3 * LANE), lambda i: (0, i)),
        out_shape=jax.ShapeDtypeStruct((length, wide), bf16),
        compiler_params=params(),
        name="attend_back",
    )(qkv, lse, grad)


def weight_grad_kernel(lanes_of, block_of, panel, steps, rows_ref, left_ref, right_ref, *refs):
    out_ref, stage_ref, turned_ref, sems = refs[-4:]
    i, j = pl.program_id(0), pl.program_id(1)
    step = i * pl.num_programs(1) + j
    spot = lax.rem(step, 2)
    pairs = panel // (2 * BLK)
    count = 4 * pairs

    def copy(which, slot, row):
        return pltpu.make_async_copy(
            stage_ref.at[slot, which], out_ref.at[row], sems.at[slot, which]
        )

    @pl.when(step >= 2)
    def _():
        for which in range(count):
            copy(which, spot, 0).wait()

    @pl.when(j == 0)
    def _():
        turned_ref[...] = left_ref[...].T

    left = turned_ref[...]
    low_top, low_all = low_lanes(HALF), low_lanes(BLK)
    for pair in range(pairs):
        right = jnp.concatenate(
            [
                right_ref[:, pl.ds(pl.multiple_of(lanes_of(j, 3 * pair + part), LANE), LANE)]
                for part in range(3)
            ],
            axis=1,
        )
        product = dot(left, right)
        for half in range(2):
            tile = product[half * BLK : (half + 1) * BLK, :]
            first, second, third = (tile[:, LANE * part : LANE * (part + 1)] for part in range(3))
            which = half * 2 * pairs + 2 * pair
            stage_ref[spot, which, 0:BLK, :] = first.astype(bf16)
            stage_ref[spot, which, BLK:PACK, :] = jnp.where(
                low_top, second[0:HALF, :], swap(second[HALF:BLK, :])
            ).astype(bf16)
            stage_ref[spot, which + 1, 0:BLK, :] = swap(
                jnp.where(low_all, third, second)
            ).astype(bf16)
            stage_ref[spot, which + 1, BLK:PACK, :] = jnp.where(
                low_top, swap(third[0:HALF, :]), third[HALF:BLK, :]
            ).astype(bf16)
    for which in range(count):
        block = block_of(i, j, which // (2 * pairs), which % (2 * pairs))
        copy(which, spot, rows_ref[block]).start()

    @pl.when(step == steps - 1)
    def _():
        for which in range(count):
            copy(which, spot, 0).wait()
            if steps > 1:
                copy(which, 1 - spot, 0).wait()


def weight_grad(slots, slot_shape, rows, left, right, grid, panel, right_spec, lanes_of, block_of):
    steps = grid[0] * grid[1]
    count = 4 * (panel // (2 * BLK))
    whole = [pl.BlockSpec((left.shape[0], 2 * BLK), lambda i, j, s: (0, i)), right_spec]
    extra, aliases = [], {}
    if slots is not None:
        extra = [slots]
        aliases = {3: 0}
    return pl.pallas_call(
        functools.partial(weight_grad_kernel, lanes_of, block_of, panel, steps),
        grid_spec=pltpu.PrefetchScalarGridSpec(
            num_scalar_prefetch=1,
            grid=grid,
            in_specs=whole + [pl.BlockSpec(memory_space=pl.ANY)] * len(extra),
            out_specs=pl.BlockSpec(memory_space=pl.ANY),
            scratch_shapes=[
                pltpu.VMEM((2, count, PACK, LANE), bf16),
                pltpu.VMEM((2 * BLK, left.shape[0]), bf16),
                pltpu.SemaphoreType.DMA((2, count)),
            ],
        ),
        out_shape=jax.ShapeDtypeStruct(slot_shape, bf16),
        input_output_aliases=aliases,
        compiler_params=params(),
        name="weight_grad",
    )(rows, left, right, *extra)


def plain_grad(slots, slot_shape, rows, left, right, base, width):
    cols = right.shape[1] // BLK
    per = width // BLK
    return weight_grad(
        slots,
        slot_shape,
        rows,
        left,
        right,
        (left.shape[1] // (2 * BLK), right.shape[1] // width),
        width,
        pl.BlockSpec((right.shape[0], width), lambda i, j, s: (0, j)),
        lambda j, piece: piece * LANE,
        lambda i, j, half, col: base + (2 * i + half) * cols + j * per + col,
    )


def qkv_grad(slots, slot_shape, rows, left, right, base, width):
    per = width // BLK
    return weight_grad(
        slots,
        slot_shape,
        rows,
        left,
        right,
        (width // (2 * BLK), 3),
        width,
        pl.BlockSpec(right.shape, lambda i, j, s: (0, 0)),
        lambda j, piece: 3 * LANE * piece + LANE * j,
        lambda i, j, half, col: base + j * per * per + (2 * i + half) * per + col,
    )


def soap_kernel(
    masters_ref, one_ref, two_ref, left_ref, right_ref, grad_ref,
    one_out, two_out, masters_out, copies_out, left_sq, right_sq, work, full,
):
    def square(refs):
        return jnp.concatenate([refs[0][...], refs[1][:, :HDIM]], axis=1).astype(bf16)

    def keep(refs, value):
        refs[0][...] = value[:, :LANE]
        refs[1][:, :HDIM] = value[:, LANE:]

    for row in range(GROUP):
        spot = row
        left_refs = [left_sq.at[spot, 0], left_sq.at[spot, 1]]
        right_refs = [right_sq.at[spot, 0], right_sq.at[spot, 1]]
        refs = [work.at[spot, 0], work.at[spot, 1]]
        to_square(triple(left_ref, row), *left_refs)
        to_square(triple(right_ref, row), *right_refs)
        left, right = square(left_refs), square(right_refs)
        main, tail = unfold(grad_ref[row])
        grad = jnp.concatenate([main, tail], axis=1)
        rotated = dot(dot(left, grad, 0, 0).astype(bf16), right)
        keep(refs, rotated)
        pieces = from_square(*refs)
        ones, twos = triple(one_ref, row), triple(two_ref, row)
        ones = [beta_one * old + (1.0 - beta_one) * new for old, new in zip(ones, pieces)]
        twos = [beta_two * old + (1.0 - beta_two) * new * new for old, new in zip(twos, pieces)]
        put_triple(one_out, row, ones)
        put_triple(two_out, row, twos)
        moves = [
            (one / fix_one) / (jnp.sqrt(two / fix_two) + adam_eps) for one, two in zip(ones, twos)
        ]
        to_square(moves, *refs)
        restored = dot(dot(left, square(refs)).astype(bf16), right, 1, 1)
        keep(refs, restored)
        pieces = from_square(*refs)
        old = triple(masters_ref, row)
        new = [
            value - matrix_rate * (step + decay_rate * value) for value, step in zip(old, pieces)
        ]
        put_triple(masters_out, row, new)
        put_triple(full, row, new)
    copies_out[0] = full[0].astype(bf16)


def soap(views, grads):
    groups = views[0].shape[0]
    view_spec = pl.BlockSpec((1, GROUP * PACK, LANE), lambda i: (i, 0, 0))
    shape = (groups, GROUP * PACK, LANE)
    square = pltpu.VMEM((GROUP, 2, BLK, LANE), f32)
    return pl.pallas_call(
        soap_kernel,
        grid=(groups,),
        in_specs=[view_spec] * 5 + [pl.BlockSpec((GROUP, PACK, LANE), lambda i: (i, 0, 0))],
        out_specs=[view_spec] * 4,
        out_shape=[jax.ShapeDtypeStruct(shape, f32)] * 3 + [jax.ShapeDtypeStruct(shape, bf16)],
        scratch_shapes=[square, square, square, pltpu.VMEM((1, GROUP * PACK, LANE), f32)],
        compiler_params=params(),
        name="soap",
    )(*views, grads)


MESH = pl.DeviceIdType.MESH


def place(size):
    index = lax.axis_index("dp")
    core = lax.rem(index, 2)
    col = lax.rem(lax.div(index, 2), size[1])
    row = lax.div(index, 2 * size[1])
    return row, col, core


def device(row, col, core, size, depth):
    return {"dp": (row * size[1] + col) * 2 + core, "seq": depth}


def greet(partners):
    barrier = pltpu.get_barrier_semaphore()
    for partner in partners:
        pl.semaphore_signal(barrier, inc=1, device_id=partner, device_id_type=MESH)
    pl.semaphore_wait(barrier, len(partners))


def send_to(source, target, send, recv, where):
    return pltpu.make_async_remote_copy(
        src_ref=source,
        dst_ref=target,
        send_sem=send,
        recv_sem=recv,
        device_id=where,
        device_id_type=MESH,
    )


def exchange(level, layers, pairs, keep_sem, send, recv):
    copies = []
    for which, (source, target) in enumerate(pairs):
        copies.append(
            pltpu.make_async_copy(source.at[level], target.at[level], keep_sem.at[which])
        )
        for hop in range(layers - 1):
            to = lax.rem(level + hop + 1, layers)
            copies.append(
                send_to(
                    source.at[to], target.at[level],
                    send.at[which, hop], recv.at[which, hop], {"seq": to},
                )
            )
    return copies


def exchange_sems(count, layers):
    return [
        pltpu.SemaphoreType.DMA((count,)),
        pltpu.SemaphoreType.DMA((count, layers - 1)),
        pltpu.SemaphoreType.DMA((count, layers - 1)),
    ]


def reduce_kernel(
    steps, rows, layers, lag, slots_ref, last_ref, grad_ref, out_ref, last_out, grad_out,
    own, inbox, first, second, up, down, down_sum, keep_sem, swap_send, swap_recv, own_sem, core_send, core_recv, one_send, one_recv, two_send, two_recv,
    up_send, up_recv, down_send, down_recv,
):
    size = (2, 2)
    y, x, core = place(size)
    level = lax.axis_index("seq")
    other_core = device(y, x, 1 - core, size, level)
    across_x = device(y, 1 - x, core, size, level)
    across_y = device(1 - y, x, core, size, level)
    above = device(y, x, core, size, lax.rem(level + 1, layers))
    below = device(y, x, core, size, lax.rem(level + layers - 1, layers))
    firsts, seconds = [across_x, across_y], [across_y, across_x]

    def span(half, step):
        return pl.ds(pl.multiple_of((half * steps + step) * rows, rows), rows)

    def remote(source, target, send, recv, half, step, where):
        return send_to(source, target, send.at[half, step], recv.at[half, step], where)

    def own_copy(half, step):
        part = span(half, step)
        return pltpu.make_async_copy(
            slots_ref.at[:, :, core, part], own.at[:, :, part], own_sem.at[half, step]
        )

    def core_copy(half, step):
        part = span(half, step)
        return remote(
            slots_ref.at[:, :, 1 - core, part], inbox.at[:, :, part],
            core_send, core_recv, half, step, other_core,
        )

    def one_copy(half, step):
        part = span(half, step)
        source = own.at[:, 1 - x, part] if half == 0 else own.at[1 - y, :, part]
        return remote(source, first.at[:, part], one_send, one_recv, half, step, firsts[half])

    def two_copy(half, step):
        part = span(half, step)
        source = own.at[1 - y, x, part] if half == 0 else own.at[y, 1 - x, part]
        return remote(source, second.at[part], two_send, two_recv, half, step, seconds[half])

    def up_copy(half, step):
        part = span(half, step)
        return remote(up.at[part], up.at[part], up_send, up_recv, half, step, above)

    def down_copy(half, step):
        part = span(half, step)
        return remote(down_sum.at[part], down.at[part], down_send, down_recv, half, step, below)

    def inside(step):
        return jnp.logical_and(step >= 0, step < steps)

    peers = [
        device(y, x, core, size, lax.rem(level + hop + 1, layers)) for hop in range(layers - 1)
    ]
    greet([other_core, across_x, across_y] + peers)
    moves = exchange(
        level, layers, [(last_ref, last_out), (grad_ref, grad_out)], keep_sem, swap_send, swap_recv
    )

    @pl.loop(0, steps)
    def _(step):
        for half in range(2):
            own_copy(half, step).start()
            core_copy(half, step).start()

    @pl.loop(0, steps + lag * (layers + 1))
    def _(tick):
        one_step = tick - lag
        two_step = tick - 2 * lag
        up_step = two_step - lag * level
        down_step = two_step - lag * (layers - 1 - level)
        last_step = two_step - lag * (layers - 1)

        for turn, move in enumerate(moves):

            @pl.when(tick == lag + turn * steps // len(moves))
            def _():
                move.start()

        @pl.when(inside(tick))
        def _():
            for half in range(2):
                part = span(half, tick)
                own_copy(half, tick).wait()
                core_copy(half, tick).wait_recv()
                own[:, :, part] = own[:, :, part] + inbox[:, :, part]

        @pl.when(inside(one_step))
        def _():
            for half in range(2):
                part = span(half, one_step)
                one_copy(half, one_step).wait_recv()
                if half == 0:
                    own[:, x, part] = own[:, x, part] + first[:, part]
                else:
                    own[y, :, part] = own[y, :, part] + first[:, part]

        @pl.when(inside(two_step))
        def _():
            for half in range(2):
                part = span(half, two_step)
                two_copy(half, two_step).wait_recv()
                own[y, x, part] = own[y, x, part] + second[part]

        @pl.when(inside(up_step))
        def _():
            for half in range(2):
                part = span(half, up_step)

                @pl.when(level > 0)
                def _():
                    up_copy(half, up_step).wait_recv()
                    up[part] = up[part] + own[y, x, part]

                @pl.when(level == 0)
                def _():
                    up[part] = own[y, x, part]

        @pl.when(inside(down_step))
        def _():
            for half in range(2):
                part = span(half, down_step)

                @pl.when(level < layers - 1)
                def _():
                    down_copy(half, down_step).wait_recv()
                    down_sum[part] = down[part] + own[y, x, part]

                @pl.when(level == layers - 1)
                def _():
                    down_sum[part] = own[y, x, part]

        @pl.when(inside(last_step))
        def _():
            for half in range(2):
                part = span(half, last_step)

                @pl.when(level < layers - 1)
                def _():
                    out_ref[part] = up[part] + down[part]

                @pl.when(level == layers - 1)
                def _():
                    out_ref[part] = up[part]

        @pl.when(inside(tick))
        def _():
            for half in range(2):
                one_copy(half, tick).start()

        @pl.when(inside(one_step))
        def _():
            for half in range(2):
                two_copy(half, one_step).start()

        @pl.when(jnp.logical_and(inside(up_step), level < layers - 1))
        def _():
            for half in range(2):
                up_copy(half, up_step).start()

        @pl.when(jnp.logical_and(inside(down_step), level > 0))
        def _():
            for half in range(2):
                down_copy(half, down_step).start()

    for move in moves:
        move.wait()

    @pl.loop(0, steps)
    def _(step):
        for half in range(2):
            core_copy(half, step).wait_send()
            one_copy(half, step).wait_send()
            two_copy(half, step).wait_send()

            @pl.when(level < layers - 1)
            def _():
                up_copy(half, step).wait_send()

            @pl.when(level > 0)
            def _():
                down_copy(half, step).wait_send()


def reduce_slots(slots, last, grad, layers, rows, lag):
    total = slots.shape[0] // 8 * PACK
    steps = total // (2 * rows)
    chunk = (total, LANE)
    sems = pltpu.SemaphoreType.DMA((2, steps))
    anywhere = pl.BlockSpec(memory_space=pl.ANY)
    out, last, grad = pl.pallas_call(
        functools.partial(reduce_kernel, steps, rows, layers, lag),
        in_specs=[anywhere] * 3,
        out_specs=[pl.BlockSpec(memory_space=pltpu.VMEM), anywhere, anywhere],
        out_shape=[
            jax.ShapeDtypeStruct(chunk, bf16),
            jax.ShapeDtypeStruct(last.shape, last.dtype),
            jax.ShapeDtypeStruct(grad.shape, grad.dtype),
        ],
        scratch_shapes=[
            pltpu.VMEM((2, 2) + chunk, bf16),
            pltpu.VMEM((2, 2) + chunk, bf16),
            pltpu.VMEM((2,) + chunk, bf16),
        ]
        + [pltpu.VMEM(chunk, bf16)] * 4
        + exchange_sems(2, layers)
        + [sems] * 11,
        compiler_params=pltpu.CompilerParams(
            vmem_limit_bytes=62 * 2**20, collective_id=0, has_side_effects=True
        ),
        cost_estimate=pl.CostEstimate(flops=0, bytes_accessed=WAIT_BYTES, transcendentals=0),
        name="reduce_slots",
    )(slots.reshape((2, 2, 2) + chunk), last, grad)
    return out.reshape(total // PACK, PACK, LANE), last, grad


def gather_kernel(
    alone, steps, rows, lag, layers, mine_ref, token_ref, cot_ref, weight_ref,
    out_ref, token_out, cot_out, weight_out, own_sem, keep_sem, swap_send, swap_recv,
    one_send, one_recv, two_send, two_recv,
    near_send, near_recv, far_send, far_recv, core_send, core_recv,
):
    size = (2, 2)
    y, x, core = place(size)
    level = lax.axis_index("seq")
    side = lax.rem(level, 2)
    other_core = device(y, x, 1 - core, size, level)
    across_x = device(y, 1 - x, core, size, level)
    across_y = device(1 - y, x, core, size, level)
    beside = device(y, x, core, size, level + 1 - 2 * side)
    firsts, seconds = [across_x, across_y], [across_y, across_x]

    half_rows = (2 * alone + steps) * rows
    turns = alone + steps

    def span(half, step):
        return pl.ds(pl.multiple_of(half * half_rows + step * rows, rows), rows)

    def place_of(turn):
        late = jnp.where(turn >= alone, 1, 0)
        return turn + side * alone * (1 - late) + alone * late

    def given_place(step):
        return (1 - side) * alone + step

    def own_copy():
        return pltpu.make_async_copy(mine_ref, out_ref.at[y, x, core], own_sem)

    def one_copy(half, turn):
        part = span(half, place_of(turn))
        return send_to(
            mine_ref.at[part], out_ref.at[y, x, core, part],
            one_send.at[half, turn], one_recv.at[half, turn], firsts[half],
        )

    def two_copy(half, turn):
        part = span(half, place_of(turn))
        ref = out_ref.at[y, :, core, part] if half == 0 else out_ref.at[:, x, core, part]
        return send_to(
            ref, ref, two_send.at[half, turn], two_recv.at[half, turn], seconds[half]
        )

    def near_copy(half, step):
        part = span(half, side * alone + step)
        ref = out_ref.at[y, 1 - x, core, part] if half == 0 else out_ref.at[1 - y, x, core, part]
        return send_to(ref, ref, near_send.at[half, step], near_recv.at[half, step], beside)

    def far_copy(half, step):
        part = span(half, side * alone + step)
        ref = out_ref.at[1 - y, :, core, part] if half == 0 else out_ref.at[:, 1 - x, core, part]
        return send_to(ref, ref, far_send.at[half, step], far_recv.at[half, step], beside)

    def core_copy(half, step, slot):
        ref = out_ref.at[:, :, core, span(half, step)]
        return send_to(ref, ref, core_send.at[half, slot], core_recv.at[half, slot], other_core)

    peers = [
        device(y, x, core, size, lax.rem(level + hop + 1, layers)) for hop in range(layers - 1)
    ]
    greet([other_core, across_x, across_y] + peers)
    pairs = [(weight_ref, weight_out), (token_ref, token_out), (cot_ref, cot_out)]
    moves = exchange(level, layers, pairs, keep_sem, swap_send, swap_recv)
    own_copy().start()
    for move in moves[:layers]:
        move.start()

    @pl.loop(0, max(turns + 2 * lag, SPREAD * alone + 6 * lag))
    def _(tick):
        @pl.when(tick < turns)
        def _():
            for half in range(2):
                one_copy(half, tick).start()

        @pl.when(tick == lag)
        def _():
            own_copy().wait()

        turn = tick - lag

        @pl.when(jnp.logical_and(turn >= 0, turn < turns))
        def _():
            for half in range(2):
                one_copy(half, turn).wait_recv()
                two_copy(half, turn).start()

        @pl.when(jnp.logical_and(turn >= 0, turn < alone))
        def _():
            for half in range(2):
                near_copy(half, turn).start()

        after = tick - 2 * lag

        @pl.when(jnp.logical_and(after >= 0, after < turns))
        def _():
            for half in range(2):
                two_copy(half, after).wait_recv()
                core_copy(half, place_of(after), after).start()

        @pl.when(jnp.logical_and(after >= 0, after < alone))
        def _():
            for half in range(2):
                far_copy(half, after).start()

        @pl.when(tick == alone + 2 * lag)
        def _():
            for move in moves[layers:]:
                move.start()

        late = tick - 6 * lag
        given = lax.div(jnp.maximum(late, 0), SPREAD)

        @pl.when(jnp.logical_and(given < alone, late == SPREAD * given))
        def _():
            for half in range(2):
                near_copy(half, given).wait_recv()
                far_copy(half, given).wait_recv()
                core_copy(half, given_place(given), turns + given).start()

    for move in moves:
        move.wait()

    @pl.loop(0, turns)
    def _(turn):
        for half in range(2):
            one_copy(half, turn).wait_send()
            two_copy(half, turn).wait_send()
            core_copy(half, place_of(turn), turn).wait()

    @pl.loop(0, alone)
    def _(step):
        for half in range(2):
            near_copy(half, step).wait_send()
            far_copy(half, step).wait_send()
            core_copy(half, given_place(step), turns + step).wait()


def gather_slots(packed, tokens, cotangent, weight, layers, rows, lag):
    total = packed.shape[0] * PACK
    alone = int(total // (2 * rows) * ALONE_SHARE)
    steps = total // (2 * rows) - 2 * alone

    def sems(count):
        return [pltpu.SemaphoreType.DMA((2, count))] * 2

    anywhere = pl.BlockSpec(memory_space=pl.ANY)
    out, tokens, cotangent, weight = pl.pallas_call(
        functools.partial(gather_kernel, alone, steps, rows, lag, layers),
        in_specs=[pl.BlockSpec(memory_space=pltpu.VMEM)] + [anywhere] * 3,
        out_specs=[anywhere] * 4,
        out_shape=[jax.ShapeDtypeStruct((2, 2, 2, total, LANE), bf16)]
        + [jax.ShapeDtypeStruct(array.shape, array.dtype) for array in (tokens, cotangent, weight)],
        scratch_shapes=[pltpu.SemaphoreType.DMA]
        + exchange_sems(3, layers)
        + sems(alone + steps) * 2 + sems(alone) * 2 + sems(2 * alone + steps),
        compiler_params=pltpu.CompilerParams(
            vmem_limit_bytes=62 * 2**20, collective_id=1, has_side_effects=True
        ),
        cost_estimate=pl.CostEstimate(flops=0, bytes_accessed=WAIT_BYTES, transcendentals=0),
        name="gather_slots",
    )(packed.reshape(total, LANE), tokens, cotangent, weight)
    return out.reshape(8 * packed.shape[0], PACK, LANE), tokens, cotangent, weight


def norm_forward(hidden, gain, shift):
    center = hidden - jnp.mean(hidden, axis=-1, keepdims=True)
    spread = jnp.mean(center * center, axis=-1, keepdims=True)
    inverse = lax.rsqrt(spread + norm_eps)
    unit = center * inverse
    return (unit * gain + shift, unit, inverse)


def norm_backward(incoming, unit, inverse, gain):
    scaled = incoming * gain
    grad_hidden = inverse * (
        scaled
        - jnp.mean(scaled, axis=-1, keepdims=True)
        - unit * jnp.mean(scaled * unit, axis=-1, keepdims=True)
    )
    return (grad_hidden, jnp.sum(incoming * unit, axis=0), jnp.sum(incoming, axis=0))


def gelu(value):
    return 0.5 * value * (1.0 + lax.erf(value * 0.5**0.5))


def gelu_slope(value):
    bell = jnp.exp(-0.5 * value * value) * (0.5 / math.pi) ** 0.5
    return 0.5 * (1.0 + lax.erf(value * 0.5**0.5)) + value * bell


def unpack(vector, width):
    return [vector[number * width : (number + 1) * width] for number in range(8)] + [
        vector[8 * width :]
    ]


def forward_layer(hidden, matrices, pieces, scale):
    w_qkv, w_out, w_up, w_down = matrices
    bias_q, bias_v, bias_out, bias_down, gain_one, shift_one, gain_two, shift_two, bias_up = pieces
    hid_low = hidden.astype(bf16)
    bias_q = bias_q.reshape(-1, LANE)
    bias_qkv = jnp.stack([bias_q, jnp.zeros_like(bias_q), bias_v.reshape(-1, LANE)], axis=1)
    qkv = (dot(hid_low, w_qkv) + bias_qkv.reshape(-1)).astype(bf16)
    mixed, lse = attend(qkv, scale)
    branch = dot(mixed, w_out) + bias_out
    normed, unit_one, inv_one = norm_forward(hidden + branch, gain_one, shift_one)
    norm_low = normed.astype(bf16)
    pre_act = dot(norm_low, w_up) + bias_up
    act_low = gelu(pre_act).astype(bf16)
    down = dot(act_low, w_down) + bias_down
    result, unit_two, inv_two = norm_forward(normed + down, gain_two, shift_two)
    kept = (
        hid_low, qkv, lse, mixed, unit_one, inv_one, norm_low, pre_act, act_low, unit_two, inv_two
    )
    return (result, kept)


def backward_layer(incoming, matrices, pieces, kept, scale, slots, slot_shape, rows, base):
    w_qkv, w_out, w_up, w_down = matrices
    gain_one, gain_two = pieces[4], pieces[6]
    hid_low, qkv, lse, mixed, unit_one, inv_one, norm_low, pre_act, act_low, unit_two, inv_two = kept
    width = mixed.shape[1]
    square = (width // BLK) ** 2
    up_count = act_low.shape[1] // BLK * (width // BLK)
    grad_two, gain_two_g, shift_two_g = norm_backward(incoming, unit_two, inv_two, gain_two)
    down_low = grad_two.astype(bf16)
    slots = plain_grad(
        slots, slot_shape, rows, act_low, down_low, base + 4 * square + up_count, width
    )
    grad_act = dot(down_low, w_down, 1, 1)
    up_low = (gelu_slope(pre_act) * grad_act).astype(bf16)
    slots = plain_grad(slots, slot_shape, rows, norm_low, up_low, base + 4 * square, width)
    grad_norm = grad_two + dot(up_low, w_up, 1, 1)
    grad_one, gain_one_g, shift_one_g = norm_backward(grad_norm, unit_one, inv_one, gain_one)
    out_low = grad_one.astype(bf16)
    slots = plain_grad(slots, slot_shape, rows, mixed, out_low, base + 3 * square, width)
    grad_mix = dot(out_low, w_out, 1, 1).astype(bf16)
    grad_qkv = attend_back(qkv, lse, grad_mix, scale)
    slots = qkv_grad(slots, slot_shape, rows, hid_low, grad_qkv, base, width)
    grad_hidden = grad_one + dot(grad_qkv, w_qkv, 1, 1)

    def total(array):
        return jnp.sum(array, axis=0, dtype=f32)

    bias_qkv = total(grad_qkv).reshape(-1, 3, LANE)
    vec_grad = jnp.concatenate(
        [
            bias_qkv[:, 0].reshape(-1),
            bias_qkv[:, 2].reshape(-1),
            total(out_low),
            total(down_low),
            gain_one_g,
            shift_one_g,
            gain_two_g,
            shift_two_g,
            total(up_low),
        ]
    )
    return grad_hidden, slots, vec_grad


def swap_in(array):
    return lax.all_to_all(array, "seq", split_axis=0, concat_axis=1, tiled=True)


def swap_out(array):
    return lax.all_to_all(array, "seq", split_axis=1, concat_axis=0, tiled=True)


def near_group(seq_count):
    layers = lax.axis_size("seq")
    return lax.axis_size("dp") == 8 and layers % 2 == 0 and seq_count == layers


def gather_blocks(packed, tokens, cotangent, tok_weight):
    layers = lax.axis_size("seq")
    total = packed.shape[0] * PACK
    if near_group(tokens.shape[0]) and total % (2 * GATHER_ROWS) == 0:
        gathered, hidden, incoming, weight = gather_slots(
            packed, tokens, cotangent, tok_weight[:, None, :], layers, GATHER_ROWS, GATHER_LAG
        )
        width = tokens.shape[-1]
        return (
            gathered, hidden.reshape(1, -1, width), incoming.reshape(1, -1, width), weight.reshape(1, -1)
        )
    gathered = lax.all_gather(packed, "dp", axis=0, tiled=True)
    return gathered, swap_in(tokens), swap_in(cotangent), swap_in(tok_weight)


def reduce_blocks(slots, last, grad):
    layers = lax.axis_size("seq")
    total = slots.shape[0] // lax.axis_size("dp") * PACK
    if near_group(last.shape[0] * layers) and total % (2 * REDUCE_ROWS) == 0:
        shape = (layers, last.shape[1] // layers, last.shape[2])
        return reduce_slots(
            slots, last.reshape(shape), grad.reshape(shape), layers, REDUCE_ROWS, REDUCE_LAG
        )
    owned = lax.psum(lax.psum_scatter(slots, "dp", scatter_dimension=0, tiled=True), "seq")
    return owned, swap_out(last), swap_out(grad)


def local(
    tokens,
    cotangent,
    tok_weight,
    mask_count,
    owner_list,
    masters,
    moment_one,
    moment_two,
    left_basis,
    right_basis,
    vectors,
    vec_moment_one,
    vec_moment_two,
):
    data_parts = lax.axis_size("dp")
    seq_count, local_len, width = tokens.shape
    layer_count = vectors.shape[0]
    inner = vectors.shape[-1] - 8 * width
    owned_count = masters.shape[0]
    block_total = owner_list.shape[0]
    scale = HDIM ** (-0.5)

    master_view = row_view(masters)
    packed = pack_blocks(master_view)[:owned_count]
    gathered, hidden, incoming, weight = gather_blocks(packed, tokens, cotangent, tok_weight)

    per_seq = hidden.shape[0]
    full_len = hidden.shape[1]
    hidden = hidden.reshape(full_len, width).astype(f32)
    incoming = incoming.reshape(full_len, width).astype(f32)
    first = lax.axis_index("seq") * per_seq
    count = lax.dynamic_slice_in_dim(mask_count, first, per_seq, 0)
    positions = jnp.arange(full_len, dtype=jnp.int32)
    masked = (positions < count[0]).astype(f32)[:, None]
    incoming = incoming * (weight.reshape(full_len, 1).astype(f32) * (1.0 + masked) * 0.25)

    per_layer = block_total // layer_count
    weights = all_weights(gathered, owner_list, layer_count, width, inner)
    saved = []
    for number in range(layer_count):
        hidden, kept = forward_layer(
            hidden, weights[number], unpack(vectors[number], width), scale
        )
        saved.append(kept)
    last = hidden.astype(bf16).reshape(per_seq, full_len, width)

    chunk = owned_count + 1
    rows = owner_list + owner_list // owned_count
    slot_shape = (data_parts * chunk, PACK, LANE)
    slots = None
    vec_grads = [None] * layer_count
    for number in reversed(range(layer_count)):
        incoming, slots, vec_grads[number] = backward_layer(
            incoming,
            weights[number],
            unpack(vectors[number], width),
            saved[number],
            scale,
            slots,
            slot_shape,
            rows,
            per_layer * number,
        )
    vec_grad = jnp.stack(vec_grads)
    vec_high = vec_grad.astype(bf16)
    vec_low = (vec_grad - vec_high.astype(f32)).astype(bf16)
    vec_slot = jnp.concatenate([vec_high.reshape(-1, LANE), vec_low.reshape(-1, LANE)], axis=0)
    slots = slots.reshape((data_parts, chunk) + vec_slot.shape)
    vec_slots = jnp.broadcast_to(vec_slot, (data_parts, 1) + vec_slot.shape)
    slots = lax.dynamic_update_slice(slots, vec_slots, (0, owned_count, 0, 0))
    owned, layer_out, input_grad = reduce_blocks(
        slots.reshape(slot_shape), last, incoming.astype(bf16).reshape(per_seq, full_len, width)
    )
    input_grad = input_grad.astype(f32)

    vec_rows = owned[owned_count].astype(f32)
    half = PACK // 2
    vec_total = (vec_rows[:half] + vec_rows[half:]).reshape(vectors.shape)
    views = [master_view] + [
        row_view(array) for array in (moment_one, moment_two, left_basis, right_basis)
    ]
    extra = views[0].shape[0] * GROUP - chunk
    if extra > 0:
        owned = jnp.pad(owned, ((0, extra), (0, 0), (0, 0)))
    new_one, new_two, new_masters, copies = [
        row_unview(array, owned_count) for array in soap(views, owned)
    ]
    vec_one = beta_one * vec_moment_one + (1.0 - beta_one) * vec_total
    vec_two = beta_two * vec_moment_two + (1.0 - beta_two) * vec_total * vec_total
    new_vectors = vectors - vector_rate * (vec_one / fix_one) / (
        jnp.sqrt(vec_two / fix_two) + adam_eps
    )
    return (
        layer_out, input_grad, new_one, new_two, new_masters, copies, new_vectors, vec_one, vec_two
    )


def solution(mesh):
    rows = P("dp", None)
    tokens = P("dp", "seq", None)
    return jax.shard_map(
        local,
        mesh=mesh,
        in_specs=(tokens, tokens, P("dp", "seq"), P("dp"), P()) + (rows,) * 5 + (P(),) * 3,
        out_specs=(tokens, tokens) + (rows,) * 4 + (P(),) * 3,
        check_vma=False,
    )
```

```python
import functools
import math
import jax
import jax.numpy as jnp
from jax import lax
from jax.experimental import pallas as pl
from jax.experimental.pallas import tpu as pltpu
from jax.sharding import PartitionSpec as P

HEADS = 12
HDIM = 64
BLK = 192
LANE = 128
HALF = BLK // 2
PACK = BLK * BLK // LANE
GROUP = 8
GATHER_ROWS = 144
GATHER_LAG = 2
ALONE_SHARE = 0.23
SPREAD = 2
LOADS = 8
STORES = 4
RING = 6
REDUCE_ROWS = 144
REDUCE_LAG = 3
WAIT_BYTES = 3 * 10**8

norm_eps = 1e-05
beta_one = 0.95
beta_two = 0.95
adam_eps = 1e-08
matrix_rate = 0.02
vector_rate = 0.2
decay_rate = 0.01
step_count = 6
fix_one = 1.0 - beta_one**step_count
fix_two = 1.0 - beta_two**step_count
bf16 = jnp.bfloat16
f32 = jnp.float32


def params(**kw):
    return pltpu.CompilerParams(vmem_limit_bytes=56 * 2**20, **kw)


def low_lanes(rows):
    return lax.broadcasted_iota(jnp.int32, (rows, LANE), 1) < HDIM


def swap(value):
    return pltpu.roll(value, HDIM, 1)


def row_view(array):
    count = array.shape[0]
    padded = -count % GROUP
    if padded:
        array = jnp.pad(array, ((0, padded), (0, 0)))
    groups = (count + padded) // GROUP
    return (
        array.reshape(groups, GROUP, PACK, LANE)
        .transpose(0, 2, 1, 3)
        .reshape(groups, GROUP * PACK, LANE)
    )


def row_unview(array, count):
    groups = array.shape[0]
    return (
        array.reshape(groups, PACK, GROUP, LANE)
        .transpose(0, 2, 1, 3)
        .reshape(groups * GROUP, PACK * LANE)[:count]
    )


def triple(ref, row):
    return [ref[pl.ds(row + GROUP * part, HALF, stride=3 * GROUP), :] for part in range(3)]


def put_triple(ref, row, pieces):
    for part, piece in enumerate(pieces):
        ref[pl.ds(row + GROUP * part, HALF, stride=3 * GROUP), :] = piece


def to_square(pieces, main_ref, tail_ref):
    first, second, third = pieces
    low = low_lanes(HALF)
    second_s, third_s = swap(second), swap(third)
    main_ref[pl.ds(0, HALF, stride=2), :] = first
    main_ref[pl.ds(1, HALF, stride=2), :] = jnp.where(low, second_s, third_s)
    tail_ref[pl.ds(0, HALF, stride=2), :] = second
    tail_ref[pl.ds(1, HALF, stride=2), :] = third_s


def from_square(main_ref, tail_ref):
    low = low_lanes(HALF)
    even_main = main_ref[pl.ds(0, HALF, stride=2), :]
    odd_main = swap(main_ref[pl.ds(1, HALF, stride=2), :])
    even_tail = tail_ref[pl.ds(0, HALF, stride=2), :]
    odd_tail = swap(tail_ref[pl.ds(1, HALF, stride=2), :])
    return [even_main, jnp.where(low, even_tail, odd_main), jnp.where(low, odd_main, odd_tail)]


def pack_kernel(src_ref, out_ref, main_ref, tail_ref):
    low = low_lanes(HALF)
    for row in range(GROUP):
        spot = row % 2
        main, tail = main_ref.at[spot], tail_ref.at[spot]
        to_square(triple(src_ref.at[0], row), main, tail)
        out_ref[row, 0:BLK, :] = main[...].astype(bf16)
        out_ref[row, BLK:PACK, :] = jnp.where(
            low, tail[0:HALF, :], swap(tail[HALF:BLK, :])
        ).astype(bf16)


def pack_blocks(view):
    groups = view.shape[0]
    return pl.pallas_call(
        pack_kernel,
        grid=(groups,),
        in_specs=[pl.BlockSpec((1, GROUP * PACK, LANE), lambda i: (i, 0, 0))],
        out_specs=pl.BlockSpec((GROUP, PACK, LANE), lambda i: (i, 0, 0)),
        out_shape=jax.ShapeDtypeStruct((groups * GROUP, PACK, LANE), bf16),
        scratch_shapes=[pltpu.VMEM((2, BLK, LANE), f32), pltpu.VMEM((2, BLK, LANE), f32)],
        compiler_params=params(),
        name="pack",
    )(view)


def unfold(block):
    fold = block[BLK:PACK, :]
    return block[0:BLK, :], jnp.concatenate([fold[:, :HDIM], fold[:, HDIM:]], axis=0)


def assemble_kernel(plan, panels, owner_ref, gathered_ref, *refs):
    outs, (blocks, stage, in_sems, out_sems) = refs[:-4], refs[-4:]
    groups = 2 * BLK // LANE * 2

    def load(panel, which):
        spot = lax.rem(panel, LOADS)
        return pltpu.make_async_copy(
            gathered_ref.at[owner_ref[4 * panel + which]],
            blocks.at[spot, which],
            in_sems.at[spot, which],
        )

    def store(panel, out_ref, row, lanes_of, group):
        spot = lax.rem(panel, STORES)
        return pltpu.make_async_copy(
            stage.at[spot, group],
            out_ref.at[pl.ds(row, BLK), pl.ds(lanes_of(group), LANE)],
            out_sems.at[spot, group],
        )

    def freed(panel):
        for group in range(groups):
            store(panel, outs[0], 0, lambda group: group * LANE, group).wait()

    @pl.loop(0, LOADS - 1)
    def _(panel):
        for which in range(4):
            load(panel, which).start()

    low = low_lanes(HALF)

    def work(panel, out_ref, row, lanes_of):
        @pl.when(panel + LOADS - 1 < panels)
        def _():
            for which in range(4):
                load(panel + LOADS - 1, which).start()

        for which in range(4):
            load(panel, which).wait()

        @pl.when(panel >= STORES)
        def _():
            freed(panel)

        spot, target = lax.rem(panel, LOADS), lax.rem(panel, STORES)
        for pair in range(2):
            fold_a = blocks[spot, 2 * pair, BLK:PACK, :].astype(f32)
            fold_b = blocks[spot, 2 * pair + 1, BLK:PACK, :].astype(f32)
            tails = [(fold_a, swap(fold_b)), (swap(fold_a), fold_b)]
            stage[target, 3 * pair] = blocks[spot, 2 * pair, 0:BLK, :]
            for half, (tail_a, tail_b) in enumerate(tails):
                rows = pl.ds(half * HALF, HALF)
                main_b = swap(blocks[spot, 2 * pair + 1, rows, :].astype(f32))
                stage[target, 3 * pair + 1, rows] = jnp.where(low, tail_a, main_b).astype(bf16)
                stage[target, 3 * pair + 2, rows] = jnp.where(low, main_b, tail_b).astype(bf16)
        for group in range(groups):
            store(panel, out_ref, row, lanes_of, group).start()

    for start, count, number, kind in plan:
        out_ref = outs[number]

        @pl.loop(0, count)
        def _(step):
            if kind is None:
                across = out_ref.shape[1] // (4 * BLK)
                row, col = lax.div(step, across), lax.rem(step, across)
                first, stride = col * 4 * BLK, LANE
            else:
                row, first, stride = step, kind * LANE, 3 * LANE
            work(
                start + step,
                out_ref,
                pl.multiple_of(row * BLK, BLK),
                lambda group: pl.multiple_of(first + group * stride, LANE),
            )

    for panel in range(max(panels - STORES, 0), panels):
        freed(panel)


def all_weights(gathered, owner_list, layers, width, inner):
    side = width // BLK
    plan, shapes, start = [], [], 0
    for layer in range(layers):
        number = len(shapes)
        shapes += [(width, 3 * width), (width, width), (width, inner), (inner, width)]
        parts = [(number, kind, side) for kind in range(3)] + [
            (number + 1, None, side),
            (number + 2, None, side * (inner // width)),
            (number + 3, None, inner // BLK),
        ]
        for out, kind, count in parts:
            plan.append((start, count, out, kind))
            start += count
    anywhere = pl.BlockSpec(memory_space=pl.ANY)
    groups = 4 * BLK // LANE
    outs = pl.pallas_call(
        functools.partial(assemble_kernel, plan, start),
        grid_spec=pltpu.PrefetchScalarGridSpec(
            num_scalar_prefetch=1,
            grid=(1,),
            in_specs=[anywhere],
            out_specs=[anywhere] * len(shapes),
            scratch_shapes=[
                pltpu.VMEM((LOADS, 4, PACK, LANE), bf16),
                pltpu.VMEM((STORES, groups, BLK, LANE), bf16),
                pltpu.SemaphoreType.DMA((LOADS, 4)),
                pltpu.SemaphoreType.DMA((STORES, groups)),
            ],
        ),
        out_shape=[jax.ShapeDtypeStruct(shape, bf16) for shape in shapes],
        compiler_params=params(),
        name="assemble",
    )(owner_list, gathered)
    return [outs[4 * layer : 4 * layer + 4] for layer in range(layers)]
def dot(left, right, left_dim=1, right_dim=0):
    return lax.dot_general(
        left, right, (((left_dim,), (right_dim,)), ((), ())), preferred_element_type=f32
    )


def head_masks():
    lane = lax.broadcasted_iota(jnp.int32, (1, LANE), 1)
    first = (lane < HDIM).astype(f32)
    return [first.astype(bf16), (1.0 - first).astype(bf16)]


def attend_kernel(scale, qkv_ref, mix_ref, lse_ref):
    length = qkv_ref.shape[0]
    query, keys, values = (qkv_ref[:, pl.ds(LANE * part, LANE)] for part in range(3))
    mixed, logs = [], []
    for mask in head_masks():
        scores = dot(query * mask, keys, 1, 1) * scale
        highest = jnp.max(scores, axis=1, keepdims=True)
        raised = jnp.exp(scores - highest)
        total = jnp.sum(raised, axis=1, keepdims=True)
        probs = raised * (1.0 / total)
        mixed.append(dot(probs.astype(bf16), values))
        logs.append(highest + jnp.log(total))
    low = low_lanes(length)
    mix_ref[...] = jnp.where(low, mixed[0], mixed[1]).astype(bf16)
    lse_ref[...] = jnp.where(low, logs[0], logs[1])


def attend(qkv, scale):
    length, wide = qkv.shape
    pairs = wide // (3 * LANE)
    return pl.pallas_call(
        functools.partial(attend_kernel, scale),
        grid=(pairs,),
        in_specs=[pl.BlockSpec((length, 3 * LANE), lambda i: (0, i))],
        out_specs=[pl.BlockSpec((length, LANE), lambda i: (0, i))] * 2,
        out_shape=[
            jax.ShapeDtypeStruct((length, wide // 3), bf16),
            jax.ShapeDtypeStruct((length, wide // 3), f32),
        ],
        compiler_params=params(),
        name="attend",
    )(qkv)


def attend_back_kernel(scale, qkv_ref, lse_ref, grad_ref, out_ref):
    length = qkv_ref.shape[0]
    query, keys, values = (qkv_ref[:, pl.ds(LANE * part, LANE)] for part in range(3))
    grad = grad_ref[...]
    parts = []
    for number, mask in enumerate(head_masks()):
        scores = dot(query * mask, keys, 1, 1) * scale
        probs = jnp.exp(scores - lse_ref[:, number * HDIM : number * HDIM + 1])
        grad_probs = dot(grad * mask, values, 1, 1)
        centre = jnp.sum(probs * grad_probs, axis=1, keepdims=True)
        grad_scores = (probs * (grad_probs - centre)).astype(bf16)
        parts.append(
            (
                dot(grad_scores, keys) * scale,
                dot(grad_scores, query, 0, 0) * scale,
                dot(probs.astype(bf16), grad, 0, 0),
            )
        )
    low = low_lanes(length)
    for part in range(3):
        out_ref[:, pl.ds(LANE * part, LANE)] = jnp.where(
            low, parts[0][part], parts[1][part]
        ).astype(bf16)


def attend_back(qkv, lse, grad, scale):
    length, wide = qkv.shape
    pairs = wide // (3 * LANE)
    return pl.pallas_call(
        functools.partial(attend_back_kernel, scale),
        grid=(pairs,),
        in_specs=[
            pl.BlockSpec((length, 3 * LANE), lambda i: (0, i)),
            pl.BlockSpec((length, LANE), lambda i: (0, i)),
            pl.BlockSpec((length, LANE), lambda i: (0, i)),
        ],
        out_specs=pl.BlockSpec((length, 3 * LANE), lambda i: (0, i)),
        out_shape=jax.ShapeDtypeStruct((length, wide), bf16),
        compiler_params=params(),
        name="attend_back",
    )(qkv, lse, grad)


def weight_grad_kernel(lanes_of, block_of, panel, steps, rows_ref, left_ref, right_ref, *refs):
    out_ref, stage_ref, turned_ref, sems = refs[-4:]
    i, j = pl.program_id(0), pl.program_id(1)
    step = i * pl.num_programs(1) + j
    spot = lax.rem(step, 2)
    pairs = panel // (2 * BLK)
    count = 4 * pairs

    def copy(which, slot, row):
        return pltpu.make_async_copy(
            stage_ref.at[slot, which], out_ref.at[row], sems.at[slot, which]
        )

    @pl.when(step >= 2)
    def _():
        for which in range(count):
            copy(which, spot, 0).wait()

    @pl.when(j == 0)
    def _():
        turned_ref[...] = left_ref[...].T

    left = turned_ref[...]
    low_top, low_all = low_lanes(HALF), low_lanes(BLK)
    for pair in range(pairs):
        right = jnp.concatenate(
            [
                right_ref[:, pl.ds(pl.multiple_of(lanes_of(j, 3 * pair + part), LANE), LANE)]
                for part in range(3)
            ],
            axis=1,
        )
        product = dot(left, right)
        for half in range(2):
            tile = product[half * BLK : (half + 1) * BLK, :]
            first, second, third = (tile[:, LANE * part : LANE * (part + 1)] for part in range(3))
            which = half * 2 * pairs + 2 * pair
            stage_ref[spot, which, 0:BLK, :] = first.astype(bf16)
            stage_ref[spot, which, BLK:PACK, :] = jnp.where(
                low_top, second[0:HALF, :], swap(second[HALF:BLK, :])
            ).astype(bf16)
            stage_ref[spot, which + 1, 0:BLK, :] = swap(
                jnp.where(low_all, third, second)
            ).astype(bf16)
            stage_ref[spot, which + 1, BLK:PACK, :] = jnp.where(
                low_top, swap(third[0:HALF, :]), third[HALF:BLK, :]
            ).astype(bf16)
    for which in range(count):
        block = block_of(i, j, which // (2 * pairs), which % (2 * pairs))
        copy(which, spot, rows_ref[block]).start()

    @pl.when(step == steps - 1)
    def _():
        for which in range(count):
            copy(which, spot, 0).wait()
            if steps > 1:
                copy(which, 1 - spot, 0).wait()


def weight_grad(slots, slot_shape, rows, left, right, grid, panel, right_spec, lanes_of, block_of):
    steps = grid[0] * grid[1]
    count = 4 * (panel // (2 * BLK))
    whole = [pl.BlockSpec((left.shape[0], 2 * BLK), lambda i, j, s: (0, i)), right_spec]
    extra, aliases = [], {}
    if slots is not None:
        extra = [slots]
        aliases = {3: 0}
    return pl.pallas_call(
        functools.partial(weight_grad_kernel, lanes_of, block_of, panel, steps),
        grid_spec=pltpu.PrefetchScalarGridSpec(
            num_scalar_prefetch=1,
            grid=grid,
            in_specs=whole + [pl.BlockSpec(memory_space=pl.ANY)] * len(extra),
            out_specs=pl.BlockSpec(memory_space=pl.ANY),
            scratch_shapes=[
                pltpu.VMEM((2, count, PACK, LANE), bf16),
                pltpu.VMEM((2 * BLK, left.shape[0]), bf16),
                pltpu.SemaphoreType.DMA((2, count)),
            ],
        ),
        out_shape=jax.ShapeDtypeStruct(slot_shape, bf16),
        input_output_aliases=aliases,
        compiler_params=params(),
        name="weight_grad",
    )(rows, left, right, *extra)


def plain_grad(slots, slot_shape, rows, left, right, base, width):
    cols = right.shape[1] // BLK
    per = width // BLK
    return weight_grad(
        slots,
        slot_shape,
        rows,
        left,
        right,
        (left.shape[1] // (2 * BLK), right.shape[1] // width),
        width,
        pl.BlockSpec((right.shape[0], width), lambda i, j, s: (0, j)),
        lambda j, piece: piece * LANE,
        lambda i, j, half, col: base + (2 * i + half) * cols + j * per + col,
    )


def qkv_grad(slots, slot_shape, rows, left, right, base, width):
    per = width // BLK
    return weight_grad(
        slots,
        slot_shape,
        rows,
        left,
        right,
        (width // (2 * BLK), 3),
        width,
        pl.BlockSpec(right.shape, lambda i, j, s: (0, 0)),
        lambda j, piece: 3 * LANE * piece + LANE * j,
        lambda i, j, half, col: base + j * per * per + (2 * i + half) * per + col,
    )


def square_of(refs):
    return jnp.concatenate([refs[0][...], refs[1][:, :HDIM]], axis=1).astype(bf16)


def keep(refs, value):
    refs[0][...] = value[:, :LANE]
    refs[1][:, :HDIM] = value[:, LANE:]


def update_block(row, grad, sources, targets, squares):
    masters_ref, one_ref, two_ref, left_ref, right_ref = sources
    one_out, two_out, masters_out = targets
    left_refs, right_refs, refs = [[pair.at[0], pair.at[1]] for pair in squares]
    to_square(triple(left_ref, row), *left_refs)
    to_square(triple(right_ref, row), *right_refs)
    left, right = square_of(left_refs), square_of(right_refs)
    main, tail = unfold(grad)
    grad = jnp.concatenate([main, tail], axis=1)
    keep(refs, dot(dot(left, grad, 0, 0).astype(bf16), right))
    pieces = from_square(*refs)
    ones, twos = triple(one_ref, row), triple(two_ref, row)
    ones = [beta_one * old + (1.0 - beta_one) * new for old, new in zip(ones, pieces)]
    twos = [beta_two * old + (1.0 - beta_two) * new * new for old, new in zip(twos, pieces)]
    put_triple(one_out, row, ones)
    put_triple(two_out, row, twos)
    moves = [
        (one / fix_one) / (jnp.sqrt(two / fix_two) + adam_eps) for one, two in zip(ones, twos)
    ]
    to_square(moves, *refs)
    keep(refs, dot(dot(left, square_of(refs)).astype(bf16), right, 1, 1))
    pieces = from_square(*refs)
    old = triple(masters_ref, row)
    new = [value - matrix_rate * (step + decay_rate * value) for value, step in zip(old, pieces)]
    put_triple(masters_out, row, new)


def soap_kernel(
    masters_ref, one_ref, two_ref, left_ref, right_ref, grad_ref,
    one_out, two_out, masters_out, copies_out, squares,
):
    sources = [ref.at[0] for ref in (masters_ref, one_ref, two_ref, left_ref, right_ref)]
    targets = [ref.at[0] for ref in (one_out, two_out, masters_out)]

    @pl.loop(0, GROUP)
    def _(row):
        update_block(
            row, grad_ref[row], sources, targets, [squares.at[which] for which in range(3)]
        )

    copies_out[...] = masters_out[...].astype(bf16)


def soap(views, grads):
    groups = views[0].shape[0]
    view_spec = pl.BlockSpec((1, GROUP * PACK, LANE), lambda i: (i, 0, 0))
    shape = (groups, GROUP * PACK, LANE)
    return pl.pallas_call(
        soap_kernel,
        grid=(groups,),
        in_specs=[view_spec] * 5 + [pl.BlockSpec((GROUP, PACK, LANE), lambda i: (i, 0, 0))],
        out_specs=[view_spec] * 4,
        out_shape=[jax.ShapeDtypeStruct(shape, f32)] * 3 + [jax.ShapeDtypeStruct(shape, bf16)],
        scratch_shapes=[pltpu.VMEM((3, 2, BLK, LANE), f32)],
        compiler_params=params(),
        name="soap",
    )(*views, grads)


MESH = pl.DeviceIdType.MESH


def place(size):
    index = lax.axis_index("dp")
    core = lax.rem(index, 2)
    col = lax.rem(lax.div(index, 2), size[1])
    row = lax.div(index, 2 * size[1])
    return row, col, core


def device(row, col, core, size, depth):
    return {"dp": (row * size[1] + col) * 2 + core, "seq": depth}


def greet(partners):
    barrier = pltpu.get_barrier_semaphore()
    for partner in partners:
        pl.semaphore_signal(barrier, inc=1, device_id=partner, device_id_type=MESH)
    pl.semaphore_wait(barrier, len(partners))


def send_to(source, target, send, recv, where):
    return pltpu.make_async_remote_copy(
        src_ref=source,
        dst_ref=target,
        send_sem=send,
        recv_sem=recv,
        device_id=where,
        device_id_type=MESH,
    )


def exchange(level, layers, pairs, keep_sem, send, recv):
    copies = []
    for which, (source, target) in enumerate(pairs):
        copies.append(
            pltpu.make_async_copy(source.at[level], target.at[level], keep_sem.at[which])
        )
        for hop in range(layers - 1):
            to = lax.rem(level + hop + 1, layers)
            copies.append(
                send_to(
                    source.at[to], target.at[level],
                    send.at[which, hop], recv.at[which, hop], {"seq": to},
                )
            )
    return copies


def exchange_sems(count, layers):
    return [
        pltpu.SemaphoreType.DMA((count,)),
        pltpu.SemaphoreType.DMA((count, layers - 1)),
        pltpu.SemaphoreType.DMA((count, layers - 1)),
    ]


def reduce_kernel(
    steps, layers, lag, slots_ref, last_ref, grad_ref,
    masters_ref, one_ref, two_ref, left_ref, right_ref,
    vec_out, last_out, grad_out, one_out, two_out, masters_out, copies_out,
    ring, own, first, second, up, down, down_sum, grad_buf, loaded, made, copied, squares,
    load_sem, store_sem, keep_sem, swap_send, swap_recv, own_sem, core_send, core_recv, one_send, one_recv, two_send, two_recv,
    up_send, up_recv, down_send, down_recv,
):
    size = (2, 2)
    rows = PACK // 2
    groups = one_out.shape[0]
    y, x, core = place(size)
    level = lax.axis_index("seq")
    other_core = device(y, x, 1 - core, size, level)
    across_x = device(y, 1 - x, core, size, level)
    across_y = device(1 - y, x, core, size, level)
    above = device(y, x, core, size, lax.rem(level + 1, layers))
    below = device(y, x, core, size, lax.rem(level + layers - 1, layers))
    firsts, seconds = [across_x, across_y], [across_y, across_x]

    def span(half, step):
        return pl.ds(pl.multiple_of((2 * step + half) * rows, rows), rows)

    def remote(source, target, send, recv, half, step, where):
        return send_to(source, target, send.at[half, step], recv.at[half, step], where)

    def own_copy(half, step):
        part = span(half, step)
        return pltpu.make_async_copy(
            slots_ref.at[:, :, core, part], ring.at[lax.rem(step, RING), half], own_sem.at[half, step]
        )

    def core_copy(half, step):
        part = span(half, step)
        return remote(
            slots_ref.at[:, :, 1 - core, part], own.at[:, :, part],
            core_send, core_recv, half, step, other_core,
        )

    def one_copy(half, step):
        part = span(half, step)
        source = own.at[:, 1 - x, part] if half == 0 else own.at[1 - y, :, part]
        return remote(source, first.at[:, part], one_send, one_recv, half, step, firsts[half])

    def two_copy(half, step):
        part = span(half, step)
        source = own.at[1 - y, x, part] if half == 0 else own.at[y, 1 - x, part]
        return remote(source, second.at[part], two_send, two_recv, half, step, seconds[half])

    def up_copy(half, step):
        part = span(half, step)
        return remote(up.at[part], up.at[part], up_send, up_recv, half, step, above)

    def down_copy(half, step):
        part = span(half, step)
        return remote(down_sum.at[part], down.at[part], down_send, down_recv, half, step, below)

    def inside(step):
        return jnp.logical_and(step >= 0, step < steps)

    peers = [
        device(y, x, core, size, lax.rem(level + hop + 1, layers)) for hop in range(layers - 1)
    ]
    greet([other_core, across_x, across_y] + peers)
    moves = exchange(
        level, layers, [(last_ref, last_out), (grad_ref, grad_out)], keep_sem, swap_send, swap_recv
    )

    def load(group, which):
        source = (masters_ref, one_ref, two_ref, left_ref, right_ref)[which]
        spot = lax.rem(group, 2)
        return pltpu.make_async_copy(
            source.at[group], loaded.at[which, spot], load_sem.at[which, spot]
        )

    def store(group, which):
        spot = lax.rem(group, 2)
        source = copied.at[spot] if which == 3 else made.at[which, spot]
        target = (one_out, two_out, masters_out, copies_out)[which]
        return pltpu.make_async_copy(source, target.at[group], store_sem.at[which, spot])

    def update(block):
        group, row = lax.div(block, GROUP), lax.rem(block, GROUP)
        spot = lax.rem(group, 2)

        @pl.when(row == 0)
        def _():
            for which in range(5):
                load(group, which).wait()

            @pl.when(group >= 2)
            def _():
                for which in range(4):
                    store(group - 2, which).wait()

        update_block(
            row,
            grad_buf[...],
            [loaded.at[which, spot] for which in range(5)],
            [made.at[which, spot] for which in range(3)],
            [squares.at[which] for which in range(3)],
        )

        @pl.when(row == GROUP - 1)
        def _():
            copied[spot] = made[2, spot].astype(bf16)
            for which in range(4):
                store(group, which).start()

            @pl.when(group + 2 < groups)
            def _():
                for which in range(5):
                    load(group + 2, which).start()

    @pl.loop(0, steps)
    def _(step):
        for half in range(2):
            core_copy(half, step).start()

    @pl.loop(0, RING - 1)
    def _(step):
        for half in range(2):
            own_copy(half, step).start()

    for group in range(min(2, groups)):
        for which in range(5):
            load(group, which).start()

    @pl.loop(0, steps + lag * (layers + 1))
    def _(tick):
        one_step = tick - lag
        two_step = tick - 2 * lag
        up_step = two_step - lag * level
        down_step = two_step - lag * (layers - 1 - level)
        last_step = two_step - lag * (layers - 1)

        for turn, move in enumerate(moves):

            @pl.when(tick == lag + turn * steps // len(moves))
            def _():
                move.start()

        @pl.when(tick + RING - 1 < steps)
        def _():
            for half in range(2):
                own_copy(half, tick + RING - 1).start()

        @pl.when(inside(tick))
        def _():
            for half in range(2):
                part = span(half, tick)
                own_copy(half, tick).wait()
                core_copy(half, tick).wait_recv()
                own[:, :, part] = own[:, :, part] + ring[lax.rem(tick, RING), half]

        @pl.when(inside(one_step))
        def _():
            for half in range(2):
                part = span(half, one_step)
                one_copy(half, one_step).wait_recv()
                if half == 0:
                    own[:, x, part] = own[:, x, part] + first[:, part]
                else:
                    own[y, :, part] = own[y, :, part] + first[:, part]

        @pl.when(inside(two_step))
        def _():
            for half in range(2):
                part = span(half, two_step)
                two_copy(half, two_step).wait_recv()
                own[y, x, part] = own[y, x, part] + second[part]

        @pl.when(inside(up_step))
        def _():
            for half in range(2):
                part = span(half, up_step)

                @pl.when(level > 0)
                def _():
                    up_copy(half, up_step).wait_recv()
                    up[part] = up[part] + own[y, x, part]

                @pl.when(level == 0)
                def _():
                    up[part] = own[y, x, part]

        @pl.when(inside(down_step))
        def _():
            for half in range(2):
                part = span(half, down_step)

                @pl.when(level < layers - 1)
                def _():
                    down_copy(half, down_step).wait_recv()
                    down_sum[part] = down[part] + own[y, x, part]

                @pl.when(level == layers - 1)
                def _():
                    down_sum[part] = own[y, x, part]

        @pl.when(inside(last_step))
        def _():
            for half in range(2):
                part = span(half, last_step)

                half_rows = pl.ds(half * rows, rows)

                @pl.when(level < layers - 1)
                def _():
                    grad_buf[half_rows] = up[part] + down[part]

                @pl.when(level == layers - 1)
                def _():
                    grad_buf[half_rows] = up[part]

        @pl.when(inside(tick))
        def _():
            for half in range(2):
                one_copy(half, tick).start()

        @pl.when(inside(one_step))
        def _():
            for half in range(2):
                two_copy(half, one_step).start()

        @pl.when(jnp.logical_and(inside(up_step), level < layers - 1))
        def _():
            for half in range(2):
                up_copy(half, up_step).start()

        @pl.when(jnp.logical_and(inside(down_step), level > 0))
        def _():
            for half in range(2):
                down_copy(half, down_step).start()

        @pl.when(jnp.logical_and(last_step >= 0, last_step < steps - 1))
        def _():
            update(last_step)

        @pl.when(last_step == steps - 1)
        def _():
            vec_out[...] = grad_buf[...]

    for move in moves:
        move.wait()
    for group in range(max(groups - 2, 0), groups):
        for which in range(4):
            store(group, which).wait()

    @pl.loop(0, steps)
    def _(step):
        for half in range(2):
            core_copy(half, step).wait_send()
            one_copy(half, step).wait_send()
            two_copy(half, step).wait_send()

            @pl.when(level < layers - 1)
            def _():
                up_copy(half, step).wait_send()

            @pl.when(level > 0)
            def _():
                down_copy(half, step).wait_send()


def reduce_slots(slots, last, grad, views, layers, lag):
    total = slots.shape[0] // 8 * PACK
    steps = total // PACK
    chunk = (total, LANE)
    view = views[0].shape
    sems = pltpu.SemaphoreType.DMA((2, steps))
    anywhere = pl.BlockSpec(memory_space=pl.ANY)
    vec_slot, last, grad, *updated = pl.pallas_call(
        functools.partial(reduce_kernel, steps, layers, lag),
        in_specs=[anywhere] * 8,
        out_specs=[pl.BlockSpec(memory_space=pltpu.VMEM)] + [anywhere] * 6,
        out_shape=[
            jax.ShapeDtypeStruct((PACK, LANE), bf16),
            jax.ShapeDtypeStruct(last.shape, last.dtype),
            jax.ShapeDtypeStruct(grad.shape, grad.dtype),
        ]
        + [jax.ShapeDtypeStruct(view, f32)] * 3
        + [jax.ShapeDtypeStruct(view, bf16)],
        scratch_shapes=[
            pltpu.VMEM((RING, 2, 2, 2, PACK // 2, LANE), bf16),
            pltpu.VMEM((2, 2) + chunk, bf16),
            pltpu.VMEM((2,) + chunk, bf16),
        ]
        + [pltpu.VMEM(chunk, bf16)] * 4
        + [
            pltpu.VMEM((PACK, LANE), bf16),
            pltpu.VMEM((5, 2) + view[1:], f32),
            pltpu.VMEM((3, 2) + view[1:], f32),
            pltpu.VMEM((2,) + view[1:], bf16),
            pltpu.VMEM((3, 2, BLK, LANE), f32),
            pltpu.SemaphoreType.DMA((5, 2)),
            pltpu.SemaphoreType.DMA((4, 2)),
        ]
        + exchange_sems(2, layers)
        + [sems] * 11,
        compiler_params=pltpu.CompilerParams(
            vmem_limit_bytes=63 * 2**20, collective_id=0, has_side_effects=True
        ),
        name="reduce_slots",
    )(slots.reshape((2, 2, 2) + chunk), last, grad, *views)
    return updated, vec_slot, last, grad


def gather_kernel(
    alone, steps, rows, lag, layers, mine_ref, token_ref, cot_ref, weight_ref,
    out_ref, token_out, cot_out, weight_out, own_sem, keep_sem, swap_send, swap_recv,
    one_send, one_recv, two_send, two_recv,
    near_send, near_recv, far_send, far_recv, core_send, core_recv,
):
    size = (2, 2)
    y, x, core = place(size)
    level = lax.axis_index("seq")
    side = lax.rem(level, 2)
    other_core = device(y, x, 1 - core, size, level)
    across_x = device(y, 1 - x, core, size, level)
    across_y = device(1 - y, x, core, size, level)
    beside = device(y, x, core, size, level + 1 - 2 * side)
    firsts, seconds = [across_x, across_y], [across_y, across_x]

    half_rows = (2 * alone + steps) * rows
    turns = alone + steps

    def span(half, step):
        return pl.ds(pl.multiple_of(half * half_rows + step * rows, rows), rows)

    def place_of(turn):
        late = jnp.where(turn >= alone, 1, 0)
        return turn + side * alone * (1 - late) + alone * late

    def given_place(step):
        return (1 - side) * alone + step

    def own_copy():
        return pltpu.make_async_copy(mine_ref, out_ref.at[y, x, core], own_sem)

    def one_copy(half, turn):
        part = span(half, place_of(turn))
        return send_to(
            mine_ref.at[part], out_ref.at[y, x, core, part],
            one_send.at[half, turn], one_recv.at[half, turn], firsts[half],
        )

    def two_copy(half, turn):
        part = span(half, place_of(turn))
        ref = out_ref.at[y, :, core, part] if half == 0 else out_ref.at[:, x, core, part]
        return send_to(
            ref, ref, two_send.at[half, turn], two_recv.at[half, turn], seconds[half]
        )

    def near_copy(half, step):
        part = span(half, side * alone + step)
        ref = out_ref.at[y, 1 - x, core, part] if half == 0 else out_ref.at[1 - y, x, core, part]
        return send_to(ref, ref, near_send.at[half, step], near_recv.at[half, step], beside)

    def far_copy(half, step):
        part = span(half, side * alone + step)
        ref = out_ref.at[1 - y, :, core, part] if half == 0 else out_ref.at[:, 1 - x, core, part]
        return send_to(ref, ref, far_send.at[half, step], far_recv.at[half, step], beside)

    def core_copy(half, step, slot):
        ref = out_ref.at[:, :, core, span(half, step)]
        return send_to(ref, ref, core_send.at[half, slot], core_recv.at[half, slot], other_core)

    peers = [
        device(y, x, core, size, lax.rem(level + hop + 1, layers)) for hop in range(layers - 1)
    ]
    greet([other_core, across_x, across_y] + peers)
    pairs = [(weight_ref, weight_out), (token_ref, token_out), (cot_ref, cot_out)]
    moves = exchange(level, layers, pairs, keep_sem, swap_send, swap_recv)
    own_copy().start()
    for move in moves[:layers]:
        move.start()

    @pl.loop(0, max(turns + 2 * lag, SPREAD * alone + 6 * lag))
    def _(tick):
        @pl.when(tick < turns)
        def _():
            for half in range(2):
                one_copy(half, tick).start()

        @pl.when(tick == lag)
        def _():
            own_copy().wait()

        turn = tick - lag

        @pl.when(jnp.logical_and(turn >= 0, turn < turns))
        def _():
            for half in range(2):
                one_copy(half, turn).wait_recv()
                two_copy(half, turn).start()

        @pl.when(jnp.logical_and(turn >= 0, turn < alone))
        def _():
            for half in range(2):
                near_copy(half, turn).start()

        after = tick - 2 * lag

        @pl.when(jnp.logical_and(after >= 0, after < turns))
        def _():
            for half in range(2):
                two_copy(half, after).wait_recv()
                core_copy(half, place_of(after), after).start()

        @pl.when(jnp.logical_and(after >= 0, after < alone))
        def _():
            for half in range(2):
                far_copy(half, after).start()

        @pl.when(tick == alone + 2 * lag)
        def _():
            for move in moves[layers:]:
                move.start()

        late = tick - 6 * lag
        given = lax.div(jnp.maximum(late, 0), SPREAD)

        @pl.when(jnp.logical_and(given < alone, late == SPREAD * given))
        def _():
            for half in range(2):
                near_copy(half, given).wait_recv()
                far_copy(half, given).wait_recv()
                core_copy(half, given_place(given), turns + given).start()

    for move in moves:
        move.wait()

    @pl.loop(0, turns)
    def _(turn):
        for half in range(2):
            one_copy(half, turn).wait_send()
            two_copy(half, turn).wait_send()
            core_copy(half, place_of(turn), turn).wait()

    @pl.loop(0, alone)
    def _(step):
        for half in range(2):
            near_copy(half, step).wait_send()
            far_copy(half, step).wait_send()
            core_copy(half, given_place(step), turns + step).wait()


def gather_slots(packed, tokens, cotangent, weight, layers, rows, lag):
    total = packed.shape[0] * PACK
    alone = int(total // (2 * rows) * ALONE_SHARE)
    steps = total // (2 * rows) - 2 * alone

    def sems(count):
        return [pltpu.SemaphoreType.DMA((2, count))] * 2

    anywhere = pl.BlockSpec(memory_space=pl.ANY)
    out, tokens, cotangent, weight = pl.pallas_call(
        functools.partial(gather_kernel, alone, steps, rows, lag, layers),
        in_specs=[pl.BlockSpec(memory_space=pltpu.VMEM)] + [anywhere] * 3,
        out_specs=[anywhere] * 4,
        out_shape=[jax.ShapeDtypeStruct((2, 2, 2, total, LANE), bf16)]
        + [jax.ShapeDtypeStruct(array.shape, array.dtype) for array in (tokens, cotangent, weight)],
        scratch_shapes=[pltpu.SemaphoreType.DMA]
        + exchange_sems(3, layers)
        + sems(alone + steps) * 2 + sems(alone) * 2 + sems(2 * alone + steps),
        compiler_params=pltpu.CompilerParams(
            vmem_limit_bytes=62 * 2**20, collective_id=1, has_side_effects=True
        ),
        cost_estimate=pl.CostEstimate(flops=0, bytes_accessed=WAIT_BYTES, transcendentals=0),
        name="gather_slots",
    )(packed.reshape(total, LANE), tokens, cotangent, weight)
    return out.reshape(8 * packed.shape[0], PACK, LANE), tokens, cotangent, weight


def norm_forward(hidden, gain, shift):
    center = hidden - jnp.mean(hidden, axis=-1, keepdims=True)
    spread = jnp.mean(center * center, axis=-1, keepdims=True)
    inverse = lax.rsqrt(spread + norm_eps)
    unit = center * inverse
    return (unit * gain + shift, unit, inverse)


def norm_backward(incoming, unit, inverse, gain):
    scaled = incoming * gain
    grad_hidden = inverse * (
        scaled
        - jnp.mean(scaled, axis=-1, keepdims=True)
        - unit * jnp.mean(scaled * unit, axis=-1, keepdims=True)
    )
    return (grad_hidden, jnp.sum(incoming * unit, axis=0), jnp.sum(incoming, axis=0))


def gelu(value):
    return 0.5 * value * (1.0 + lax.erf(value * 0.5**0.5))


def gelu_slope(value):
    bell = jnp.exp(-0.5 * value * value) * (0.5 / math.pi) ** 0.5
    return 0.5 * (1.0 + lax.erf(value * 0.5**0.5)) + value * bell


def unpack(vector, width):
    return [vector[number * width : (number + 1) * width] for number in range(8)] + [
        vector[8 * width :]
    ]


def forward_layer(hidden, matrices, pieces, scale):
    w_qkv, w_out, w_up, w_down = matrices
    bias_q, bias_v, bias_out, bias_down, gain_one, shift_one, gain_two, shift_two, bias_up = pieces
    hid_low = hidden.astype(bf16)
    bias_q = bias_q.reshape(-1, LANE)
    bias_qkv = jnp.stack([bias_q, jnp.zeros_like(bias_q), bias_v.reshape(-1, LANE)], axis=1)
    qkv = (dot(hid_low, w_qkv) + bias_qkv.reshape(-1)).astype(bf16)
    mixed, lse = attend(qkv, scale)
    branch = dot(mixed, w_out) + bias_out
    normed, unit_one, inv_one = norm_forward(hidden + branch, gain_one, shift_one)
    norm_low = normed.astype(bf16)
    pre_act = dot(norm_low, w_up) + bias_up
    act_low = gelu(pre_act).astype(bf16)
    down = dot(act_low, w_down) + bias_down
    result, unit_two, inv_two = norm_forward(normed + down, gain_two, shift_two)
    kept = (
        hid_low, qkv, lse, mixed, unit_one, inv_one, norm_low, pre_act, act_low, unit_two, inv_two
    )
    return (result, kept)


def backward_layer(incoming, matrices, pieces, kept, scale, slots, slot_shape, rows, base):
    w_qkv, w_out, w_up, w_down = matrices
    gain_one, gain_two = pieces[4], pieces[6]
    hid_low, qkv, lse, mixed, unit_one, inv_one, norm_low, pre_act, act_low, unit_two, inv_two = kept
    width = mixed.shape[1]
    square = (width // BLK) ** 2
    up_count = act_low.shape[1] // BLK * (width // BLK)
    grad_two, gain_two_g, shift_two_g = norm_backward(incoming, unit_two, inv_two, gain_two)
    down_low = grad_two.astype(bf16)
    slots = plain_grad(
        slots, slot_shape, rows, act_low, down_low, base + 4 * square + up_count, width
    )
    grad_act = dot(down_low, w_down, 1, 1)
    up_low = (gelu_slope(pre_act) * grad_act).astype(bf16)
    slots = plain_grad(slots, slot_shape, rows, norm_low, up_low, base + 4 * square, width)
    grad_norm = grad_two + dot(up_low, w_up, 1, 1)
    grad_one, gain_one_g, shift_one_g = norm_backward(grad_norm, unit_one, inv_one, gain_one)
    out_low = grad_one.astype(bf16)
    slots = plain_grad(slots, slot_shape, rows, mixed, out_low, base + 3 * square, width)
    grad_mix = dot(out_low, w_out, 1, 1).astype(bf16)
    grad_qkv = attend_back(qkv, lse, grad_mix, scale)
    slots = qkv_grad(slots, slot_shape, rows, hid_low, grad_qkv, base, width)
    grad_hidden = grad_one + dot(grad_qkv, w_qkv, 1, 1)

    def total(array):
        return jnp.sum(array, axis=0, dtype=f32)

    bias_qkv = total(grad_qkv).reshape(-1, 3, LANE)
    vec_grad = jnp.concatenate(
        [
            bias_qkv[:, 0].reshape(-1),
            bias_qkv[:, 2].reshape(-1),
            total(out_low),
            total(down_low),
            gain_one_g,
            shift_one_g,
            gain_two_g,
            shift_two_g,
            total(up_low),
        ]
    )
    return grad_hidden, slots, vec_grad


def swap_in(array):
    return lax.all_to_all(array, "seq", split_axis=0, concat_axis=1, tiled=True)


def swap_out(array):
    return lax.all_to_all(array, "seq", split_axis=1, concat_axis=0, tiled=True)


def near_group(seq_count):
    layers = lax.axis_size("seq")
    return lax.axis_size("dp") == 8 and layers % 2 == 0 and seq_count == layers


def gather_blocks(packed, tokens, cotangent, tok_weight):
    layers = lax.axis_size("seq")
    total = packed.shape[0] * PACK
    if near_group(tokens.shape[0]) and total % (2 * GATHER_ROWS) == 0:
        gathered, hidden, incoming, weight = gather_slots(
            packed, tokens, cotangent, tok_weight[:, None, :], layers, GATHER_ROWS, GATHER_LAG
        )
        width = tokens.shape[-1]
        return (
            gathered, hidden.reshape(1, -1, width), incoming.reshape(1, -1, width), weight.reshape(1, -1)
        )
    gathered = lax.all_gather(packed, "dp", axis=0, tiled=True)
    return gathered, swap_in(tokens), swap_in(cotangent), swap_in(tok_weight)


def reduce_blocks(slots, last, grad, views, owned_count):
    layers = lax.axis_size("seq")
    if near_group(last.shape[0] * layers) and owned_count % GROUP == 0:
        shape = (layers, last.shape[1] // layers, last.shape[2])
        return reduce_slots(
            slots, last.reshape(shape), grad.reshape(shape), views, layers, REDUCE_LAG
        )
    owned = lax.psum(lax.psum_scatter(slots, "dp", scatter_dimension=0, tiled=True), "seq")
    vec_slot = owned[owned_count]
    extra = views[0].shape[0] * GROUP - owned.shape[0]
    if extra > 0:
        owned = jnp.pad(owned, ((0, extra), (0, 0), (0, 0)))
    return soap(views, owned), vec_slot, swap_out(last), swap_out(grad)


def local(
    tokens,
    cotangent,
    tok_weight,
    mask_count,
    owner_list,
    masters,
    moment_one,
    moment_two,
    left_basis,
    right_basis,
    vectors,
    vec_moment_one,
    vec_moment_two,
):
    data_parts = lax.axis_size("dp")
    seq_count, local_len, width = tokens.shape
    layer_count = vectors.shape[0]
    inner = vectors.shape[-1] - 8 * width
    owned_count = masters.shape[0]
    block_total = owner_list.shape[0]
    scale = HDIM ** (-0.5)

    master_view = row_view(masters)
    packed = pack_blocks(master_view)[:owned_count]
    gathered, hidden, incoming, weight = gather_blocks(packed, tokens, cotangent, tok_weight)

    per_seq = hidden.shape[0]
    full_len = hidden.shape[1]
    hidden = hidden.reshape(full_len, width).astype(f32)
    incoming = incoming.reshape(full_len, width).astype(f32)
    first = lax.axis_index("seq") * per_seq
    count = lax.dynamic_slice_in_dim(mask_count, first, per_seq, 0)
    positions = jnp.arange(full_len, dtype=jnp.int32)
    masked = (positions < count[0]).astype(f32)[:, None]
    incoming = incoming * (weight.reshape(full_len, 1).astype(f32) * (1.0 + masked) * 0.25)

    per_layer = block_total // layer_count
    weights = all_weights(gathered, owner_list, layer_count, width, inner)
    saved = []
    for number in range(layer_count):
        hidden, kept = forward_layer(
            hidden, weights[number], unpack(vectors[number], width), scale
        )
        saved.append(kept)
    last = hidden.astype(bf16).reshape(per_seq, full_len, width)

    chunk = owned_count + 1
    rows = owner_list + owner_list // owned_count
    slot_shape = (data_parts * chunk, PACK, LANE)
    slots = None
    vec_grads = [None] * layer_count
    for number in reversed(range(layer_count)):
        incoming, slots, vec_grads[number] = backward_layer(
            incoming,
            weights[number],
            unpack(vectors[number], width),
            saved[number],
            scale,
            slots,
            slot_shape,
            rows,
            per_layer * number,
        )
    vec_grad = jnp.stack(vec_grads)
    vec_high = vec_grad.astype(bf16)
    vec_low = (vec_grad - vec_high.astype(f32)).astype(bf16)
    vec_slot = jnp.concatenate([vec_high.reshape(-1, LANE), vec_low.reshape(-1, LANE)], axis=0)
    slots = slots.reshape((data_parts, chunk) + vec_slot.shape)
    vec_slots = jnp.broadcast_to(vec_slot, (data_parts, 1) + vec_slot.shape)
    slots = lax.dynamic_update_slice(slots, vec_slots, (0, owned_count, 0, 0))
    views = [master_view] + [
        row_view(array) for array in (moment_one, moment_two, left_basis, right_basis)
    ]
    updated, vec_slot, layer_out, input_grad = reduce_blocks(
        slots.reshape(slot_shape),
        last,
        incoming.astype(bf16).reshape(per_seq, full_len, width),
        views,
        owned_count,
    )
    input_grad = input_grad.astype(f32)
    new_one, new_two, new_masters, copies = [row_unview(array, owned_count) for array in updated]

    vec_rows = vec_slot.astype(f32)
    half = PACK // 2
    vec_total = (vec_rows[:half] + vec_rows[half:]).reshape(vectors.shape)
    vec_one = beta_one * vec_moment_one + (1.0 - beta_one) * vec_total
    vec_two = beta_two * vec_moment_two + (1.0 - beta_two) * vec_total * vec_total
    new_vectors = vectors - vector_rate * (vec_one / fix_one) / (
        jnp.sqrt(vec_two / fix_two) + adam_eps
    )
    return (
        layer_out, input_grad, new_one, new_two, new_masters, copies, new_vectors, vec_one, vec_two
    )


def solution(mesh):
    rows = P("dp", None)
    tokens = P("dp", "seq", None)
    return jax.shard_map(
        local,
        mesh=mesh,
        in_specs=(tokens, tokens, P("dp", "seq"), P("dp"), P()) + (rows,) * 5 + (P(),) * 3,
        out_specs=(tokens, tokens) + (rows,) * 4 + (P(),) * 3,
        check_vma=False,
    )
```
